32 devices in a mesh: dom: 16 (over z, y, x), sub: 2 (over core).
Axes of the slice: x: 2, y: 2, z: 4, core: 2. Of those that a mesh axis runs over, the one named last changes fastest.
Arguments:
- node_feats: float32 [8192, 128], P(('dom', 'sub')), may hold values from -6 to 6
- edge_in: float32 [2, 256, 128], replicated, may hold values from -0.375 to 0.375
- edge_out: float32 [2, 128, 128], replicated, may hold values from -0.5 to 0.5
- node_in: float32 [2, 256, 128], replicated, may hold values from -0.375 to 0.375
- node_out: float32 [2, 128, 128], replicated, may hold values from -0.5 to 0.5
- decoder: float32 [128], replicated, may hold values from -0.5 to 0.5
- edge_index: int32 [2, 40960], P(None, ('dom', 'sub')), may hold values from 0 to 255
- halo_index: int32 [32, 4, 64], P(('dom', 'sub')), may hold values from 0 to 255, as said below
- target: float32 [8192], P(('dom', 'sub')), may hold values from -6 to 6
Outputs:
- loss: float32 [], replicated
- prediction: float32 [8192], P(('dom', 'sub'))
- grad_edge_in: float32 [2, 256, 128], replicated
- grad_edge_out: float32 [2, 128, 128], replicated
- grad_node_in: float32 [2, 256, 128], replicated
- grad_node_out: float32 [2, 128, 128], replicated
- grad_decoder: float32 [128], replicated
The draws below stay inside these ranges and needn't reach their ends.
Inputs may be any that keep to these rules, and one draw needn't show every extreme that they name: For each sub-partition the 256 entries halo_index[p] are distinct local node numbers; entry [p, k, j] and entry [q, k', j] of the neighbour q across direction k name the same physical mesh node.
All inputs are finite; a program needn't handle non-finite values.
Results may differ from the reference program's by a relative error of at most 0.0003.
Values sent between devices are 32-bit elements; how exact they have to be, the bound alone decides.
No kernel may reach another device: no remote copies, remote signals or barrier semaphores. Data moves between devices by JAX's collectives and lax.ppermute only.
A program may use at most 64 MiB of HBM per device.

```python
import jax
import jax.numpy as jnp
from jax import lax

WIDTH = 128
LAYERS = 2
NODES_DEV = 256
HALO = 64
EDGES_DEV = 1280
NPART = 32
NALL = 8192
PARAMS = 196736
N_DOM = 16
N_SUB = 2


def draw_halo_index(key, part):
    keys = jax.random.split(jax.random.fold_in(key, 17), NPART)
    orders = jax.vmap(lambda single: jax.random.permutation(single, NODES_DEV))(keys)
    return orders[:, :4 * HALO].reshape(NPART, 4, HALO).astype(jnp.int32)


def set_ends(array, own_key, low, largest):
    longest = array.shape.index(max(array.shape))
    spots = []
    for shift in (0, 1):
        where = [jax.random.randint(jax.random.fold_in(own_key, axis), (), 0, length) for axis, length in enumerate(array.shape)]
        where[longest] = (where[longest] + shift) % array.shape[longest]
        spots.append(tuple(where))
    return array.at[spots[0]].set(low).at[spots[1]].set(largest)


def shard_levels(stream_key, extent, shards, low, high):
    def one(axis_at, shards_of):
        steps = jax.random.uniform(jax.random.fold_in(jax.random.fold_in(stream_key, 6), axis_at), (shards_of,), jnp.float32, low / len(shards), high / len(shards))
        return jnp.repeat(jnp.exp(steps), extent[axis_at] // shards_of).reshape((-1,) + (1,) * (len(extent) - axis_at - 1))

    level = one(*shards[0])
    for cut in shards[1:]:
        level = level * one(*cut)
    return level


def normal_values(key, dims, scale, bound, pieces=(), kind=jnp.bfloat16):
    level = shard_levels(key, dims, pieces, -0.22, 0.18) if pieces else 1.0
    entries = jax.random.normal(key, dims, jnp.float32) * scale * level
    return jnp.minimum(jnp.maximum(entries, -bound), bound).astype(kind)


def setup_inputs(seed: int = 0) -> dict:
    key_of = jax.random.split(jax.random.key(seed), 10)
    node_feats = normal_values(key_of[0], (NALL, WIDTH), 1.0, 6.0, ((0, 32),), jnp.float32)
    edge_in = normal_values(key_of[1], (LAYERS, 2 * WIDTH, WIDTH), (2 * WIDTH) ** -0.5, 0.375, (), jnp.float32)
    edge_out = normal_values(key_of[2], (LAYERS, WIDTH, WIDTH), WIDTH ** -0.5, 0.5, (), jnp.float32)
    node_in = normal_values(key_of[3], (LAYERS, 2 * WIDTH, WIDTH), (2 * WIDTH) ** -0.5, 0.375, (), jnp.float32)
    node_out = normal_values(key_of[4], (LAYERS, WIDTH, WIDTH), WIDTH ** -0.5, 0.5, (), jnp.float32)
    decoder = normal_values(key_of[5], (WIDTH,), WIDTH ** -0.5, 0.5, (), jnp.float32)
    edge_index = set_ends(jax.random.randint(key_of[6], (2, NPART * EDGES_DEV), 0, NODES_DEV), jax.random.fold_in(key_of[6], 1), 0, NODES_DEV - 1).astype(jnp.int32)
    halo_index = draw_halo_index(jax.random.fold_in(key_of[9], 71), 0)
    target = normal_values(key_of[8], (NALL,), 1.0, 6.0, ((0, 32),), jnp.float32)
    return {"node_feats": node_feats, "edge_in": edge_in, "edge_out": edge_out, "node_in": node_in, "node_out": node_out, "decoder": decoder, "edge_index": edge_index, "halo_index": halo_index, "target": target}


highest_precision = lax.Precision.HIGHEST

def product(left, right):
    return jnp.dot(left, right, precision=highest_precision, preferred_element_type=jnp.float32)

def message_sum(features, receivers, senders, weight_in, weight_out):
    to_receiver = product(features, weight_in[:WIDTH])
    to_sender = product(features, weight_in[WIDTH:])
    preact = to_receiver[receivers] + to_sender[senders]
    messages = product(jax.nn.silu(preact), weight_out)
    return jnp.zeros_like(features).at[receivers].add(messages)

def node_update(features, summed, weight_in, weight_out):
    preact = product(features, weight_in[:WIDTH]) + product(summed, weight_in[WIDTH:])
    return features + product(jax.nn.silu(preact), weight_out)

def shared_sum(summed, halo_index):
    outgoing = jax.vmap(lambda block, lists: block[lists])(summed, halo_index)
    outgoing = outgoing.reshape(N_DOM, N_SUB, 4, HALO, WIDTH)
    zero_dom = jnp.zeros((1, N_SUB, HALO, WIDTH), summed.dtype)
    zero_sub = jnp.zeros((N_DOM, 1, HALO, WIDTH), summed.dtype)
    lower_dom = jnp.concatenate([zero_dom, outgoing[:-1, :, 1]], 0)
    upper_dom = jnp.concatenate([outgoing[1:, :, 0], zero_dom], 0)
    lower_sub = jnp.concatenate([zero_sub, outgoing[:, :-1, 3]], 1)
    upper_sub = jnp.concatenate([outgoing[:, 1:, 2], zero_sub], 1)
    incoming = jnp.stack([lower_dom, upper_dom, lower_sub, upper_sub], 2)
    incoming = incoming.reshape(NPART, 4 * HALO, WIDTH)
    flat_lists = halo_index.reshape(NPART, 4 * HALO)
    return jax.vmap(lambda block, lists, extra: block.at[lists].add(extra))(summed, flat_lists, incoming)

def reference(node_feats, edge_in, edge_out, node_in, node_out, decoder, edge_index, halo_index, target):
    receivers = edge_index[0].reshape(NPART, EDGES_DEV)
    senders = edge_index[1].reshape(NPART, EDGES_DEV)
    checked_sum = jax.checkpoint(message_sum)

    def forward(w_edge_in, w_edge_out, w_node_in, w_node_out, w_decoder):
        features = node_feats.reshape(NPART, NODES_DEV, WIDTH)
        for layer_index in range(LAYERS):
            local_sum = jax.vmap(checked_sum, in_axes=(0, 0, 0, None, None))(features, receivers, senders, w_edge_in[layer_index], w_edge_out[layer_index])
            summed = shared_sum(local_sum, halo_index).reshape(NALL, WIDTH)
            flat = node_update(features.reshape(NALL, WIDTH), summed, w_node_in[layer_index], w_node_out[layer_index])
            features = flat.reshape(NPART, NODES_DEV, WIDTH)
        predicted = product(features.reshape(NALL, WIDTH), w_decoder)
        misfit = predicted - target
        return (jnp.sum(misfit * misfit) / NALL, predicted)
    loss, backward, predicted = jax.vjp(forward, edge_in, edge_out, node_in, node_out, decoder, has_aux=True)
    grads = backward(jnp.ones_like(loss))
    square_sum = sum((jnp.sum(grad * grad) for grad in grads))
    scale = 1.0 / jnp.sqrt(square_sum / PARAMS + 1e-06)
    return (loss, predicted, grads[0] * scale, grads[1] * scale, grads[2] * scale, grads[3] * scale, grads[4] * scale)
```

```python
import functools

import jax
import jax.numpy as jnp
from jax import lax
from jax.experimental import pallas as pl
from jax.experimental.pallas import tpu as pltpu
from jax.sharding import PartitionSpec as P

F32 = jnp.float32
BF16 = jnp.bfloat16
VMEM = pl.BlockSpec(memory_space=pltpu.VMEM)
EXTRA = 8


def halves(x):
    high = x.astype(BF16)
    low = (x - high.astype(F32)).astype(BF16)
    return high, low


def side(x):
    return jnp.concatenate(halves(x), axis=1)


def fold(x):
    width = x.shape[1] // 2
    return x[:, :width] + x[:, width:]


def dot(a, b, dims=((1,), (0,))):
    return lax.dot_general(a, b, (dims, ((), ())), preferred_element_type=F32)


def mm(x, w):
    wide = side(w)
    return fold(dot(side(x), jnp.concatenate([wide, wide], axis=0)))


def mmt(x, w):
    high, low = halves(w)
    both = jnp.concatenate(
        [jnp.concatenate([high, high], axis=1), jnp.concatenate([low, low], axis=1)], axis=0
    )
    return fold(dot(side(x), both, ((1,), (1,))))


def tmm(x, y):
    wide = fold(dot(side(x), side(y), ((0,), (0,))))
    width = x.shape[1]
    return wide[:width] + wide[width:]


def silu_parts(v):
    gate = 1.0 / (1.0 + jnp.exp(-v))
    return v * gate, gate * (1.0 + v * (1.0 - gate))


def row_of(column):
    n = column.shape[0]
    eye = lax.broadcasted_iota(jnp.int32, (n, n), 0) == lax.broadcasted_iota(jnp.int32, (n, n), 1)
    return jnp.sum(jnp.where(eye, column, 0.0), axis=0, keepdims=True)


def onehot(mask):
    return jnp.where(mask, 1.0, 0.0).astype(BF16)


def edge_forward(features, weight_in, recv, send, recv_t, slope_ref, chunk):
    width = features.shape[1]
    to_recv = side(mm(features, weight_in[:width]))
    to_send = side(mm(features, weight_in[width:]))
    total = None
    for start in range(0, recv.shape[0], chunk):
        rows = pl.ds(start, chunk)
        pre = fold(dot(recv[rows, :], to_recv) + dot(send[rows, :], to_send))
        act, slope = silu_parts(pre)
        slope_ref[rows, :] = slope
        part = dot(recv_t[:, rows], side(act))
        total = part if total is None else total + part
    return fold(total)


def edge_backward(local_grad, weight_out, recv, recv_t, send_t, slope_ref, chunk):
    spread = side(mmt(local_grad, weight_out))
    total_r = total_s = None
    for start in range(0, recv.shape[0], chunk):
        rows = pl.ds(start, chunk)
        grad = side(fold(dot(recv[rows, :], spread)) * slope_ref[rows, :])
        part_r = dot(recv_t[:, rows], grad)
        part_s = dot(send_t[:, rows], grad)
        total_r = part_r if total_r is None else total_r + part_r
        total_s = part_s if total_s is None else total_s + part_s
    return fold(total_r), fold(total_s)


def node_forward(features, summed, weight_in, weight_out):
    width = features.shape[1]
    pre = mm(features, weight_in[:width]) + mm(summed, weight_in[width:])
    act, slope = silu_parts(pre)
    return features + mm(act, weight_out), act, slope


def put_blocks(value, refs):
    size = refs[0].shape[0]
    for at, ref in enumerate(refs):
        ref[...] = value[at * size : (at + 1) * size]


def take_sum(own, came):
    parts = [
        ref[...] + came[at][...] if came[at] is not None else ref[...]
        for at, ref in enumerate(own)
    ]
    return jnp.concatenate(parts, axis=0)


def even(axis):
    return lax.rem(lax.axis_index(axis), 2) == 0


def first_kernel(
    chunk, feats, index, halo, weight_in, weight_out,
    flat_out, recv, send, recv_t, send_t, h_out, slope, q_out, *blocks
):
    nodes = feats.shape[0]
    edges = index.shape[1]
    lanes = 128
    count = edges // lanes
    size = halo.shape[2]
    pieces = [index[0:1, pl.ds(b * lanes, lanes)] for b in range(count)]
    pieces += [index[1:2, pl.ds(b * lanes, lanes)] for b in range(count)]
    table = jnp.concatenate(pieces, axis=0).astype(F32)
    lists = jnp.concatenate([halo[0].astype(F32), jnp.zeros((4, lanes - size), F32)], axis=1)
    rest = jnp.zeros((lanes - 2 * count - 4, lanes), F32)
    columns = jnp.concatenate([table, lists, rest], axis=0).T
    by_dir = [columns[:size, 2 * count + k : 2 * count + k + 1] for k in range(4)]
    dom_even, sub_even = even("dom"), even("sub")
    flat = jnp.concatenate(
        [
            jnp.where(dom_even, by_dir[1], by_dir[0]),
            jnp.where(dom_even, by_dir[0], by_dir[1]),
            jnp.where(sub_even, by_dir[3], by_dir[2]),
            jnp.where(sub_even, by_dir[2], by_dir[3]),
        ],
        axis=0,
    )
    flat_row = row_of(flat)
    flat_out[...] = jnp.broadcast_to(flat, flat_out.shape)
    for b in range(count):
        rows = pl.ds(b * lanes, lanes)
        recv[rows, :] = onehot(columns[:, b : b + 1] == flat_row)
        send[rows, :] = onehot(columns[:, count + b : count + b + 1] == flat_row)
        recv_t[:, rows] = onehot(flat == table[b : b + 1])
        send_t[:, rows] = onehot(flat == table[count + b : count + b + 1])
    place = onehot(flat == lax.broadcasted_iota(jnp.int32, (nodes, nodes), 1).astype(F32))
    features = fold(dot(place, side(feats[...])))
    h_out[...] = features
    q = edge_forward(features, weight_in[0], recv, send, recv_t, slope, chunk)
    q_out[...] = q
    put_blocks(mm(q, weight_out[0]), blocks)


def middle_kernel(
    chunk, layer, names, *refs
):
    own, refs = refs[:4], refs[4:]
    came, refs = unpack(names, refs)
    (h, recv, send, recv_t, node_in, node_out, edge_in, edge_out,
     agg_out, h_out, node_act, node_slope, slope, q_out, *blocks) = refs
    summed = take_sum(own, came)
    agg_out[...] = summed
    features, act, gate = node_forward(h[...], summed, node_in[layer], node_out[layer])
    h_out[...] = features
    node_act[...] = act
    node_slope[...] = gate
    q = edge_forward(features, edge_in[layer + 1], recv, send, recv_t, slope, chunk)
    q_out[...] = q
    put_blocks(mm(q, edge_out[layer + 1]), blocks)


def unpack(names, refs):
    came = []
    at = 0
    for there in names:
        came.append(refs[at] if there else None)
        at += there
    return came, refs[at:]


def last_kernel(
    layer, count, names, *refs
):
    own, refs = refs[:4], refs[4:]
    came, refs = unpack(names, refs)
    (h, flat_ref, target, decoder, node_in, node_out,
     agg_out, node_act, pre_grad_out, top_grad_out, through_out, pred_out, tail_out, *blocks) = refs
    nodes, width = h.shape
    summed = take_sum(own, came)
    agg_out[...] = summed
    features, act, gate = node_forward(h[...], summed, node_in[layer], node_out[layer])
    node_act[...] = act
    weights = decoder[...]
    predicted = jnp.sum(features * weights, axis=1, keepdims=True)
    flat = flat_ref[:, 0:1]
    here = flat == lax.broadcasted_iota(jnp.int32, (nodes, nodes), 1).astype(F32)
    pred_out[...] = jnp.sum(jnp.where(here, predicted, 0.0), axis=0, keepdims=True)
    wanted = jnp.sum(jnp.where(here, target[...], 0.0), axis=1, keepdims=True)
    misfit = predicted - wanted
    seed = 2.0 * misfit / count
    decoder_grad = jnp.sum(seed * features, axis=0, keepdims=True)
    loss = jnp.broadcast_to(jnp.sum(misfit * misfit, axis=0, keepdims=True), (1, width))
    tail_out[...] = jnp.concatenate([decoder_grad, loss, jnp.zeros((EXTRA - 2, width), F32)], 0)
    top = seed * weights
    top_grad_out[...] = top
    pre_grad = mmt(top, node_out[layer]) * gate
    pre_grad_out[...] = pre_grad
    through_out[...] = top + mmt(pre_grad, node_in[layer, :width])
    put_blocks(mmt(pre_grad, node_in[layer, width:]), blocks)


def node_grads_kernel(h, summed, act, pre_grad, top_grad, out):
    width = h.shape[1]
    out[0:width, :] = tmm(h[...], pre_grad[...])
    out[width : 2 * width, :] = tmm(summed[...], pre_grad[...])
    out[2 * width :, :] = tmm(act[...], top_grad[...])


def edge_grads_kernel(h, q, local_grad, to_recv, to_send, out):
    width = h.shape[1]
    out[0:width, :] = tmm(h[...], to_recv[...])
    out[width : 2 * width, :] = tmm(h[...], to_send[...])
    out[2 * width :, :] = tmm(q[...], local_grad[...])


def back_kernel(
    chunk, layer, names, *refs
):
    own, refs = refs[:4], refs[4:]
    came, refs = unpack(names, refs)
    (through, node_slope, recv, recv_t, send_t, slope, edge_in, edge_out, node_in, node_out,
     local_out, recv_out, send_out, top_out, pre_out, *blocks) = refs
    width = through.shape[1]
    local_grad = take_sum(own, came)
    local_out[...] = local_grad
    to_recv, to_send = edge_backward(
        local_grad, edge_out[layer], recv, recv_t, send_t, slope, chunk
    )
    recv_out[...] = to_recv
    send_out[...] = to_send
    top = (
        through[...]
        + mmt(to_recv, edge_in[layer, :width])
        + mmt(to_send, edge_in[layer, width:])
    )
    top_out[...] = top
    pre_grad = mmt(top, node_out[layer - 1]) * node_slope[...]
    pre_out[...] = pre_grad
    put_blocks(mmt(pre_grad, node_in[layer - 1, width:]), blocks)


def split_rows(value, ref, first):
    per = ref.shape[1] - EXTRA
    at = 0
    while at < value.shape[0]:
        group, inside = divmod(first + at, per)
        take = min(per - inside, value.shape[0] - at)
        ref[group, inside : inside + take, :] = value[at : at + take]
        at += take


def end_kernel(
    chunk, names, *refs
):
    own, refs = refs[:4], refs[4:]
    came, refs = unpack(names, refs)
    (h, q, recv, recv_t, send_t, slope, edge_out, node_low, node_high, edge_high, tail,
     mine, other) = refs
    local_grad = take_sum(own, came)
    to_recv, to_send = edge_backward(local_grad, edge_out[0], recv, recv_t, send_t, slope, chunk)
    low = [
        node_low[...],
        tmm(h[...], to_recv),
        tmm(h[...], to_send),
        tmm(q[...], local_grad),
    ]
    per = mine.shape[1] - EXTRA
    blank = jnp.zeros((mine.shape[0], EXTRA, mine.shape[2]), F32)

    def write(ref_high, ref_low):
        ref_high[:, per:, :] = blank
        ref_low[:, per:, :] = blank
        ref_high[0, per:, :] = tail[...]
        at = 0
        for value in low:
            split_rows(value, ref_low, at)
            at += value.shape[0]
        split_rows(node_high[...], ref_high, 0)
        split_rows(edge_high[...], ref_high, node_high.shape[0])

    first = lax.axis_index("sub") == 0
    pl.when(first)(lambda: write(mine, other))
    pl.when(jnp.logical_not(first))(lambda: write(other, mine))


def add_kernel(a, b, out):
    out[...] = a[...] + b[...]


def total_kernel(parts, out):
    total = jnp.sum(parts[...], axis=0)
    per = total.shape[0] - EXTRA
    body = total[: per + 1]
    squares = jnp.sum(jnp.sum(body * body, axis=0, keepdims=True), axis=1, keepdims=True)
    last = jnp.broadcast_to(squares, (1, total.shape[1]))
    total = jnp.concatenate([total[:-1], last], axis=0)
    out[...] = jnp.broadcast_to(total[None], out.shape)


def scale_kernel(
    params, count, mine, other, loss, edge_in, edge_out, node_in, node_out, decoder
):
    rows = mine.shape[1]
    per = rows - EXTRA
    width = mine.shape[2]
    squares = jnp.sum(
        mine[:, rows - 1 : rows, :] + other[:, rows - 1 : rows, :], axis=0
    )
    scale = 1.0 / jnp.sqrt(squares / params + 1e-06)

    def join(ref, first, size):
        parts = []
        at = 0
        while at < size:
            group, inside = divmod(first + at, per)
            take = min(per - inside, size - at)
            parts.append(ref[group, inside : inside + take, :])
            at += take
        return jnp.concatenate(parts, axis=0) * scale

    def write(high, low):
        for layer, ref in ((1, high), (0, low)):
            node_in[layer] = join(ref, 0, 2 * width)
            node_out[layer] = join(ref, 2 * width, width)
            edge_in[layer] = join(ref, 3 * width, 2 * width)
            edge_out[layer] = join(ref, 5 * width, width)
        decoder[...] = high[0, per : per + 1, :] * scale
        loss[...] = high[0, per + 1 : per + 2, :] / count

    first = lax.axis_index("sub") == 0
    pl.when(first)(lambda: write(mine, other))
    pl.when(jnp.logical_not(first))(lambda: write(other, mine))


def call(kernel, outs, *args):
    shapes = [jax.ShapeDtypeStruct(shape, dtype) for shape, dtype in outs]
    return pl.pallas_call(
        kernel,
        out_shape=shapes,
        in_specs=[VMEM] * len(args),
        out_specs=[VMEM] * len(shapes),
    )(*args)


def pairs(count, offset):
    found = []
    for low in range(offset, count - 1, 2):
        found += [(low, low + 1), (low + 1, low)]
    return found


def per_device(
    node_feats, edge_in, edge_out, node_in, node_out, decoder, edge_index, halo_index, target
):
    nodes, width = node_feats.shape
    edges = edge_index.shape[1]
    size = halo_index.shape[2]
    n_dom, n_sub = lax.axis_size("dom"), lax.axis_size("sub")
    count = nodes * n_dom * n_sub
    if edge_in.shape[0] != 2 or 4 * size != nodes:
        raise ValueError("unsupported sizes")
    chunk = 256
    routes = [("dom", 1), ("dom", 0), ("sub", 0), ("sub", 1)]
    order = [1, 0, 2, 3]
    links = [pairs(lax.axis_size(axis), offset) for axis, offset in routes]
    links = [links[1], links[0], links[2], links[3]]
    axes = ["dom", "dom", "sub", "sub"]
    names = tuple(1 if link else 0 for link in links)

    def exchange(blocks):
        came = [None] * 4
        for at in order:
            if links[at]:
                came[at] = lax.ppermute(blocks[at], axes[at], links[at])
        return [block for block in came if block is not None]

    node_shape = ((nodes, width), F32)
    edge_shape = ((edges, width), F32)
    block_shapes = [((size, width), F32)] * 4

    flat, recv, send, recv_t, send_t, h0, slope0, q0, *blocks = call(
        functools.partial(first_kernel, chunk),
        [
            ((nodes, 128), F32),
            ((edges, nodes), BF16), ((edges, nodes), BF16),
            ((nodes, edges), BF16), ((nodes, edges), BF16),
            node_shape, edge_shape, node_shape, *block_shapes,
        ],
        node_feats, edge_index, halo_index, edge_in, edge_out,
    )
    agg0, h1, act0, gate0, slope1, q1, *blocks = call(
        functools.partial(middle_kernel, chunk, 0, names),
        [node_shape, node_shape, node_shape, node_shape, edge_shape, node_shape, *block_shapes],
        *blocks, *exchange(blocks),
        h0, recv, send, recv_t, node_in, node_out, edge_in, edge_out,
    )
    agg1, act1, pre1, top1, through, pred, tail, *blocks = call(
        functools.partial(last_kernel, 1, count, names),
        [node_shape, node_shape, node_shape, node_shape, node_shape,
         ((1, nodes), F32), ((EXTRA, width), F32), *block_shapes],
        *blocks, *exchange(blocks),
        h1, flat, target.reshape(1, nodes), decoder.reshape(1, width), node_in, node_out,
    )
    grads_shape = [((3 * width, width), F32)]
    came = exchange(blocks)
    (node_high,) = call(node_grads_kernel, grads_shape, h1, agg1, act1, pre1, top1)
    local1, to_recv1, to_send1, top0, pre0, *blocks = call(
        functools.partial(back_kernel, chunk, 1, names),
        [node_shape, node_shape, node_shape, node_shape, node_shape, *block_shapes],
        *blocks, *came,
        through, gate0, recv, recv_t, send_t, slope1, edge_in, edge_out, node_in, node_out,
    )
    came = exchange(blocks)
    (edge_high,) = call(edge_grads_kernel, grads_shape, h1, q1, local1, to_recv1, to_send1)
    (node_low,) = call(node_grads_kernel, grads_shape, h0, agg0, act0, pre0, top0)
    per = 6 * width // n_dom
    if n_sub != 2 or per % 8 or 6 * width % n_dom:
        return slow_tail(
            count, blocks, came, names, chunk, h0, q0, recv, recv_t, send_t, slope0, edge_out,
            node_low, node_high, edge_high, tail, pred, nodes,
        )
    packed = ((n_dom, per + EXTRA, width), F32)
    mine, other = call(
        functools.partial(end_kernel, chunk, names),
        [packed, packed],
        *blocks, *came,
        h0, q0, recv, recv_t, send_t, slope0, edge_out, node_low, node_high, edge_high, tail,
    )
    swap = pairs(n_sub, 0)
    (halved,) = call(add_kernel, [packed], mine, lax.ppermute(other, "sub", swap))
    parts = lax.all_to_all(halved, "dom", 0, 0, tiled=True)
    (spread,) = call(total_kernel, [packed], parts)
    mine = lax.all_to_all(spread, "dom", 0, 0, tiled=True)
    other = lax.ppermute(mine, "sub", swap)
    params = 2 * 6 * width * width + width
    loss, g_edge_in, g_edge_out, g_node_in, g_node_out, g_decoder = call(
        functools.partial(scale_kernel, params, count),
        [
            ((1, width), F32),
            ((2, 2 * width, width), F32), ((2, width, width), F32),
            ((2, 2 * width, width), F32), ((2, width, width), F32),
            ((1, width), F32),
        ],
        mine, other,
    )
    return (
        loss[0, 0], pred.reshape(nodes), g_edge_in, g_edge_out, g_node_in, g_node_out,
        g_decoder.reshape(width),
    )


def low_kernel(chunk, names, *refs):
    own, refs = refs[:4], refs[4:]
    came, refs = unpack(names, refs)
    h, q, recv, recv_t, send_t, slope, edge_out, out = refs
    local_grad = take_sum(own, came)
    to_recv, to_send = edge_backward(local_grad, edge_out[0], recv, recv_t, send_t, slope, chunk)
    width = h.shape[1]
    out[0:width, :] = tmm(h[...], to_recv)
    out[width : 2 * width, :] = tmm(h[...], to_send)
    out[2 * width :, :] = tmm(q[...], local_grad)


def slow_tail(
    count, blocks, came, names, chunk, h0, q0, recv, recv_t, send_t, slope0, edge_out,
    node_low, node_high, edge_high, tail, pred, nodes,
):
    width = h0.shape[1]
    (edge_low,) = call(
        functools.partial(low_kernel, chunk, names), [((3 * width, width), F32)],
        *blocks, *came, h0, q0, recv, recv_t, send_t, slope0, edge_out,
    )
    total = lax.psum(
        jnp.concatenate([node_low, edge_low, node_high, edge_high, tail], 0), ("dom", "sub")
    )
    rows = 12 * width
    body = total[: rows + 1]
    params = (rows + 1) * width
    scale = 1.0 / jnp.sqrt(jnp.sum(body * body) / params + 1e-06)
    grads = (total[:rows] * scale).reshape(2, 2, 3 * width, width)
    return (
        total[rows + 1, 0] / count, pred.reshape(nodes),
        grads[:, 1, : 2 * width], grads[:, 1, 2 * width :],
        grads[:, 0, : 2 * width], grads[:, 0, 2 * width :],
        total[rows] * scale,
    )


def solution(mesh):
    placed = (
        P(("dom", "sub"), None),
        P(),
        P(),
        P(),
        P(),
        P(),
        P(None, ("dom", "sub")),
        P(("dom", "sub"), None, None),
        P(("dom", "sub")),
    )
    return jax.shard_map(
        per_device,
        mesh=mesh,
        in_specs=placed,
        out_specs=(P(), P(("dom", "sub")), P(), P(), P(), P(), P()),
        check_vma=False,
    )
```

```python
import functools

import jax
import jax.numpy as jnp
from jax import lax
from jax.experimental import pallas as pl
from jax.experimental.pallas import tpu as pltpu
from jax.sharding import PartitionSpec as P

F32 = jnp.float32
BF16 = jnp.bfloat16
VMEM = pl.BlockSpec(memory_space=pltpu.VMEM)
EXTRA = 8


def halves(x):
    high = x.astype(BF16)
    low = (x - high.astype(F32)).astype(BF16)
    return high, low


def side(x):
    return jnp.concatenate(halves(x), axis=1)


def fold(x):
    width = x.shape[1] // 2
    return x[:, :width] + x[:, width:]


def dot(a, b, dims=((1,), (0,))):
    return lax.dot_general(a, b, (dims, ((), ())), preferred_element_type=F32)


def mm(x, w):
    wide = side(w)
    return fold(dot(side(x), jnp.concatenate([wide, wide], axis=0)))


def mmt(x, w):
    high, low = halves(w)
    both = jnp.concatenate(
        [jnp.concatenate([high, high], axis=1), jnp.concatenate([low, low], axis=1)], axis=0
    )
    return fold(dot(side(x), both, ((1,), (1,))))


def tmm(x, y):
    wide = fold(dot(side(x), side(y), ((0,), (0,))))
    width = x.shape[1]
    return wide[:width] + wide[width:]


def silu_parts(v):
    gate = 1.0 / (1.0 + jnp.exp(-v))
    return v * gate, gate * (1.0 + v * (1.0 - gate))


def row_of(column):
    n = column.shape[0]
    eye = lax.broadcasted_iota(jnp.int32, (n, n), 0) == lax.broadcasted_iota(jnp.int32, (n, n), 1)
    return jnp.sum(jnp.where(eye, column, 0.0), axis=0, keepdims=True)


def onehot(mask):
    return jnp.where(mask, 1.0, 0.0).astype(BF16)


def edge_forward(features, weight_in, recv, send, recv_t, slope_ref, chunk):
    width = features.shape[1]
    to_recv = side(mm(features, weight_in[:width]))
    to_send = side(mm(features, weight_in[width:]))
    total = None
    for start in range(0, recv.shape[0], chunk):
        rows = pl.ds(start, chunk)
        pre = fold(dot(recv[rows, :], to_recv) + dot(send[rows, :], to_send))
        act, slope = silu_parts(pre)
        slope_ref[rows, :] = slope
        part = dot(recv_t[:, rows], side(act))
        total = part if total is None else total + part
    return fold(total)


def edge_backward(local_grad, weight_out, recv, recv_t, send_t, slope_ref, chunk):
    spread = side(mmt(local_grad, weight_out))
    total_r = total_s = None
    for start in range(0, recv.shape[0], chunk):
        rows = pl.ds(start, chunk)
        grad = side(fold(dot(recv[rows, :], spread)) * slope_ref[rows, :])
        part_r = dot(recv_t[:, rows], grad)
        part_s = dot(send_t[:, rows], grad)
        total_r = part_r if total_r is None else total_r + part_r
        total_s = part_s if total_s is None else total_s + part_s
    return fold(total_r), fold(total_s)


def node_forward(features, summed, weight_in, weight_out):
    width = features.shape[1]
    pre = mm(features, weight_in[:width]) + mm(summed, weight_in[width:])
    act, slope = silu_parts(pre)
    return features + mm(act, weight_out), act, slope


def put_blocks(value, refs):
    size = refs[0].shape[0]
    for at, ref in enumerate(refs):
        ref[...] = value[at * size : (at + 1) * size]


def take_sum(own, came):
    parts = [
        ref[...] + came[at][...] if came[at] is not None else ref[...]
        for at, ref in enumerate(own)
    ]
    return jnp.concatenate(parts, axis=0)


def even(axis):
    return lax.rem(lax.axis_index(axis), 2) == 0


def first_kernel(
    chunk, feats, index, halo, weight_in, weight_out,
    flat_out, recv, send, recv_t, send_t, h_out, slope, q_out, *blocks
):
    nodes = feats.shape[0]
    edges = index.shape[1]
    lanes = 128
    count = edges // lanes
    size = halo.shape[2]
    pieces = [index[0:1, pl.ds(b * lanes, lanes)] for b in range(count)]
    pieces += [index[1:2, pl.ds(b * lanes, lanes)] for b in range(count)]
    table = jnp.concatenate(pieces, axis=0).astype(F32)
    lists = jnp.concatenate([halo[0].astype(F32), jnp.zeros((4, lanes - size), F32)], axis=1)
    rest = jnp.zeros((lanes - 2 * count - 4, lanes), F32)
    columns = jnp.concatenate([table, lists, rest], axis=0).T
    by_dir = [columns[:size, 2 * count + k : 2 * count + k + 1] for k in range(4)]
    dom_even, sub_even = even("dom"), even("sub")
    flat = jnp.concatenate(
        [
            jnp.where(dom_even, by_dir[1], by_dir[0]),
            jnp.where(dom_even, by_dir[0], by_dir[1]),
            jnp.where(sub_even, by_dir[3], by_dir[2]),
            jnp.where(sub_even, by_dir[2], by_dir[3]),
        ],
        axis=0,
    )
    flat_row = row_of(flat)
    flat_out[...] = jnp.broadcast_to(flat, flat_out.shape)
    for b in range(count):
        rows = pl.ds(b * lanes, lanes)
        recv[rows, :] = onehot(columns[:, b : b + 1] == flat_row)
        send[rows, :] = onehot(columns[:, count + b : count + b + 1] == flat_row)
        recv_t[:, rows] = onehot(flat == table[b : b + 1])
        send_t[:, rows] = onehot(flat == table[count + b : count + b + 1])
    place = onehot(flat == lax.broadcasted_iota(jnp.int32, (nodes, nodes), 1).astype(F32))
    features = fold(dot(place, side(feats[...])))
    h_out[...] = features
    q = edge_forward(features, weight_in[0], recv, send, recv_t, slope, chunk)
    q_out[...] = q
    put_blocks(mm(q, weight_out[0]), blocks)


def middle_kernel(
    chunk, layer, names, *refs
):
    own, refs = refs[:4], refs[4:]
    came, refs = unpack(names, refs)
    (h, recv, send, recv_t, node_in, node_out, edge_in, edge_out,
     agg_out, h_out, node_act, node_slope, slope, q_out, *blocks) = refs
    summed = take_sum(own, came)
    agg_out[...] = summed
    features, act, gate = node_forward(h[...], summed, node_in[layer], node_out[layer])
    h_out[...] = features
    node_act[...] = act
    node_slope[...] = gate
    q = edge_forward(features, edge_in[layer + 1], recv, send, recv_t, slope, chunk)
    q_out[...] = q
    put_blocks(mm(q, edge_out[layer + 1]), blocks)


def unpack(names, refs):
    came = []
    at = 0
    for there in names:
        came.append(refs[at] if there else None)
        at += there
    return came, refs[at:]


def last_kernel(
    layer, count, names, *refs
):
    own, refs = refs[:4], refs[4:]
    came, refs = unpack(names, refs)
    (h, flat_ref, target, decoder, node_in, node_out,
     agg_out, node_act, pre_grad_out, top_grad_out, through_out, pred_out, tail_out, *blocks) = refs
    nodes, width = h.shape
    summed = take_sum(own, came)
    agg_out[...] = summed
    features, act, gate = node_forward(h[...], summed, node_in[layer], node_out[layer])
    node_act[...] = act
    weights = decoder[...]
    predicted = jnp.sum(features * weights, axis=1, keepdims=True)
    flat = flat_ref[:, 0:1]
    here = flat == lax.broadcasted_iota(jnp.int32, (nodes, nodes), 1).astype(F32)
    pred_out[...] = jnp.sum(jnp.where(here, predicted, 0.0), axis=0, keepdims=True)
    wanted = jnp.sum(jnp.where(here, target[...], 0.0), axis=1, keepdims=True)
    misfit = predicted - wanted
    seed = 2.0 * misfit / count
    decoder_grad = jnp.sum(seed * features, axis=0, keepdims=True)
    loss = jnp.broadcast_to(jnp.sum(misfit * misfit, axis=0, keepdims=True), (1, width))
    tail_out[...] = jnp.concatenate([decoder_grad, loss, jnp.zeros((EXTRA - 2, width), F32)], 0)
    top = seed * weights
    top_grad_out[...] = top
    pre_grad = mmt(top, node_out[layer]) * gate
    pre_grad_out[...] = pre_grad
    through_out[...] = top + mmt(pre_grad, node_in[layer, :width])
    put_blocks(mmt(pre_grad, node_in[layer, width:]), blocks)


def node_grads_kernel(h, summed, act, pre_grad, top_grad, out):
    width = h.shape[1]
    out[0:width, :] = tmm(h[...], pre_grad[...])
    out[width : 2 * width, :] = tmm(summed[...], pre_grad[...])
    out[2 * width :, :] = tmm(act[...], top_grad[...])


def edge_grads_kernel(h, q, local_grad, to_recv, to_send, out):
    width = h.shape[1]
    out[0:width, :] = tmm(h[...], to_recv[...])
    out[width : 2 * width, :] = tmm(h[...], to_send[...])
    out[2 * width :, :] = tmm(q[...], local_grad[...])


def back_kernel(
    chunk, layer, names, *refs
):
    own, refs = refs[:4], refs[4:]
    came, refs = unpack(names, refs)
    (through, node_slope, recv, recv_t, send_t, slope, edge_in, edge_out, node_in, node_out,
     local_out, recv_out, send_out, top_out, pre_out, *blocks) = refs
    width = through.shape[1]
    local_grad = take_sum(own, came)
    local_out[...] = local_grad
    to_recv, to_send = edge_backward(
        local_grad, edge_out[layer], recv, recv_t, send_t, slope, chunk
    )
    recv_out[...] = to_recv
    send_out[...] = to_send
    top = (
        through[...]
        + mmt(to_recv, edge_in[layer, :width])
        + mmt(to_send, edge_in[layer, width:])
    )
    top_out[...] = top
    pre_grad = mmt(top, node_out[layer - 1]) * node_slope[...]
    pre_out[...] = pre_grad
    put_blocks(mmt(pre_grad, node_in[layer - 1, width:]), blocks)


def split_rows(value, ref, first):
    per = ref.shape[1] - EXTRA
    at = 0
    while at < value.shape[0]:
        group, inside = divmod(first + at, per)
        take = min(per - inside, value.shape[0] - at)
        ref[group, inside : inside + take, :] = value[at : at + take]
        at += take


def end_kernel(
    chunk, names, *refs
):
    own, refs = refs[:4], refs[4:]
    came, refs = unpack(names, refs)
    (h, q, recv, recv_t, send_t, slope, edge_out, node_low, node_high, edge_high, tail,
     mine, other) = refs
    local_grad = take_sum(own, came)
    to_recv, to_send = edge_backward(local_grad, edge_out[0], recv, recv_t, send_t, slope, chunk)
    low = [
        node_low[...],
        tmm(h[...], to_recv),
        tmm(h[...], to_send),
        tmm(q[...], local_grad),
    ]
    per = mine.shape[1] - EXTRA
    blank = jnp.zeros((mine.shape[0], EXTRA, mine.shape[2]), F32)

    def write(ref_high, ref_low):
        ref_high[:, per:, :] = blank
        ref_low[:, per:, :] = blank
        ref_high[0, per:, :] = tail[...]
        at = 0
        for value in low:
            split_rows(value, ref_low, at)
            at += value.shape[0]
        split_rows(node_high[...], ref_high, 0)
        split_rows(edge_high[...], ref_high, node_high.shape[0])

    first = lax.axis_index("sub") == 0
    pl.when(first)(lambda: write(mine, other))
    pl.when(jnp.logical_not(first))(lambda: write(other, mine))


def add_kernel(a, b, out):
    out[...] = a[...] + b[...]


def total_kernel(parts, out):
    total = jnp.sum(parts[...], axis=0)
    per = total.shape[0] - EXTRA
    body = total[: per + 1]
    squares = jnp.sum(jnp.sum(body * body, axis=0, keepdims=True), axis=1, keepdims=True)
    last = jnp.broadcast_to(squares, (1, total.shape[1]))
    total = jnp.concatenate([total[:-1], last], axis=0)
    out[...] = jnp.broadcast_to(total[None], out.shape)


def scale_kernel(
    params, count, mine, other, loss, edge_in, edge_out, node_in, node_out, decoder
):
    rows = mine.shape[1]
    per = rows - EXTRA
    width = mine.shape[2]
    squares = jnp.sum(
        mine[:, rows - 1 : rows, :] + other[:, rows - 1 : rows, :], axis=0
    )
    scale = 1.0 / jnp.sqrt(squares / params + 1e-06)

    def join(ref, first, size):
        parts = []
        at = 0
        while at < size:
            group, inside = divmod(first + at, per)
            take = min(per - inside, size - at)
            parts.append(ref[group, inside : inside + take, :])
            at += take
        return jnp.concatenate(parts, axis=0) * scale

    def write(high, low):
        for layer, ref in ((1, high), (0, low)):
            node_in[layer] = join(ref, 0, 2 * width)
            node_out[layer] = join(ref, 2 * width, width)
            edge_in[layer] = join(ref, 3 * width, 2 * width)
            edge_out[layer] = join(ref, 5 * width, width)
        decoder[...] = high[0, per : per + 1, :] * scale
        loss[...] = high[0, per + 1 : per + 2, :] / count

    first = lax.axis_index("sub") == 0
    pl.when(first)(lambda: write(mine, other))
    pl.when(jnp.logical_not(first))(lambda: write(other, mine))


def call(kernel, outs, *args):
    shapes = [jax.ShapeDtypeStruct(shape, dtype) for shape, dtype in outs]
    return pl.pallas_call(
        kernel,
        out_shape=shapes,
        in_specs=[VMEM] * len(args),
        out_specs=[VMEM] * len(shapes),
        compiler_params=pltpu.CompilerParams(vmem_limit_bytes=16 * 2**20),
    )(*args)


def pairs(count, offset):
    found = []
    for low in range(offset, count - 1, 2):
        found += [(low, low + 1), (low + 1, low)]
    return found


def per_device(
    node_feats, edge_in, edge_out, node_in, node_out, decoder, edge_index, halo_index, target
):
    nodes, width = node_feats.shape
    edges = edge_index.shape[1]
    size = halo_index.shape[2]
    n_dom, n_sub = lax.axis_size("dom"), lax.axis_size("sub")
    count = nodes * n_dom * n_sub
    if edge_in.shape[0] != 2 or 4 * size != nodes:
        raise ValueError("unsupported sizes")
    chunk = 256
    routes = [("dom", 1), ("dom", 0), ("sub", 0), ("sub", 1)]
    order = [1, 0, 2, 3]
    links = [pairs(lax.axis_size(axis), offset) for axis, offset in routes]
    links = [links[1], links[0], links[2], links[3]]
    axes = ["dom", "dom", "sub", "sub"]
    names = tuple(1 if link else 0 for link in links)

    def exchange(blocks):
        came = [None] * 4
        for at in order:
            if links[at]:
                came[at] = lax.ppermute(blocks[at], axes[at], links[at])
        return [block for block in came if block is not None]

    node_shape = ((nodes, width), F32)
    edge_shape = ((edges, width), F32)
    block_shapes = [((size, width), F32)] * 4

    flat, recv, send, recv_t, send_t, h0, slope0, q0, *blocks = call(
        functools.partial(first_kernel, chunk),
        [
            ((nodes, 128), F32),
            ((edges, nodes), BF16), ((edges, nodes), BF16),
            ((nodes, edges), BF16), ((nodes, edges), BF16),
            node_shape, edge_shape, node_shape, *block_shapes,
        ],
        node_feats, edge_index, halo_index, edge_in, edge_out,
    )
    agg0, h1, act0, gate0, slope1, q1, *blocks = call(
        functools.partial(middle_kernel, chunk, 0, names),
        [node_shape, node_shape, node_shape, node_shape, edge_shape, node_shape, *block_shapes],
        *blocks, *exchange(blocks),
        h0, recv, send, recv_t, node_in, node_out, edge_in, edge_out,
    )
    agg1, act1, pre1, top1, through, pred, tail, *blocks = call(
        functools.partial(last_kernel, 1, count, names),
        [node_shape, node_shape, node_shape, node_shape, node_shape,
         ((1, nodes), F32), ((EXTRA, width), F32), *block_shapes],
        *blocks, *exchange(blocks),
        h1, flat, target.reshape(1, nodes), decoder.reshape(1, width), node_in, node_out,
    )
    grads_shape = [((3 * width, width), F32)]
    came = exchange(blocks)
    (node_high,) = call(node_grads_kernel, grads_shape, h1, agg1, act1, pre1, top1)
    local1, to_recv1, to_send1, top0, pre0, *blocks = call(
        functools.partial(back_kernel, chunk, 1, names),
        [node_shape, node_shape, node_shape, node_shape, node_shape, *block_shapes],
        *blocks, *came,
        through, gate0, recv, recv_t, send_t, slope1, edge_in, edge_out, node_in, node_out,
    )
    came = exchange(blocks)
    (edge_high,) = call(edge_grads_kernel, grads_shape, h1, q1, local1, to_recv1, to_send1)
    (node_low,) = call(node_grads_kernel, grads_shape, h0, agg0, act0, pre0, top0)
    per = 6 * width // n_dom
    if n_sub != 2 or per % 8 or 6 * width % n_dom:
        return slow_tail(
            count, blocks, came, names, chunk, h0, q0, recv, recv_t, send_t, slope0, edge_out,
            node_low, node_high, edge_high, tail, pred, nodes,
        )
    packed = ((n_dom, per + EXTRA, width), F32)
    mine, other = call(
        functools.partial(end_kernel, chunk, names),
        [packed, packed],
        *blocks, *came,
        h0, q0, recv, recv_t, send_t, slope0, edge_out, node_low, node_high, edge_high, tail,
    )
    swap = pairs(n_sub, 0)
    (halved,) = call(add_kernel, [packed], mine, lax.ppermute(other, "sub", swap))
    parts = lax.all_to_all(halved, "dom", 0, 0, tiled=True)
    (spread,) = call(total_kernel, [packed], parts)
    mine = lax.all_to_all(spread, "dom", 0, 0, tiled=True)
    other = lax.ppermute(mine, "sub", swap)
    params = 2 * 6 * width * width + width
    loss, g_edge_in, g_edge_out, g_node_in, g_node_out, g_decoder = call(
        functools.partial(scale_kernel, params, count),
        [
            ((1, width), F32),
            ((2, 2 * width, width), F32), ((2, width, width), F32),
            ((2, 2 * width, width), F32), ((2, width, width), F32),
            ((1, width), F32),
        ],
        mine, other,
    )
    return (
        loss[0, 0], pred.reshape(nodes), g_edge_in, g_edge_out, g_node_in, g_node_out,
        g_decoder.reshape(width),
    )


def low_kernel(chunk, names, *refs):
    own, refs = refs[:4], refs[4:]
    came, refs = unpack(names, refs)
    h, q, recv, recv_t, send_t, slope, edge_out, out = refs
    local_grad = take_sum(own, came)
    to_recv, to_send = edge_backward(local_grad, edge_out[0], recv, recv_t, send_t, slope, chunk)
    width = h.shape[1]
    out[0:width, :] = tmm(h[...], to_recv)
    out[width : 2 * width, :] = tmm(h[...], to_send)
    out[2 * width :, :] = tmm(q[...], local_grad)


def slow_tail(
    count, blocks, came, names, chunk, h0, q0, recv, recv_t, send_t, slope0, edge_out,
    node_low, node_high, edge_high, tail, pred, nodes,
):
    width = h0.shape[1]
    (edge_low,) = call(
        functools.partial(low_kernel, chunk, names), [((3 * width, width), F32)],
        *blocks, *came, h0, q0, recv, recv_t, send_t, slope0, edge_out,
    )
    total = lax.psum(
        jnp.concatenate([node_low, edge_low, node_high, edge_high, tail], 0), ("dom", "sub")
    )
    rows = 12 * width
    body = total[: rows + 1]
    params = (rows + 1) * width
    scale = 1.0 / jnp.sqrt(jnp.sum(body * body) / params + 1e-06)
    grads = (total[:rows] * scale).reshape(2, 2, 3 * width, width)
    return (
        total[rows + 1, 0] / count, pred.reshape(nodes),
        grads[:, 1, : 2 * width], grads[:, 1, 2 * width :],
        grads[:, 0, : 2 * width], grads[:, 0, 2 * width :],
        total[rows] * scale,
    )


def solution(mesh):
    placed = (
        P(("dom", "sub"), None),
        P(),
        P(),
        P(),
        P(),
        P(),
        P(None, ("dom", "sub")),
        P(("dom", "sub"), None, None),
        P(("dom", "sub")),
    )
    return jax.shard_map(
        per_device,
        mesh=mesh,
        in_specs=placed,
        out_specs=(P(), P(("dom", "sub")), P(), P(), P(), P(), P()),
        check_vma=False,
    )
```

```python
import functools

import jax
import jax.numpy as jnp
from jax import lax
from jax.experimental import pallas as pl
from jax.experimental.pallas import tpu as pltpu
from jax.sharding import PartitionSpec as P

F32 = jnp.float32
BF16 = jnp.bfloat16
VMEM = pl.BlockSpec(memory_space=pltpu.VMEM)
EXTRA = 8


def halves(x):
    high = x.astype(BF16)
    low = (x - high.astype(F32)).astype(BF16)
    return high, low


def side(x):
    return jnp.concatenate(halves(x), axis=1)


def fold(x):
    width = x.shape[1] // 2
    return x[:, :width] + x[:, width:]


def dot(a, b, dims=((1,), (0,))):
    return lax.dot_general(a, b, (dims, ((), ())), preferred_element_type=F32)


def mm(x, w):
    wide = side(w)
    return fold(dot(side(x), jnp.concatenate([wide, wide], axis=0)))


def mmt(x, w):
    high, low = halves(w)
    both = jnp.concatenate(
        [jnp.concatenate([high, high], axis=1), jnp.concatenate([low, low], axis=1)], axis=0
    )
    return fold(dot(side(x), both, ((1,), (1,))))


def tmm(x, y):
    wide = fold(dot(side(x), side(y), ((0,), (0,))))
    width = x.shape[1]
    return wide[:width] + wide[width:]


def silu_parts(v):
    gate = 1.0 / (1.0 + jnp.exp(-v))
    return v * gate, gate * (1.0 + v * (1.0 - gate))


def row_of(column):
    n = column.shape[0]
    eye = lax.broadcasted_iota(jnp.int32, (n, n), 0) == lax.broadcasted_iota(jnp.int32, (n, n), 1)
    return jnp.sum(jnp.where(eye, column, 0.0), axis=0, keepdims=True)


def onehot(mask):
    return jnp.where(mask, 1.0, 0.0).astype(BF16)


def edge_forward(features, weight_in, recv, send, recv_t, slope_ref, chunk):
    width = features.shape[1]
    to_recv = side(mm(features, weight_in[:width]))
    to_send = side(mm(features, weight_in[width:]))
    total = None
    for start in range(0, recv.shape[0], chunk):
        rows = pl.ds(start, chunk)
        pre = fold(dot(recv[rows, :], to_recv) + dot(send[rows, :], to_send))
        act, slope = silu_parts(pre)
        slope_ref[rows, :] = slope
        part = dot(recv_t[:, rows], side(act))
        total = part if total is None else total + part
    return fold(total)


def edge_backward(local_grad, weight_out, recv, recv_t, send_t, slope_ref, chunk):
    spread = side(mmt(local_grad, weight_out))
    total_r = total_s = None
    for start in range(0, recv.shape[0], chunk):
        rows = pl.ds(start, chunk)
        grad = side(fold(dot(recv[rows, :], spread)) * slope_ref[rows, :])
        part_r = dot(recv_t[:, rows], grad)
        part_s = dot(send_t[:, rows], grad)
        total_r = part_r if total_r is None else total_r + part_r
        total_s = part_s if total_s is None else total_s + part_s
    return fold(total_r), fold(total_s)


def node_forward(features, summed, weight_in, weight_out):
    width = features.shape[1]
    pre = mm(features, weight_in[:width]) + mm(summed, weight_in[width:])
    act, slope = silu_parts(pre)
    return features + mm(act, weight_out), act, slope


def put_blocks(value, refs):
    size = refs[0].shape[0]
    for at, ref in enumerate(refs):
        ref[...] = value[at * size : (at + 1) * size]


def take_sum(own, came):
    parts = [
        ref[...] + came[at][...] if came[at] is not None else ref[...]
        for at, ref in enumerate(own)
    ]
    return jnp.concatenate(parts, axis=0)


def even(axis):
    return lax.rem(lax.axis_index(axis), 2) == 0


def first_kernel(
    chunk, feats_hbm, index_hbm, halo_hbm, target_hbm, decoder_hbm, *refs
):
    weights_hbm, refs = refs[:4], refs[4:]
    (target, decoder, edge_in, edge_out, node_in, node_out,
     flat_out, recv, send, recv_t, send_t, h_out, slope, q_out) = refs[:14]
    blocks, (feats, index, halo, sems) = refs[14:18], refs[18:]
    copies = [
        pltpu.make_async_copy(source, place, sems.at[at])
        for at, (source, place) in enumerate(
            zip(
                (index_hbm, halo_hbm, feats_hbm, *weights_hbm, target_hbm, decoder_hbm),
                (index, halo, feats, edge_in, edge_out, node_in, node_out, target, decoder),
            )
        )
    ]
    for copy in copies:
        copy.start()
    copies[0].wait()
    copies[1].wait()
    nodes = feats.shape[0]
    edges = index.shape[1]
    lanes = 128
    count = edges // lanes
    size = halo.shape[2]
    pieces = [index[0:1, pl.ds(b * lanes, lanes)] for b in range(count)]
    pieces += [index[1:2, pl.ds(b * lanes, lanes)] for b in range(count)]
    table = jnp.concatenate(pieces, axis=0).astype(F32)
    lists = jnp.concatenate([halo[0].astype(F32), jnp.zeros((4, lanes - size), F32)], axis=1)
    rest = jnp.zeros((lanes - 2 * count - 4, lanes), F32)
    columns = jnp.concatenate([table, lists, rest], axis=0).T
    by_dir = [columns[:size, 2 * count + k : 2 * count + k + 1] for k in range(4)]
    dom_even, sub_even = even("dom"), even("sub")
    flat = jnp.concatenate(
        [
            jnp.where(dom_even, by_dir[1], by_dir[0]),
            jnp.where(dom_even, by_dir[0], by_dir[1]),
            jnp.where(sub_even, by_dir[3], by_dir[2]),
            jnp.where(sub_even, by_dir[2], by_dir[3]),
        ],
        axis=0,
    )
    flat_row = row_of(flat)
    flat_out[...] = jnp.broadcast_to(flat, flat_out.shape)
    for b in range(count):
        rows = pl.ds(b * lanes, lanes)
        recv[rows, :] = onehot(columns[:, b : b + 1] == flat_row)
        send[rows, :] = onehot(columns[:, count + b : count + b + 1] == flat_row)
        recv_t[:, rows] = onehot(flat == table[b : b + 1])
        send_t[:, rows] = onehot(flat == table[count + b : count + b + 1])
    place = onehot(flat == lax.broadcasted_iota(jnp.int32, (nodes, nodes), 1).astype(F32))
    copies[2].wait()
    features = fold(dot(place, side(feats[...])))
    h_out[...] = features
    copies[3].wait()
    q = edge_forward(features, edge_in[0], recv, send, recv_t, slope, chunk)
    q_out[...] = q
    copies[4].wait()
    put_blocks(mm(q, edge_out[0]), blocks)
    for copy in copies[5:]:
        copy.wait()


def unpack(names, refs):
    came = []
    at = 0
    for there in names:
        came.append(refs[at] if there else None)
        at += there
    return came, refs[at:]


def middle_kernel(chunk, names, *refs):
    own, refs = refs[:4], refs[4:]
    came, refs = unpack(names, refs)
    (h, flat_ref, target, decoder, recv, send, recv_t, node_in, node_out, edge_in, edge_out,
     agg_out, h_out, node_act, node_slope, slope, q_out, pre_out, known_out, *messages) = refs
    nodes, width = h.shape
    summed = take_sum(own, came)
    agg_out[...] = summed
    features, act, gate = node_forward(h[...], summed, node_in[0], node_out[0])
    h_out[...] = features
    node_act[...] = act
    node_slope[...] = gate
    pre = mm(features, node_in[1, :width])
    pre_out[...] = pre
    base = jnp.sum(features * decoder[...], axis=1, keepdims=True)
    here = flat_ref[:, 0:1] == lax.broadcasted_iota(jnp.int32, (nodes, nodes), 1).astype(F32)
    wanted = jnp.sum(jnp.where(here, target[...], 0.0), axis=1, keepdims=True)
    first = lax.broadcasted_iota(jnp.int32, (nodes, width), 1) == 0
    known_out[...] = jnp.where(first, base, wanted)
    size = own[0].shape[0]
    short = base - wanted
    for at, message in enumerate(messages):
        rows = slice(at * size, (at + 1) * size)
        message[size : 2 * size, :] = pre[rows]
        line = row_of(short[rows])
        line = jnp.concatenate([line, jnp.zeros((1, width - size), F32)], axis=1)
        message[2 * size :, :] = jnp.concatenate(
            [line, jnp.ones((1, width), F32), jnp.zeros((EXTRA - 2, width), F32)], axis=0
        )
    q = edge_forward(features, edge_in[1], recv, send, recv_t, slope, chunk)
    q_out[...] = q
    local = mm(q, edge_out[1])
    for at, message in enumerate(messages):
        message[:size, :] = local[at * size : (at + 1) * size]


def column_of(row):
    n = row.shape[1]
    eye = lax.broadcasted_iota(jnp.int32, (n, n), 0) == lax.broadcasted_iota(jnp.int32, (n, n), 1)
    return jnp.sum(jnp.where(eye, row, 0.0), axis=1, keepdims=True)


def row_product(row, weight):
    return mm(jnp.broadcast_to(row, (8, row.shape[1])), weight)[0:1]


def back_kernel(chunk, count, names, *refs):
    own, refs = refs[:4], refs[4:]
    came, refs = unpack(names, refs)
    (flat_ref, decoder, pre_ref, known, node_slope, recv, recv_t, send_t, slope,
     edge_in, edge_out, node_in, node_out,
     agg_out, act_out, pre1_out, seed_out, local_out, recv_out, send_out, top_out, pre0_out,
     pred_out, loss_out, *blocks) = refs
    nodes, width = pre_ref.shape
    size = blocks[0].shape[0]
    summed = jnp.concatenate(
        [
            ref[:size, :] + came[at][:size, :] if came[at] is not None else ref[:size, :]
            for at, ref in enumerate(own)
        ],
        axis=0,
    )
    agg_out[...] = summed
    pre_agg = mm(summed, node_in[1, width:])
    act, gate = silu_parts(pre_ref[...] + pre_agg)
    act_out[...] = act
    weights = decoder[...]
    lead = row_of(jnp.sum(node_out[1] * weights, axis=1, keepdims=True))
    base, wanted = known[:, 0:1], known[:, 1:2]
    predicted = base + jnp.sum(act * lead, axis=1, keepdims=True)
    misfit = predicted - wanted
    seed = 2.0 * misfit / count
    seed_out[...] = jnp.broadcast_to(seed, seed_out.shape)
    here = flat_ref[:, 0:1] == lax.broadcasted_iota(jnp.int32, (nodes, nodes), 1).astype(F32)
    pred_out[...] = jnp.sum(jnp.where(here, predicted, 0.0), axis=0, keepdims=True)
    loss_out[...] = jnp.broadcast_to(
        jnp.sum(misfit * misfit, axis=0, keepdims=True), loss_out.shape
    )
    pre_grad = seed * lead * gate
    pre1_out[...] = pre_grad
    shared = []
    for at in range(4):
        rows = slice(at * size, (at + 1) * size)
        if came[at] is None:
            shared.append(pre_grad[rows])
            continue
        far_act, far_gate = silu_parts(came[at][size : 2 * size, :] + pre_agg[rows])
        far_misfit = column_of(came[at][2 * size : 2 * size + 1, :size])
        far_misfit = far_misfit + jnp.sum(far_act * lead, axis=1, keepdims=True)
        there = came[at][2 * size + 1 : 2 * size + 2, 0:1]
        far_seed = 2.0 * far_misfit / count * there
        shared.append(pre_grad[rows] + far_seed * lead * far_gate)
    local_grad = mmt(jnp.concatenate(shared, axis=0), node_in[1, width:])
    local_out[...] = local_grad
    to_recv, to_send = edge_backward(local_grad, edge_out[1], recv, recv_t, send_t, slope, chunk)
    recv_out[...] = to_recv
    send_out[...] = to_send
    top = (
        seed * weights
        + mmt(pre_grad, node_in[1, :width])
        + mmt(to_recv, edge_in[1, :width])
        + mmt(to_send, edge_in[1, width:])
    )
    top_out[...] = top
    pre0 = mmt(top, node_out[0]) * node_slope[...]
    pre0_out[...] = pre0
    put_blocks(mmt(pre0, node_in[0, width:]), blocks)


def grads_kernel(
    h0, agg0, act0, pre0, top0, h1, agg1, act1, pre1, seed, q1, local1, to_recv1, to_send1,
    decoder, node_out, loss, high, low, tail
):
    width = h0.shape[1]
    rows = seed[...]
    top1 = rows * decoder[...]
    act = act1[...]
    parts = [
        tmm(h1[...], pre1[...]),
        tmm(agg1[...], pre1[...]),
        tmm(act, top1),
        tmm(h1[...], to_recv1[...]),
        tmm(h1[...], to_send1[...]),
        tmm(q1[...], local1[...]),
    ]
    for at, part in enumerate(parts):
        high[at * width : (at + 1) * width, :] = part
    low[0:width, :] = tmm(h0[...], pre0[...])
    low[width : 2 * width, :] = tmm(agg0[...], pre0[...])
    low[2 * width :, :] = tmm(act0[...], top0[...])
    line = jnp.sum(rows * h1[...], axis=0, keepdims=True)
    line = line + row_product(jnp.sum(rows * act, axis=0, keepdims=True), node_out[1])
    tail[...] = jnp.concatenate([line, loss[...], jnp.zeros((EXTRA - 2, width), F32)], axis=0)


def split_rows(value, ref, first):
    per = ref.shape[1]
    at = 0
    while at < value.shape[0]:
        group, inside = divmod(first + at, per)
        take = min(per - inside, value.shape[0] - at)
        ref[group, inside : inside + take, :] = value[at : at + take]
        at += take


def end_kernel(chunk, names, *refs):
    own, refs = refs[:4], refs[4:]
    came, refs = unpack(names, refs)
    h, q, recv, recv_t, send_t, slope, edge_out, node_low, high, mine, other = refs
    local_grad = take_sum(own, came)
    to_recv, to_send = edge_backward(local_grad, edge_out[0], recv, recv_t, send_t, slope, chunk)
    low = [
        node_low[...],
        tmm(h[...], to_recv),
        tmm(h[...], to_send),
        tmm(q[...], local_grad),
    ]

    def write(ref_high, ref_low):
        at = 0
        for value in low:
            split_rows(value, ref_low, at)
            at += value.shape[0]
        split_rows(high[...], ref_high, 0)

    first = lax.axis_index("sub") == 0
    pl.when(first)(lambda: write(mine, other))
    pl.when(jnp.logical_not(first))(lambda: write(other, mine))


def add_kernel(a, b, out):
    out[...] = a[...] + b[...]


def total_kernel(parts, tail, out):
    total = jnp.sum(parts[...], axis=0)
    squares = jnp.sum(jnp.sum(total * total, axis=0, keepdims=True), axis=1, keepdims=True)
    last = jnp.broadcast_to(squares, (1, total.shape[1]))
    total = jnp.concatenate([total, tail[: EXTRA - 1, :], last], axis=0)
    out[...] = jnp.broadcast_to(total[None], out.shape)


def scale_kernel(
    params, count, mine, other, loss, edge_in, edge_out, node_in, node_out, decoder
):
    rows = mine.shape[1]
    per = rows - EXTRA
    width = mine.shape[2]
    extra = jnp.sum(mine[:, per:, :] + other[:, per:, :], axis=0)
    line = extra[0:1]
    squares = extra[EXTRA - 1 : EXTRA] + jnp.sum(line * line, axis=1, keepdims=True)
    scale = 1.0 / jnp.sqrt(squares / params + 1e-06)

    def join(ref, first, size):
        parts = []
        at = 0
        while at < size:
            group, inside = divmod(first + at, per)
            take = min(per - inside, size - at)
            parts.append(ref[group, inside : inside + take, :])
            at += take
        return jnp.concatenate(parts, axis=0) * scale

    def write(high, low):
        for layer, ref in ((1, high), (0, low)):
            node_in[layer] = join(ref, 0, 2 * width)
            node_out[layer] = join(ref, 2 * width, width)
            edge_in[layer] = join(ref, 3 * width, 2 * width)
            edge_out[layer] = join(ref, 5 * width, width)

    decoder[...] = line * scale
    loss[...] = extra[1:2] / count
    first = lax.axis_index("sub") == 0
    pl.when(first)(lambda: write(mine, other))
    pl.when(jnp.logical_not(first))(lambda: write(other, mine))


def call(kernel, outs, *args):
    shapes = [jax.ShapeDtypeStruct(shape, dtype) for shape, dtype in outs]
    return pl.pallas_call(
        kernel,
        out_shape=shapes,
        in_specs=[VMEM] * len(args),
        out_specs=[VMEM] * len(shapes),
        compiler_params=pltpu.CompilerParams(vmem_limit_bytes=16 * 2**20),
    )(*args)


def pairs(count, offset):
    found = []
    for low in range(offset, count - 1, 2):
        found += [(low, low + 1), (low + 1, low)]
    return found


def per_device(
    node_feats, edge_in, edge_out, node_in, node_out, decoder, edge_index, halo_index, target
):
    nodes, width = node_feats.shape
    edges = edge_index.shape[1]
    size = halo_index.shape[2]
    n_dom, n_sub = lax.axis_size("dom"), lax.axis_size("sub")
    count = nodes * n_dom * n_sub
    if edge_in.shape[0] != 2 or 4 * size != nodes:
        raise ValueError("unsupported sizes")
    chunk = 256
    routes = [("dom", 1), ("dom", 0), ("sub", 0), ("sub", 1)]
    order = [1, 0, 2, 3]
    links = [pairs(lax.axis_size(axis), offset) for axis, offset in routes]
    links = [links[1], links[0], links[2], links[3]]
    axes = ["dom", "dom", "sub", "sub"]
    names = tuple(1 if link else 0 for link in links)

    def exchange(blocks):
        came = [None] * 4
        for at in order:
            if links[at]:
                came[at] = lax.ppermute(blocks[at], axes[at], links[at])
        return [block for block in came if block is not None]

    node_shape = ((nodes, width), F32)
    edge_shape = ((edges, width), F32)
    block_shapes = [((size, width), F32)] * 4

    weights = (edge_in, edge_out, node_in, node_out)
    sources = (
        node_feats, edge_index, halo_index, target.reshape(1, nodes), decoder.reshape(1, width),
        *weights,
    )
    shapes = [
        ((1, nodes), F32), ((1, width), F32), *[(weight.shape, F32) for weight in weights],
        ((nodes, 128), F32),
        ((edges, nodes), BF16), ((edges, nodes), BF16),
        ((nodes, edges), BF16), ((nodes, edges), BF16),
        node_shape, edge_shape, node_shape, *block_shapes,
    ]
    (wanted, readout, edge_in, edge_out, node_in, node_out,
     flat, recv, send, recv_t, send_t, h0, slope0, q0, *blocks) = pl.pallas_call(
        functools.partial(first_kernel, chunk),
        out_shape=[jax.ShapeDtypeStruct(shape, dtype) for shape, dtype in shapes],
        in_specs=[pl.BlockSpec(memory_space=pltpu.HBM)] * len(sources),
        out_specs=[VMEM] * len(shapes),
        scratch_shapes=[
            pltpu.VMEM(node_feats.shape, F32),
            pltpu.VMEM(edge_index.shape, jnp.int32),
            pltpu.VMEM(halo_index.shape, jnp.int32),
            pltpu.SemaphoreType.DMA((len(sources),)),
        ],
        compiler_params=pltpu.CompilerParams(vmem_limit_bytes=16 * 2**20),
    )(*[pltpu.with_memory_space_constraint(source, pltpu.HBM) for source in sources])
    message = ((2 * size + EXTRA, width), F32)
    agg0, h1, act0, gate0, slope1, q1, pre, known, *messages = call(
        functools.partial(middle_kernel, chunk, names),
        [node_shape, node_shape, node_shape, node_shape, edge_shape, node_shape,
         node_shape, node_shape, *[message] * 4],
        *blocks, *exchange(blocks),
        h0, flat, wanted, readout, recv, send, recv_t, node_in, node_out, edge_in, edge_out,
    )
    (agg1, act1, pre1, seed, local1, to_recv1, to_send1, top0, pre0, pred, loss,
     *blocks) = call(
        functools.partial(back_kernel, chunk, count, names),
        [*[node_shape] * 9, ((1, nodes), F32), ((1, width), F32), *block_shapes],
        *messages, *exchange(messages),
        flat, readout, pre, known, gate0, recv, recv_t, send_t, slope1,
        edge_in, edge_out, node_in, node_out,
    )
    came = exchange(blocks)
    high, node_low, tail = call(
        grads_kernel,
        [((6 * width, width), F32), ((3 * width, width), F32), ((EXTRA, width), F32)],
        h0, agg0, act0, pre0, top0, h1, agg1, act1, pre1, seed, q1, local1, to_recv1, to_send1,
        readout, node_out, loss,
    )
    per = 6 * width // n_dom
    if n_sub != 2 or per % 8 or 6 * width % n_dom:
        return slow_tail(
            count, blocks, came, names, chunk, h0, q0, recv, recv_t, send_t, slope0, edge_out,
            node_low, high, tail, pred, nodes,
        )
    halved = ((n_dom, per, width), F32)
    packed = ((n_dom, per + EXTRA, width), F32)
    mine, other = call(
        functools.partial(end_kernel, chunk, names),
        [halved, halved],
        *blocks, *came, h0, q0, recv, recv_t, send_t, slope0, edge_out, node_low, high,
    )
    swap = pairs(n_sub, 0)
    (both,) = call(add_kernel, [halved], mine, lax.ppermute(other, "sub", swap))
    parts = lax.all_to_all(both, "dom", 0, 0, tiled=True)
    (spread,) = call(total_kernel, [packed], parts, tail)
    mine = lax.all_to_all(spread, "dom", 0, 0, tiled=True)
    other = lax.ppermute(mine, "sub", swap)
    params = 2 * 6 * width * width + width
    loss, g_edge_in, g_edge_out, g_node_in, g_node_out, g_decoder = call(
        functools.partial(scale_kernel, params, count),
        [
            ((1, width), F32),
            ((2, 2 * width, width), F32), ((2, width, width), F32),
            ((2, 2 * width, width), F32), ((2, width, width), F32),
            ((1, width), F32),
        ],
        mine, other,
    )
    return (
        loss[0, 0], pred.reshape(nodes), g_edge_in, g_edge_out, g_node_in, g_node_out,
        g_decoder.reshape(width),
    )


def low_kernel(chunk, names, *refs):
    own, refs = refs[:4], refs[4:]
    came, refs = unpack(names, refs)
    h, q, recv, recv_t, send_t, slope, edge_out, out = refs
    local_grad = take_sum(own, came)
    to_recv, to_send = edge_backward(local_grad, edge_out[0], recv, recv_t, send_t, slope, chunk)
    width = h.shape[1]
    out[0:width, :] = tmm(h[...], to_recv)
    out[width : 2 * width, :] = tmm(h[...], to_send)
    out[2 * width :, :] = tmm(q[...], local_grad)


def slow_tail(
    count, blocks, came, names, chunk, h0, q0, recv, recv_t, send_t, slope0, edge_out,
    node_low, high, tail, pred, nodes,
):
    width = h0.shape[1]
    (edge_low,) = call(
        functools.partial(low_kernel, chunk, names), [((3 * width, width), F32)],
        *blocks, *came, h0, q0, recv, recv_t, send_t, slope0, edge_out,
    )
    total = lax.psum(
        jnp.concatenate([node_low, edge_low, high, tail], 0), ("dom", "sub")
    )
    rows = 12 * width
    body = total[: rows + 1]
    params = (rows + 1) * width
    scale = 1.0 / jnp.sqrt(jnp.sum(body * body) / params + 1e-06)
    grads = (total[:rows] * scale).reshape(2, 2, 3 * width, width)
    return (
        total[rows + 1, 0] / count, pred.reshape(nodes),
        grads[:, 1, : 2 * width], grads[:, 1, 2 * width :],
        grads[:, 0, : 2 * width], grads[:, 0, 2 * width :],
        total[rows] * scale,
    )


def solution(mesh):
    placed = (
        P(("dom", "sub"), None),
        P(),
        P(),
        P(),
        P(),
        P(),
        P(None, ("dom", "sub")),
        P(("dom", "sub"), None, None),
        P(("dom", "sub")),
    )
    return jax.shard_map(
        per_device,
        mesh=mesh,
        in_specs=placed,
        out_specs=(P(), P(("dom", "sub")), P(), P(), P(), P(), P()),
        check_vma=False,
    )
```

```python
import functools

import jax
import jax.numpy as jnp
from jax import lax
from jax.experimental import pallas as pl
from jax.experimental.pallas import tpu as pltpu
from jax.sharding import PartitionSpec as P

F32 = jnp.float32
BF16 = jnp.bfloat16
VMEM = pl.BlockSpec(memory_space=pltpu.VMEM)
EXTRA = 8


def halves(x):
    high = x.astype(BF16)
    low = (x - high.astype(F32)).astype(BF16)
    return high, low


def side(x):
    return jnp.concatenate(halves(x), axis=1)


def fold(x):
    width = x.shape[1] // 2
    return x[:, :width] + x[:, width:]


def dot(a, b, dims=((1,), (0,))):
    return lax.dot_general(a, b, (dims, ((), ())), preferred_element_type=F32)


def mm(x, w):
    wide = side(w)
    return fold(dot(side(x), jnp.concatenate([wide, wide], axis=0)))


def mmt(x, w):
    high, low = halves(w)
    both = jnp.concatenate(
        [jnp.concatenate([high, high], axis=1), jnp.concatenate([low, low], axis=1)], axis=0
    )
    return fold(dot(side(x), both, ((1,), (1,))))


def tmm(x, y):
    wide = fold(dot(side(x), side(y), ((0,), (0,))))
    width = x.shape[1]
    return wide[:width] + wide[width:]


def silu_parts(v):
    gate = 1.0 / (1.0 + jnp.exp(-v))
    return v * gate, gate * (1.0 + v * (1.0 - gate))


def row_of(column):
    n = column.shape[0]
    eye = lax.broadcasted_iota(jnp.int32, (n, n), 0) == lax.broadcasted_iota(jnp.int32, (n, n), 1)
    return jnp.sum(jnp.where(eye, column, 0.0), axis=0, keepdims=True)


def onehot(mask):
    return jnp.where(mask, 1.0, 0.0).astype(BF16)


def edge_forward(features, weight_in, recv, send, recv_t, slope_ref, chunk):
    width = features.shape[1]
    to_recv = side(mm(features, weight_in[:width]))
    to_send = side(mm(features, weight_in[width:]))
    total = None
    for start in range(0, recv.shape[0], chunk):
        rows = pl.ds(start, chunk)
        pre = fold(dot(recv[rows, :], to_recv) + dot(send[rows, :], to_send))
        act, slope = silu_parts(pre)
        slope_ref[rows, :] = slope
        part = dot(recv_t[:, rows], side(act))
        total = part if total is None else total + part
    return fold(total)


def edge_backward(local_grad, weight_out, recv, recv_t, send_t, slope_ref, chunk):
    spread = side(mmt(local_grad, weight_out))
    total_r = total_s = None
    for start in range(0, recv.shape[0], chunk):
        rows = pl.ds(start, chunk)
        grad = side(fold(dot(recv[rows, :], spread)) * slope_ref[rows, :])
        part_r = dot(recv_t[:, rows], grad)
        part_s = dot(send_t[:, rows], grad)
        total_r = part_r if total_r is None else total_r + part_r
        total_s = part_s if total_s is None else total_s + part_s
    return fold(total_r), fold(total_s)


def node_forward(features, summed, weight_in, weight_out):
    width = features.shape[1]
    pre = mm(features, weight_in[:width]) + mm(summed, weight_in[width:])
    act, slope = silu_parts(pre)
    return features + mm(act, weight_out), act, slope


def put_blocks(value, refs):
    size = refs[0].shape[0]
    for at, ref in enumerate(refs):
        ref[...] = value[at * size : (at + 1) * size]


def take_sum(own, came):
    parts = [
        ref[...] + came[at][...] if came[at] is not None else ref[...]
        for at, ref in enumerate(own)
    ]
    return jnp.concatenate(parts, axis=0)


def even(axis):
    return lax.rem(lax.axis_index(axis), 2) == 0


def first_kernel(
    chunk, feats_hbm, index_hbm, halo_hbm, target_hbm, decoder_hbm, *refs
):
    weights_hbm, refs = refs[:4], refs[4:]
    (target, decoder, edge_in, edge_out, node_in, node_out,
     flat_out, recv, send, recv_t, send_t, h_out, slope, q_out) = refs[:14]
    blocks, (feats, index, halo, sems) = refs[14:18], refs[18:]
    copies = [
        pltpu.make_async_copy(source, place, sems.at[at])
        for at, (source, place) in enumerate(
            zip(
                (index_hbm, halo_hbm, feats_hbm, *weights_hbm, target_hbm, decoder_hbm),
                (index, halo, feats, edge_in, edge_out, node_in, node_out, target, decoder),
            )
        )
    ]
    for copy in copies:
        copy.start()
    copies[0].wait()
    copies[1].wait()
    nodes = feats.shape[0]
    edges = index.shape[1]
    lanes = 128
    count = edges // lanes
    size = halo.shape[2]
    pieces = [index[0:1, pl.ds(b * lanes, lanes)] for b in range(count)]
    pieces += [index[1:2, pl.ds(b * lanes, lanes)] for b in range(count)]
    table = jnp.concatenate(pieces, axis=0).astype(F32)
    lists = jnp.concatenate([halo[0].astype(F32), jnp.zeros((4, lanes - size), F32)], axis=1)
    rest = jnp.zeros((lanes - 2 * count - 4, lanes), F32)
    columns = jnp.concatenate([table, lists, rest], axis=0).T
    by_dir = [columns[:size, 2 * count + k : 2 * count + k + 1] for k in range(4)]
    dom_even, sub_even = even("dom"), even("sub")
    flat = jnp.concatenate(
        [
            jnp.where(dom_even, by_dir[0], by_dir[1]),
            jnp.where(dom_even, by_dir[1], by_dir[0]),
            jnp.where(sub_even, by_dir[3], by_dir[2]),
            jnp.where(sub_even, by_dir[2], by_dir[3]),
        ],
        axis=0,
    )
    flat_row = row_of(flat)
    flat_out[...] = jnp.broadcast_to(flat, flat_out.shape)
    for b in range(count):
        rows = pl.ds(b * lanes, lanes)
        recv[rows, :] = onehot(columns[:, b : b + 1] == flat_row)
        send[rows, :] = onehot(columns[:, count + b : count + b + 1] == flat_row)
        recv_t[:, rows] = onehot(flat == table[b : b + 1])
        send_t[:, rows] = onehot(flat == table[count + b : count + b + 1])
    place = onehot(flat == lax.broadcasted_iota(jnp.int32, (nodes, nodes), 1).astype(F32))
    copies[2].wait()
    features = fold(dot(place, side(feats[...])))
    h_out[...] = features
    copies[3].wait()
    q = edge_forward(features, edge_in[0], recv, send, recv_t, slope, chunk)
    q_out[...] = q
    copies[4].wait()
    put_blocks(mm(q, edge_out[0]), blocks)
    for copy in copies[5:]:
        copy.wait()


def unpack(names, refs):
    came = []
    at = 0
    for there in names:
        came.append(refs[at] if there else None)
        at += there
    return came, refs[at:]


def middle_kernel(chunk, names, *refs):
    own, refs = refs[:4], refs[4:]
    came, refs = unpack(names, refs)
    (h, flat_ref, target, decoder, recv, send, recv_t, node_in, node_out, edge_in, edge_out,
     agg_out, h_out, node_act, node_slope, slope, q_out, pre_out, known_out, *messages) = refs
    nodes, width = h.shape
    summed = take_sum(own, came)
    agg_out[...] = summed
    features, act, gate = node_forward(h[...], summed, node_in[0], node_out[0])
    h_out[...] = features
    node_act[...] = act
    node_slope[...] = gate
    pre = mm(features, node_in[1, :width])
    pre_out[...] = pre
    base = jnp.sum(features * decoder[...], axis=1, keepdims=True)
    here = flat_ref[:, 0:1] == lax.broadcasted_iota(jnp.int32, (nodes, nodes), 1).astype(F32)
    wanted = jnp.sum(jnp.where(here, target[...], 0.0), axis=1, keepdims=True)
    first = lax.broadcasted_iota(jnp.int32, (nodes, width), 1) == 0
    known_out[...] = jnp.where(first, base, wanted)
    size = own[0].shape[0]
    short = base - wanted
    for at, message in enumerate(messages):
        rows = slice(at * size, (at + 1) * size)
        message[size : 2 * size, :] = pre[rows]
        line = row_of(short[rows])
        line = jnp.concatenate([line, jnp.zeros((1, width - size), F32)], axis=1)
        message[2 * size :, :] = jnp.concatenate(
            [line, jnp.ones((1, width), F32), jnp.zeros((EXTRA - 2, width), F32)], axis=0
        )
    q = edge_forward(features, edge_in[1], recv, send, recv_t, slope, chunk)
    q_out[...] = q
    local = mm(q, edge_out[1])
    for at, message in enumerate(messages):
        message[:size, :] = local[at * size : (at + 1) * size]


def column_of(row):
    n = row.shape[1]
    eye = lax.broadcasted_iota(jnp.int32, (n, n), 0) == lax.broadcasted_iota(jnp.int32, (n, n), 1)
    return jnp.sum(jnp.where(eye, row, 0.0), axis=1, keepdims=True)


def row_product(row, weight):
    return mm(jnp.broadcast_to(row, (8, row.shape[1])), weight)[0:1]


def back_kernel(chunk, count, names, *refs):
    own, refs = refs[:4], refs[4:]
    came, refs = unpack(names, refs)
    (flat_ref, decoder, pre_ref, known, node_slope, recv, recv_t, send_t, slope,
     edge_in, edge_out, node_in, node_out,
     agg_out, act_out, pre1_out, seed_out, local_out, recv_out, send_out, top_out, pre0_out,
     pred_out, loss_out, *blocks) = refs
    nodes, width = pre_ref.shape
    size = blocks[0].shape[0]
    summed = jnp.concatenate(
        [
            ref[:size, :] + came[at][:size, :] if came[at] is not None else ref[:size, :]
            for at, ref in enumerate(own)
        ],
        axis=0,
    )
    agg_out[...] = summed
    pre_agg = mm(summed, node_in[1, width:])
    act, gate = silu_parts(pre_ref[...] + pre_agg)
    act_out[...] = act
    weights = decoder[...]
    lead = row_of(jnp.sum(node_out[1] * weights, axis=1, keepdims=True))
    base, wanted = known[:, 0:1], known[:, 1:2]
    predicted = base + jnp.sum(act * lead, axis=1, keepdims=True)
    misfit = predicted - wanted
    seed = 2.0 * misfit / count
    seed_out[...] = jnp.broadcast_to(seed, seed_out.shape)
    here = flat_ref[:, 0:1] == lax.broadcasted_iota(jnp.int32, (nodes, nodes), 1).astype(F32)
    pred_out[...] = jnp.sum(jnp.where(here, predicted, 0.0), axis=0, keepdims=True)
    loss_out[...] = jnp.broadcast_to(
        jnp.sum(misfit * misfit, axis=0, keepdims=True), loss_out.shape
    )
    pre_grad = seed * lead * gate
    pre1_out[...] = pre_grad
    shared = []
    for at in range(4):
        rows = slice(at * size, (at + 1) * size)
        if came[at] is None:
            shared.append(pre_grad[rows])
            continue
        far_act, far_gate = silu_parts(came[at][size : 2 * size, :] + pre_agg[rows])
        far_misfit = column_of(came[at][2 * size : 2 * size + 1, :size])
        far_misfit = far_misfit + jnp.sum(far_act * lead, axis=1, keepdims=True)
        there = came[at][2 * size + 1 : 2 * size + 2, 0:1]
        far_seed = 2.0 * far_misfit / count * there
        shared.append(pre_grad[rows] + far_seed * lead * far_gate)
    local_grad = mmt(jnp.concatenate(shared, axis=0), node_in[1, width:])
    local_out[...] = local_grad
    to_recv, to_send = edge_backward(local_grad, edge_out[1], recv, recv_t, send_t, slope, chunk)
    recv_out[...] = to_recv
    send_out[...] = to_send
    top = (
        seed * weights
        + mmt(pre_grad, node_in[1, :width])
        + mmt(to_recv, edge_in[1, :width])
        + mmt(to_send, edge_in[1, width:])
    )
    top_out[...] = top
    pre0 = mmt(top, node_out[0]) * node_slope[...]
    pre0_out[...] = pre0
    put_blocks(mmt(pre0, node_in[0, width:]), blocks)


def grads_kernel(
    h0, agg0, act0, pre0, top0, h1, agg1, act1, pre1, seed, q1, local1, to_recv1, to_send1,
    decoder, node_out, loss, high, low, tail
):
    width = h0.shape[1]
    rows = seed[...]
    top1 = rows * decoder[...]
    act = act1[...]
    parts = [
        tmm(h1[...], pre1[...]),
        tmm(agg1[...], pre1[...]),
        tmm(act, top1),
        tmm(h1[...], to_recv1[...]),
        tmm(h1[...], to_send1[...]),
        tmm(q1[...], local1[...]),
    ]
    for at, part in enumerate(parts):
        high[at * width : (at + 1) * width, :] = part
    low[0:width, :] = tmm(h0[...], pre0[...])
    low[width : 2 * width, :] = tmm(agg0[...], pre0[...])
    low[2 * width :, :] = tmm(act0[...], top0[...])
    line = jnp.sum(rows * h1[...], axis=0, keepdims=True)
    line = line + row_product(jnp.sum(rows * act, axis=0, keepdims=True), node_out[1])
    tail[...] = jnp.concatenate([line, loss[...], jnp.zeros((EXTRA - 2, width), F32)], axis=0)


def put_rows(ref, at, value):
    ref[at : at + value.shape[0], :] = value
    return at + value.shape[0]


def end_kernel(chunk, names, *refs):
    own, refs = refs[:4], refs[4:]
    came, refs = unpack(names, refs)
    h, q, recv, recv_t, send_t, slope, edge_out, node_low, high, tail, mine, other = refs
    local_grad = take_sum(own, came)
    to_recv, to_send = edge_backward(local_grad, edge_out[0], recv, recv_t, send_t, slope, chunk)
    low = [
        node_low[...],
        tmm(h[...], to_recv),
        tmm(h[...], to_send),
        tmm(q[...], local_grad),
        tail[...],
    ]

    def write(ref_high, ref_low):
        at = 0
        for value in low:
            at = put_rows(ref_low, at, value)
        put_rows(ref_high, put_rows(ref_high, 0, high[...]), tail[...])

    first = lax.axis_index("sub") == 0
    pl.when(first)(lambda: write(mine, other))
    pl.when(jnp.logical_not(first))(lambda: write(other, mine))


def quarters_kernel(mine, other, *outs):
    per = outs[0].shape[0] - EXTRA
    own = lax.rem(lax.axis_index("dom"), 4)
    tail = mine[4 * per :, :] + other[4 * per :, :]
    for away, out in enumerate(outs):
        rows = pl.ds(pl.multiple_of(jnp.bitwise_xor(own, away) * per, 8), per)
        out[:per, :] = mine[rows, :] + other[rows, :]
        out[per:, :] = tail


def four_kernel(a, b, c, d, out):
    out[...] = (a[...] + b[...]) + (c[...] + d[...])


def two_kernel(a, b, out):
    out[...] = a[...] + b[...]


def last_sum_kernel(a, b, out, tail):
    per = out.shape[0]
    out[...] = a[:per, :] + b[:per, :]
    tail[...] = a[per:, :] + b[per:, :]


def scale_kernel(params, count, *refs):
    near, far = refs[:4], refs[4:8]
    tail, loss, edge_in, edge_out, node_in, node_out, decoder = refs[8:]
    width = tail.shape[1]
    line = tail[0:1]
    squares = []
    for group in (near, far):
        sums = [jnp.sum(ref[...] * ref[...], axis=0, keepdims=True) for ref in group]
        squares.append((sums[0] + sums[1]) + (sums[2] + sums[3]))
    every = jnp.sum(squares[0] + squares[1] + line * line, axis=1, keepdims=True)
    scale = 1.0 / jnp.sqrt(every / params + 1e-06)
    decoder[...] = line * scale
    loss[...] = tail[1:2] / count
    where = [(node_in, at) for at in range(2)] + [(node_out, 0)]
    where = where + [(edge_in, at) for at in range(2)] + [(edge_out, 0)]

    def write(own, layer, group):
        per = group[0].shape[0]
        for quarter in range(4):
            ref = group[quarter ^ own]
            at = 0
            while at < per:
                block, inside = divmod(quarter * per + at, width)
                take = min(width - inside, per - at)
                out, half = where[block]
                first = half * width + inside
                out[layer, first : first + take, :] = ref[at : at + take, :] * scale
                at += take

    here = lax.rem(lax.axis_index("dom"), 4)
    side_here = lax.axis_index("sub")
    for own in range(4):
        for core in range(2):
            def both(own=own, core=core):
                write(own, 1 - core, near)
                write(own, core, far)

            pl.when(jnp.logical_and(here == own, side_here == core))(both)


def call(kernel, outs, *args):
    shapes = [jax.ShapeDtypeStruct(shape, dtype) for shape, dtype in outs]
    return pl.pallas_call(
        kernel,
        out_shape=shapes,
        in_specs=[VMEM] * len(args),
        out_specs=[VMEM] * len(shapes),
        compiler_params=pltpu.CompilerParams(vmem_limit_bytes=16 * 2**20),
    )(*args)


def pairs(count, offset):
    found = []
    for low in range(offset, count - 1, 2):
        found += [(low, low + 1), (low + 1, low)]
    return found


def per_device(
    node_feats, edge_in, edge_out, node_in, node_out, decoder, edge_index, halo_index, target
):
    nodes, width = node_feats.shape
    edges = edge_index.shape[1]
    size = halo_index.shape[2]
    n_dom, n_sub = lax.axis_size("dom"), lax.axis_size("sub")
    count = nodes * n_dom * n_sub
    if edge_in.shape[0] != 2 or 4 * size != nodes:
        raise ValueError("unsupported sizes")
    chunk = 256
    axes = ["dom", "dom", "sub", "sub"]
    links = [pairs(lax.axis_size(axis), offset) for axis, offset in zip(axes, (1, 0, 0, 1))]
    names = tuple(1 if link else 0 for link in links)

    def exchange(blocks):
        came = [None] * 4
        for at in range(4):
            if links[at]:
                came[at] = lax.ppermute(blocks[at], axes[at], links[at])
        return [block for block in came if block is not None]

    node_shape = ((nodes, width), F32)
    edge_shape = ((edges, width), F32)
    block_shapes = [((size, width), F32)] * 4

    weights = (edge_in, edge_out, node_in, node_out)
    sources = (
        node_feats, edge_index, halo_index, target.reshape(1, nodes), decoder.reshape(1, width),
        *weights,
    )
    shapes = [
        ((1, nodes), F32), ((1, width), F32), *[(weight.shape, F32) for weight in weights],
        ((nodes, 128), F32),
        ((edges, nodes), BF16), ((edges, nodes), BF16),
        ((nodes, edges), BF16), ((nodes, edges), BF16),
        node_shape, edge_shape, node_shape, *block_shapes,
    ]
    (wanted, readout, edge_in, edge_out, node_in, node_out,
     flat, recv, send, recv_t, send_t, h0, slope0, q0, *blocks) = pl.pallas_call(
        functools.partial(first_kernel, chunk),
        out_shape=[jax.ShapeDtypeStruct(shape, dtype) for shape, dtype in shapes],
        in_specs=[pl.BlockSpec(memory_space=pltpu.HBM)] * len(sources),
        out_specs=[VMEM] * len(shapes),
        scratch_shapes=[
            pltpu.VMEM(node_feats.shape, F32),
            pltpu.VMEM(edge_index.shape, jnp.int32),
            pltpu.VMEM(halo_index.shape, jnp.int32),
            pltpu.SemaphoreType.DMA((len(sources),)),
        ],
        compiler_params=pltpu.CompilerParams(vmem_limit_bytes=16 * 2**20),
    )(*[pltpu.with_memory_space_constraint(source, pltpu.HBM) for source in sources])
    message = ((2 * size + EXTRA, width), F32)
    agg0, h1, act0, gate0, slope1, q1, pre, known, *messages = call(
        functools.partial(middle_kernel, chunk, names),
        [node_shape, node_shape, node_shape, node_shape, edge_shape, node_shape,
         node_shape, node_shape, *[message] * 4],
        *blocks, *exchange(blocks),
        h0, flat, wanted, readout, recv, send, recv_t, node_in, node_out, edge_in, edge_out,
    )
    (agg1, act1, pre1, seed, local1, to_recv1, to_send1, top0, pre0, pred, loss,
     *blocks) = call(
        functools.partial(back_kernel, chunk, count, names),
        [*[node_shape] * 9, ((1, nodes), F32), ((1, width), F32), *block_shapes],
        *messages, *exchange(messages),
        flat, readout, pre, known, gate0, recv, recv_t, send_t, slope1,
        edge_in, edge_out, node_in, node_out,
    )
    came = exchange(blocks)
    high, node_low, tail = call(
        grads_kernel,
        [((6 * width, width), F32), ((3 * width, width), F32), ((EXTRA, width), F32)],
        h0, agg0, act0, pre0, top0, h1, agg1, act1, pre1, seed, q1, local1, to_recv1, to_send1,
        readout, node_out, loss,
    )
    rows = 6 * width
    groups = n_dom // 4
    if n_sub != 2 or n_dom % 4 or groups & (groups - 1) or rows % 32:
        return slow_tail(
            count, blocks, came, names, chunk, h0, q0, recv, recv_t, send_t, slope0, edge_out,
            node_low, high, tail, pred, nodes,
        )
    per = rows // 4
    half = ((rows + EXTRA, width), F32)
    quarter = ((per + EXTRA, width), F32)
    mine, other = call(
        functools.partial(end_kernel, chunk, names),
        [half, half],
        *blocks, *came, h0, q0, recv, recv_t, send_t, slope0, edge_out, node_low, high, tail,
    )

    def swap(value):
        return lax.ppermute(value, "sub", pairs(n_sub, 0))

    def across(value, away):
        return lax.ppermute(value, "dom", [(at, at ^ away) for at in range(n_dom)])

    parts = call(quarters_kernel, [quarter] * 4, mine, swap(other))
    came = [across(parts[away], away) for away in (3, 2, 1)]
    (total,) = call(four_kernel, [quarter], parts[0], came[2], came[1], came[0])
    away = 4
    while away < n_dom // 2:
        (total,) = call(two_kernel, [quarter], total, across(total, away))
        away *= 2
    if away < n_dom:
        far = across(total, away)
    else:
        far = jnp.zeros_like(total)
    total, tail = call(
        last_sum_kernel, [((per, width), F32), ((EXTRA, width), F32)], total, far
    )
    near = [total] + [across(total, away) for away in range(1, 4)]
    far = [swap(value) for value in near]
    params = 2 * 6 * width * width + width
    loss, g_edge_in, g_edge_out, g_node_in, g_node_out, g_decoder = call(
        functools.partial(scale_kernel, params, count),
        [
            ((1, width), F32),
            ((2, 2 * width, width), F32), ((2, width, width), F32),
            ((2, 2 * width, width), F32), ((2, width, width), F32),
            ((1, width), F32),
        ],
        *near, *far, tail,
    )
    return (
        loss[0, 0], pred.reshape(nodes), g_edge_in, g_edge_out, g_node_in, g_node_out,
        g_decoder.reshape(width),
    )


def low_kernel(chunk, names, *refs):
    own, refs = refs[:4], refs[4:]
    came, refs = unpack(names, refs)
    h, q, recv, recv_t, send_t, slope, edge_out, out = refs
    local_grad = take_sum(own, came)
    to_recv, to_send = edge_backward(local_grad, edge_out[0], recv, recv_t, send_t, slope, chunk)
    width = h.shape[1]
    out[0:width, :] = tmm(h[...], to_recv)
    out[width : 2 * width, :] = tmm(h[...], to_send)
    out[2 * width :, :] = tmm(q[...], local_grad)


def slow_tail(
    count, blocks, came, names, chunk, h0, q0, recv, recv_t, send_t, slope0, edge_out,
    node_low, high, tail, pred, nodes,
):
    width = h0.shape[1]
    (edge_low,) = call(
        functools.partial(low_kernel, chunk, names), [((3 * width, width), F32)],
        *blocks, *came, h0, q0, recv, recv_t, send_t, slope0, edge_out,
    )
    total = lax.psum(
        jnp.concatenate([node_low, edge_low, high, tail], 0), ("dom", "sub")
    )
    rows = 12 * width
    body = total[: rows + 1]
    params = (rows + 1) * width
    scale = 1.0 / jnp.sqrt(jnp.sum(body * body) / params + 1e-06)
    grads = (total[:rows] * scale).reshape(2, 2, 3 * width, width)
    return (
        total[rows + 1, 0] / count, pred.reshape(nodes),
        grads[:, 1, : 2 * width], grads[:, 1, 2 * width :],
        grads[:, 0, : 2 * width], grads[:, 0, 2 * width :],
        total[rows] * scale,
    )


def solution(mesh):
    placed = (
        P(("dom", "sub"), None),
        P(),
        P(),
        P(),
        P(),
        P(),
        P(None, ("dom", "sub")),
        P(("dom", "sub"), None, None),
        P(("dom", "sub")),
    )
    return jax.shard_map(
        per_device,
        mesh=mesh,
        in_specs=placed,
        out_specs=(P(), P(("dom", "sub")), P(), P(), P(), P(), P()),
        check_vma=False,
    )
```

```python
import functools

import jax
import jax.numpy as jnp
from jax import lax
from jax.experimental import pallas as pl
from jax.experimental.pallas import tpu as pltpu
from jax.sharding import PartitionSpec as P


F32 = jnp.float32
BF16 = jnp.bfloat16
VMEM = pl.BlockSpec(memory_space=pltpu.VMEM)
EXTRA = 8


def halves(x):
    high = x.astype(BF16)
    low = (x - high.astype(F32)).astype(BF16)
    return high, low


def side(x):
    return jnp.concatenate(halves(x), axis=1)


def fold(x):
    width = x.shape[1] // 2
    return x[:, :width] + x[:, width:]


def dot(a, b, dims=((1,), (0,))):
    return lax.dot_general(a, b, (dims, ((), ())), preferred_element_type=F32)


def mm(x, w):
    wide = side(w)
    return fold(dot(side(x), jnp.concatenate([wide, wide], axis=0)))


def mmt(x, w):
    high, low = halves(w)
    both = jnp.concatenate(
        [jnp.concatenate([high, high], axis=1), jnp.concatenate([low, low], axis=1)], axis=0
    )
    return fold(dot(side(x), both, ((1,), (1,))))


def tmm(x, y):
    wide = fold(dot(side(x), side(y), ((0,), (0,))))
    width = x.shape[1]
    return wide[:width] + wide[width:]


def silu_parts(v):
    gate = 1.0 / (1.0 + jnp.exp(-v))
    return v * gate, gate * (1.0 + v * (1.0 - gate))


def row_of(column):
    n = column.shape[0]
    eye = lax.broadcasted_iota(jnp.int32, (n, n), 0) == lax.broadcasted_iota(jnp.int32, (n, n), 1)
    return jnp.sum(jnp.where(eye, column, 0.0), axis=0, keepdims=True)


def onehot(mask):
    return jnp.where(mask, 1.0, 0.0).astype(BF16)


def edge_forward(features, weight_in, recv, send, recv_t, slope_ref, chunk):
    width = features.shape[1]
    to_recv = side(mm(features, weight_in[:width]))
    to_send = side(mm(features, weight_in[width:]))
    total = None
    for start in range(0, recv.shape[0], chunk):
        rows = pl.ds(start, chunk)
        pre = fold(dot(recv[rows, :], to_recv) + dot(send[rows, :], to_send))
        act, slope = silu_parts(pre)
        slope_ref[rows, :] = slope
        part = dot(recv_t[:, rows], side(act))
        total = part if total is None else total + part
    return fold(total)


def edge_backward(local_grad, weight_out, recv, recv_t, send_t, slope_ref, chunk):
    spread = side(mmt(local_grad, weight_out))
    total_r = total_s = None
    for start in range(0, recv.shape[0], chunk):
        rows = pl.ds(start, chunk)
        grad = side(fold(dot(recv[rows, :], spread)) * slope_ref[rows, :])
        part_r = dot(recv_t[:, rows], grad)
        part_s = dot(send_t[:, rows], grad)
        total_r = part_r if total_r is None else total_r + part_r
        total_s = part_s if total_s is None else total_s + part_s
    return fold(total_r), fold(total_s)


def node_forward(features, summed, weight_in, weight_out):
    width = features.shape[1]
    pre = mm(features, weight_in[:width]) + mm(summed, weight_in[width:])
    act, slope = silu_parts(pre)
    return features + mm(act, weight_out), act, slope


def put_blocks(value, refs):
    size = refs[0].shape[0]
    for at, ref in enumerate(refs):
        ref[...] = value[at * size : (at + 1) * size]


def take_sum(own, came):
    parts = [
        ref[...] + came[at][...] if came[at] is not None else ref[...]
        for at, ref in enumerate(own)
    ]
    return jnp.concatenate(parts, axis=0)


def even(axis):
    return lax.rem(lax.axis_index(axis), 2) == 0


def first_kernel(
    chunk, feats_hbm, index_hbm, halo_hbm, target_hbm, decoder_hbm, *refs
):
    weights_hbm, refs = refs[:4], refs[4:]
    (target, decoder, edge_in, edge_out, node_in, node_out,
     flat_out, recv, send, recv_t, send_t, h_out, slope, q_out, raw) = refs[:15]
    blocks, (feats, index, halo, sems) = refs[15:19], refs[19:]
    copies = [
        pltpu.make_async_copy(source, place, sems.at[at])
        for at, (source, place) in enumerate(
            zip(
                (index_hbm, halo_hbm, feats_hbm, *weights_hbm, target_hbm, decoder_hbm),
                (index, halo, feats, edge_in, edge_out, node_in, node_out, target, decoder),
            )
        )
    ]
    for copy in copies:
        copy.start()
    copies[0].wait()
    copies[1].wait()
    nodes = feats.shape[0]
    edges = index.shape[1]
    lanes = 128
    count = edges // lanes
    size = halo.shape[2]
    pieces = [index[0:1, pl.ds(b * lanes, lanes)] for b in range(count)]
    pieces += [index[1:2, pl.ds(b * lanes, lanes)] for b in range(count)]
    table = jnp.concatenate(pieces, axis=0).astype(F32)
    lists = jnp.concatenate([halo[0].astype(F32), jnp.zeros((4, lanes - size), F32)], axis=1)
    rest = jnp.zeros((lanes - 2 * count - 4, lanes), F32)
    columns = jnp.concatenate([table, lists, rest], axis=0).T
    by_dir = [columns[:size, 2 * count + k : 2 * count + k + 1] for k in range(4)]
    dom_even, sub_even = even("dom"), even("sub")
    flat = jnp.concatenate(
        [
            jnp.where(dom_even, by_dir[0], by_dir[1]),
            jnp.where(dom_even, by_dir[1], by_dir[0]),
            jnp.where(sub_even, by_dir[3], by_dir[2]),
            jnp.where(sub_even, by_dir[2], by_dir[3]),
        ],
        axis=0,
    )
    raw[nodes:, :] = jnp.concatenate(
        [
            table,
            jnp.where(dom_even, lists[0:1], lists[1:2]),
            jnp.where(dom_even, lists[1:2], lists[0:1]),
            jnp.where(sub_even, lists[3:4], lists[2:3]),
            jnp.where(sub_even, lists[2:3], lists[3:4]),
        ],
        axis=0,
    )
    flat_row = row_of(flat)
    flat_out[...] = jnp.broadcast_to(flat, flat_out.shape)
    for b in range(count):
        rows = pl.ds(b * lanes, lanes)
        recv[rows, :] = onehot(columns[:, b : b + 1] == flat_row)
        send[rows, :] = onehot(columns[:, count + b : count + b + 1] == flat_row)
        recv_t[:, rows] = onehot(flat == table[b : b + 1])
        send_t[:, rows] = onehot(flat == table[count + b : count + b + 1])
    place = onehot(flat == lax.broadcasted_iota(jnp.int32, (nodes, nodes), 1).astype(F32))
    copies[2].wait()
    plain = feats[...]
    raw[:nodes, :] = plain
    features = fold(dot(place, side(plain)))
    h_out[...] = features
    copies[3].wait()
    q = edge_forward(features, edge_in[0], recv, send, recv_t, slope, chunk)
    q_out[...] = q
    copies[4].wait()
    put_blocks(mm(q, edge_out[0]), blocks)
    for copy in copies[5:]:
        copy.wait()


def unpack(names, refs):
    came = []
    at = 0
    for there in names:
        came.append(refs[at] if there else None)
        at += there
    return came, refs[at:]


def middle_kernel(chunk, names, *refs):
    own, refs = refs[:4], refs[4:]
    came, refs = unpack(names, refs)
    (h, flat_ref, target, decoder, recv, send, recv_t, node_in, node_out, edge_in, edge_out,
     agg_out, h_out, node_act, node_slope, slope, q_out, pre_out, known_out, *messages) = refs
    nodes, width = h.shape
    summed = take_sum(own, came)
    agg_out[...] = summed
    features, act, gate = node_forward(h[...], summed, node_in[0], node_out[0])
    h_out[...] = features
    node_act[...] = act
    node_slope[...] = gate
    pre = mm(features, node_in[1, :width])
    pre_out[...] = pre
    base = jnp.sum(features * decoder[...], axis=1, keepdims=True)
    here = flat_ref[:, 0:1] == lax.broadcasted_iota(jnp.int32, (nodes, nodes), 1).astype(F32)
    wanted = jnp.sum(jnp.where(here, target[...], 0.0), axis=1, keepdims=True)
    first = lax.broadcasted_iota(jnp.int32, (nodes, width), 1) == 0
    known_out[...] = jnp.where(first, base, wanted)
    size = own[0].shape[0]
    short = base - wanted
    for at, message in enumerate(messages):
        rows = slice(at * size, (at + 1) * size)
        message[size : 2 * size, :] = pre[rows]
        line = row_of(short[rows])
        line = jnp.concatenate([line, jnp.zeros((1, width - size), F32)], axis=1)
        message[2 * size :, :] = jnp.concatenate(
            [line, jnp.ones((1, width), F32), jnp.zeros((EXTRA - 2, width), F32)], axis=0
        )
    q = edge_forward(features, edge_in[1], recv, send, recv_t, slope, chunk)
    q_out[...] = q
    local = mm(q, edge_out[1])
    for at, message in enumerate(messages):
        message[:size, :] = local[at * size : (at + 1) * size]


def column_of(row):
    n = row.shape[1]
    eye = lax.broadcasted_iota(jnp.int32, (n, n), 0) == lax.broadcasted_iota(jnp.int32, (n, n), 1)
    return jnp.sum(jnp.where(eye, row, 0.0), axis=1, keepdims=True)


def row_product(row, weight):
    return mm(jnp.broadcast_to(row, (8, row.shape[1])), weight)[0:1]


def back_kernel(chunk, count, names, *refs):
    own, refs = refs[:4], refs[4:]
    came, refs = unpack(names, refs)
    (flat_ref, decoder, pre_ref, known, node_slope, recv, recv_t, send_t, slope,
     edge_in, edge_out, node_in, node_out, _,
     agg_out, act_out, pre1_out, seed_out, local_out, recv_out, send_out, top_out, pre0_out,
     pred_out, loss_out, *blocks) = refs
    nodes, width = pre_ref.shape
    size = blocks[0].shape[0]
    summed = jnp.concatenate(
        [
            ref[:size, :] + came[at][:size, :] if came[at] is not None else ref[:size, :]
            for at, ref in enumerate(own)
        ],
        axis=0,
    )
    agg_out[...] = summed
    pre_agg = mm(summed, node_in[1, width:])
    act, gate = silu_parts(pre_ref[...] + pre_agg)
    act_out[...] = act
    weights = decoder[...]
    lead = row_of(jnp.sum(node_out[1] * weights, axis=1, keepdims=True))
    base, wanted = known[:, 0:1], known[:, 1:2]
    predicted = base + jnp.sum(act * lead, axis=1, keepdims=True)
    misfit = predicted - wanted
    seed = 2.0 * misfit / count
    seed_out[...] = jnp.broadcast_to(seed, seed_out.shape)
    here = flat_ref[:, 0:1] == lax.broadcasted_iota(jnp.int32, (nodes, nodes), 1).astype(F32)
    pred_out[...] = jnp.sum(jnp.where(here, predicted, 0.0), axis=0, keepdims=True)
    loss_out[...] = jnp.broadcast_to(
        jnp.sum(misfit * misfit, axis=0, keepdims=True), loss_out.shape
    )
    pre_grad = seed * lead * gate
    pre1_out[...] = pre_grad
    shared = []
    for at in range(4):
        rows = slice(at * size, (at + 1) * size)
        if came[at] is None:
            shared.append(pre_grad[rows])
            continue
        far_act, far_gate = silu_parts(came[at][size : 2 * size, :] + pre_agg[rows])
        far_misfit = column_of(came[at][2 * size : 2 * size + 1, :size])
        far_misfit = far_misfit + jnp.sum(far_act * lead, axis=1, keepdims=True)
        there = came[at][2 * size + 1 : 2 * size + 2, 0:1]
        far_seed = 2.0 * far_misfit / count * there
        shared.append(pre_grad[rows] + far_seed * lead * far_gate)
    local_grad = mmt(jnp.concatenate(shared, axis=0), node_in[1, width:])
    local_out[...] = local_grad
    to_recv, to_send = edge_backward(local_grad, edge_out[1], recv, recv_t, send_t, slope, chunk)
    recv_out[...] = to_recv
    send_out[...] = to_send
    top = (
        seed * weights
        + mmt(pre_grad, node_in[1, :width])
        + mmt(to_recv, edge_in[1, :width])
        + mmt(to_send, edge_in[1, width:])
    )
    top_out[...] = top
    pre0 = mmt(top, node_out[0]) * node_slope[...]
    pre0_out[...] = pre0
    put_blocks(mmt(pre0, node_in[0, width:]), blocks)


def grads_kernel(
    h0, agg0, act0, pre0, top0, h1, agg1, act1, pre1, seed, q1, local1, to_recv1, to_send1,
    decoder, node_out, loss, block, raw, shared, far_slope, far_q, far_recv, far_recv_t, far_send_t,
    edge_out, high, low, far, tail, *, chunk
):
    width = h0.shape[1]
    rows = seed[...]
    top1 = rows * decoder[...]
    act = act1[...]
    parts = [
        tmm(h1[...], pre1[...]),
        tmm(agg1[...], pre1[...]),
        tmm(act, top1),
        tmm(h1[...], to_recv1[...]),
        tmm(h1[...], to_send1[...]),
        tmm(q1[...], local1[...]),
    ]
    for at, part in enumerate(parts):
        high[at * width : (at + 1) * width, :] = part
    low[0:width, :] = tmm(h0[...], pre0[...])
    low[width : 2 * width, :] = tmm(agg0[...], pre0[...])
    low[2 * width :, :] = tmm(act0[...], top0[...])
    to_recv, to_send = edge_backward(
        block[...], edge_out[0], far_recv, far_recv_t, far_send_t, far_slope, chunk
    )
    far[0:width, :] = tmm(shared[...], to_recv)
    far[width : 2 * width, :] = tmm(raw[: h0.shape[0], :], to_send)
    far[2 * width :, :] = tmm(far_q[...], block[...])
    line = jnp.sum(rows * h1[...], axis=0, keepdims=True)
    line = line + row_product(jnp.sum(rows * act, axis=0, keepdims=True), node_out[1])
    tail[...] = jnp.concatenate([line, loss[...], jnp.zeros((EXTRA - 2, width), F32)], axis=0)


def far_kernel(chunk, names, size, *refs):
    raws, refs = unpack(names, refs)
    edge_in, refs = refs[0], refs[1:]
    at = 0
    for place, raw in enumerate(raws):
        if raw is None:
            continue
        shared_out, slope, q_out, recv, recv_t, send, send_t = refs[at : at + 7]
        at += 7
        edges, width = slope.shape
        nodes = send_t.shape[0]
        count = edges // width
        block = jnp.concatenate(
            [raw[nodes:, :], jnp.zeros((width + nodes - raw.shape[0], width), F32)], axis=0
        )
        columns = block.T
        own = block[2 * count + place : 2 * count + place + 1, :size]
        down = columns[:size, 2 * count + place : 2 * count + place + 1]
        along = lax.broadcasted_iota(jnp.int32, (1, nodes), 1).astype(F32)
        across = lax.broadcasted_iota(jnp.int32, (nodes, 1), 0).astype(F32)
        for b in range(count):
            rows = pl.ds(b * width, width)
            recv[rows, :] = onehot(columns[:, b : b + 1] == own)
            send[rows, :] = onehot(columns[:, count + b : count + b + 1] == along)
            recv_t[:, rows] = onehot(down == block[b : b + 1])
            send_t[:, rows] = onehot(across == block[count + b : count + b + 1])
        features = raw[:nodes, :]
        shared = fold(dot(onehot(down == along), side(features)))
        shared_out[...] = shared
        to_recv = side(mm(shared, edge_in[0, :width]))
        to_send = side(mm(features, edge_in[0, width:]))
        total = None
        for start in range(0, edges, chunk):
            rows = pl.ds(start, chunk)
            pre = fold(dot(recv[rows, :], to_recv) + dot(send[rows, :], to_send))
            act, rise = silu_parts(pre)
            slope[rows, :] = rise
            part = dot(recv_t[:, rows], side(act))
            total = part if total is None else total + part
        q_out[...] = fold(total)


def put_rows(ref, at, value):
    ref[at : at + value.shape[0], :] = value
    return at + value.shape[0]


def end_kernel(chunk, names, *refs):
    own, refs = refs[:4], refs[4:]
    came, refs = unpack(names, refs)
    h, q, recv, recv_t, send_t, slope, edge_out, node_low, high, far, tail, mine, other = refs
    local_grad = take_sum(own, came)
    to_recv, to_send = edge_backward(local_grad, edge_out[0], recv, recv_t, send_t, slope, chunk)
    width = h.shape[1]
    low = [
        node_low[...],
        tmm(h[...], to_recv) + far[0:width, :],
        tmm(h[...], to_send) + far[width : 2 * width, :],
        tmm(q[...], local_grad) + far[2 * width :, :],
        tail[...],
    ]

    def write(ref_high, ref_low):
        at = 0
        for value in low:
            at = put_rows(ref_low, at, value)
        put_rows(ref_high, put_rows(ref_high, 0, high[...]), tail[...])

    first = lax.axis_index("sub") == 0
    pl.when(first)(lambda: write(mine, other))
    pl.when(jnp.logical_not(first))(lambda: write(other, mine))


def quarters_kernel(mine, other, *outs):
    per = outs[0].shape[0] - EXTRA
    own = lax.rem(lax.axis_index("dom"), 4)
    tail = mine[4 * per :, :] + other[4 * per :, :]
    for away, out in enumerate(outs):
        rows = pl.ds(pl.multiple_of(jnp.bitwise_xor(own, away) * per, 8), per)
        out[:per, :] = mine[rows, :] + other[rows, :]
        out[per:, :] = tail


def four_kernel(a, b, c, d, out):
    out[...] = (a[...] + b[...]) + (c[...] + d[...])


def two_kernel(a, b, out):
    out[...] = a[...] + b[...]


def last_sum_kernel(a, b, out, tail):
    per = out.shape[0]
    out[...] = a[:per, :] + b[:per, :]
    tail[...] = a[per:, :] + b[per:, :]


def scale_kernel(params, count, *refs):
    near, far = refs[:4], refs[4:8]
    tail, loss, edge_in, edge_out, node_in, node_out, decoder = refs[8:]
    width = tail.shape[1]
    line = tail[0:1]
    squares = []
    for group in (near, far):
        sums = [jnp.sum(ref[...] * ref[...], axis=0, keepdims=True) for ref in group]
        squares.append((sums[0] + sums[1]) + (sums[2] + sums[3]))
    every = jnp.sum(squares[0] + squares[1] + line * line, axis=1, keepdims=True)
    scale = 1.0 / jnp.sqrt(every / params + 1e-06)
    decoder[...] = line * scale
    loss[...] = tail[1:2] / count
    where = [(node_in, at) for at in range(2)] + [(node_out, 0)]
    where = where + [(edge_in, at) for at in range(2)] + [(edge_out, 0)]

    def write(own, layer, group):
        per = group[0].shape[0]
        for quarter in range(4):
            ref = group[quarter ^ own]
            at = 0
            while at < per:
                block, inside = divmod(quarter * per + at, width)
                take = min(width - inside, per - at)
                out, half = where[block]
                first = half * width + inside
                out[layer, first : first + take, :] = ref[at : at + take, :] * scale
                at += take

    here = lax.rem(lax.axis_index("dom"), 4)
    side_here = lax.axis_index("sub")
    for own in range(4):
        for core in range(2):
            def both(own=own, core=core):
                write(own, 1 - core, near)
                write(own, core, far)

            pl.when(jnp.logical_and(here == own, side_here == core))(both)


def call(kernel, outs, *args):
    shapes = [jax.ShapeDtypeStruct(shape, dtype) for shape, dtype in outs]
    return pl.pallas_call(
        kernel,
        out_shape=shapes,
        in_specs=[VMEM] * len(args),
        out_specs=[VMEM] * len(shapes),
        compiler_params=pltpu.CompilerParams(vmem_limit_bytes=16 * 2**20),
    )(*args)


def pairs(count, offset):
    found = []
    for low in range(offset, count - 1, 2):
        found += [(low, low + 1), (low + 1, low)]
    return found


def per_device(
    node_feats, edge_in, edge_out, node_in, node_out, decoder, edge_index, halo_index, target
):
    nodes, width = node_feats.shape
    edges = edge_index.shape[1]
    size = halo_index.shape[2]
    n_dom, n_sub = lax.axis_size("dom"), lax.axis_size("sub")
    count = nodes * n_dom * n_sub
    if n_dom < 3 or edge_in.shape[0] != 2 or 4 * size != nodes:
        raise ValueError("unsupported sizes")
    chunk = 256
    axes = ["dom", "dom", "sub", "sub"]
    links = [pairs(lax.axis_size(axis), offset) for axis, offset in zip(axes, (1, 0, 0, 1))]
    names = tuple(1 if link else 0 for link in links)

    def exchange(blocks, last=4, first=0):
        came = [None] * 4
        for at in range(first, last):
            if links[at]:
                came[at] = lax.ppermute(blocks[at], axes[at], links[at])
        return [block for block in came if block is not None]

    node_shape = ((nodes, width), F32)
    edge_shape = ((edges, width), F32)
    block_shapes = [((size, width), F32)] * 4

    weights = (edge_in, edge_out, node_in, node_out)
    sources = (
        node_feats, edge_index, halo_index, target.reshape(1, nodes), decoder.reshape(1, width),
        *weights,
    )
    raw_shape = ((nodes + 2 * edges // width + 4, width), F32)
    shapes = [
        ((1, nodes), F32), ((1, width), F32), *[(weight.shape, F32) for weight in weights],
        ((nodes, 128), F32),
        ((edges, nodes), BF16), ((edges, nodes), BF16),
        ((nodes, edges), BF16), ((nodes, edges), BF16),
        node_shape, edge_shape, node_shape, raw_shape, *block_shapes,
    ]
    (wanted, readout, edge_in, edge_out, node_in, node_out,
     flat, recv, send, recv_t, send_t, h0, slope0, q0, raw, *blocks) = pl.pallas_call(
        functools.partial(first_kernel, chunk),
        out_shape=[jax.ShapeDtypeStruct(shape, dtype) for shape, dtype in shapes],
        in_specs=[pl.BlockSpec(memory_space=pltpu.HBM)] * len(sources),
        out_specs=[VMEM] * len(shapes),
        scratch_shapes=[
            pltpu.VMEM(node_feats.shape, F32),
            pltpu.VMEM(edge_index.shape, jnp.int32),
            pltpu.VMEM(halo_index.shape, jnp.int32),
            pltpu.SemaphoreType.DMA((len(sources),)),
        ],
        compiler_params=pltpu.CompilerParams(vmem_limit_bytes=16 * 2**20),
    )(*[pltpu.with_memory_space_constraint(source, pltpu.HBM) for source in sources])
    message = ((2 * size + EXTRA, width), F32)
    came = exchange(blocks)
    far_names = (names[0], 0, 0, 0)
    raws = exchange([raw], 1, 0)
    agg0, h1, act0, gate0, slope1, q1, pre, known, *messages = call(
        functools.partial(middle_kernel, chunk, names),
        [node_shape, node_shape, node_shape, node_shape, edge_shape, node_shape,
         node_shape, node_shape, *[message] * 4],
        *blocks, *came,
        h0, flat, wanted, readout, recv, send, recv_t, node_in, node_out, edge_in, edge_out,
    )
    came = exchange(messages)
    far_shapes = [
        ((size, width), F32), edge_shape, ((size, width), F32),
        ((edges, size), BF16), ((size, edges), BF16), ((edges, nodes), BF16), ((nodes, edges), BF16),
    ]
    fars = call(
        functools.partial(far_kernel, chunk, far_names, size), far_shapes * len(raws), *raws, edge_in
    )
    shared, far_slope, far_q, far_recv, far_recv_t, _, far_send_t = fars
    (agg1, act1, pre1, seed, local1, to_recv1, to_send1, top0, pre0, pred, loss,
     *blocks) = call(
        functools.partial(back_kernel, chunk, count, names),
        [*[node_shape] * 9, ((1, nodes), F32), ((1, width), F32), *block_shapes],
        *messages, *came,
        flat, readout, pre, known, gate0, recv, recv_t, send_t, slope1,
        edge_in, edge_out, node_in, node_out, far_q,
    )
    came = exchange(blocks, 4, 1)
    high, node_low, far, tail = call(
        functools.partial(grads_kernel, chunk=chunk),
        [((6 * width, width), F32), ((3 * width, width), F32), ((3 * width, width), F32),
         ((EXTRA, width), F32)],
        h0, agg0, act0, pre0, top0, h1, agg1, act1, pre1, seed, q1, local1, to_recv1, to_send1,
        readout, node_out, loss, blocks[0], *raws, shared, far_slope, far_q, far_recv, far_recv_t,
        far_send_t, edge_out,
    )
    rows = 6 * width
    groups = n_dom // 4
    half = ((rows + EXTRA, width), F32)
    end_grads = call(
        functools.partial(end_kernel, chunk, (0,) + names[1:]),
        [half, half],
        *blocks, *came, h0, q0, recv, recv_t, send_t, slope0, edge_out, node_low, high, far, tail,
    )
    if n_sub != 2 or n_dom % 4 or groups & (groups - 1) or rows % 32:
        return slow_tail(count, *end_grads, pred)
    per = rows // 4
    quarter = ((per + EXTRA, width), F32)
    mine, other = end_grads

    def swap(value):
        return lax.ppermute(value, "sub", pairs(n_sub, 0))

    def across(value, away):
        return lax.ppermute(value, "dom", [(at, at ^ away) for at in range(n_dom)])

    parts = call(quarters_kernel, [quarter] * 4, mine, swap(other))
    came = [across(parts[away], away) for away in (3, 2, 1)]
    (total,) = call(four_kernel, [quarter], parts[0], came[2], came[1], came[0])
    away = 4
    while away < n_dom // 2:
        (total,) = call(two_kernel, [quarter], total, across(total, away))
        away *= 2
    if away < n_dom:
        far = across(total, away)
    else:
        far = jnp.zeros_like(total)
    total, tail = call(
        last_sum_kernel, [((per, width), F32), ((EXTRA, width), F32)], total, far
    )
    near = [total] + [across(total, away) for away in range(1, 4)]
    far = [swap(value) for value in near]
    params = 2 * 6 * width * width + width
    loss, g_edge_in, g_edge_out, g_node_in, g_node_out, g_decoder = call(
        functools.partial(scale_kernel, params, count),
        [
            ((1, width), F32),
            ((2, 2 * width, width), F32), ((2, width, width), F32),
            ((2, 2 * width, width), F32), ((2, width, width), F32),
            ((1, width), F32),
        ],
        *near, *far, tail,
    )
    return (
        loss[0, 0], pred.reshape(nodes), g_edge_in, g_edge_out, g_node_in, g_node_out,
        g_decoder.reshape(width),
    )


def slow_tail(count, mine, other, pred):
    first = lax.axis_index("sub") == 0
    width = mine.shape[1]
    rows = mine.shape[0] - EXTRA
    high = jnp.where(first, mine, other)
    low = jnp.where(first, other, mine)
    total = lax.psum(jnp.concatenate([low[:rows], high], axis=0), ("dom", "sub"))
    body = total[: 2 * rows + 1]
    params = (2 * rows + 1) * width
    scale = 1.0 / jnp.sqrt(jnp.sum(body * body) / params + 1e-06)
    grads = (total[: 2 * rows] * scale).reshape(2, 2, 3 * width, width)
    return (
        total[2 * rows + 1, 0] / count, pred.reshape(-1),
        grads[:, 1, : 2 * width], grads[:, 1, 2 * width :],
        grads[:, 0, : 2 * width], grads[:, 0, 2 * width :],
        total[2 * rows] * scale,
    )


def solution(mesh):
    placed = (
        P(("dom", "sub"), None),
        P(),
        P(),
        P(),
        P(),
        P(),
        P(None, ("dom", "sub")),
        P(("dom", "sub"), None, None),
        P(("dom", "sub")),
    )
    return jax.shard_map(
        per_device,
        mesh=mesh,
        in_specs=placed,
        out_specs=(P(), P(("dom", "sub")), P(), P(), P(), P(), P()),
        check_vma=False,
    )
```

```python
import functools

import jax
import jax.numpy as jnp
from jax import lax
from jax.experimental import pallas as pl
from jax.experimental.pallas import tpu as pltpu
from jax.sharding import PartitionSpec as P


F32 = jnp.float32
BF16 = jnp.bfloat16
VMEM = pl.BlockSpec(memory_space=pltpu.VMEM)
EXTRA = 8


def halves(x):
    high = x.astype(BF16)
    low = (x - high.astype(F32)).astype(BF16)
    return high, low


def side(x):
    return jnp.concatenate(halves(x), axis=1)


def fold(x):
    width = x.shape[1] // 2
    return x[:, :width] + x[:, width:]


def dot(a, b, dims=((1,), (0,))):
    return lax.dot_general(a, b, (dims, ((), ())), preferred_element_type=F32)


def mm(x, w):
    wide = side(w)
    return fold(dot(side(x), jnp.concatenate([wide, wide], axis=0)))


def mmt(x, w):
    high, low = halves(w)
    both = jnp.concatenate(
        [jnp.concatenate([high, high], axis=1), jnp.concatenate([low, low], axis=1)], axis=0
    )
    return fold(dot(side(x), both, ((1,), (1,))))


def tmm(x, y):
    wide = fold(dot(side(x), side(y), ((0,), (0,))))
    width = x.shape[1]
    return wide[:width] + wide[width:]


def silu_parts(v):
    gate = 1.0 / (1.0 + jnp.exp(-v))
    return v * gate, gate * (1.0 + v * (1.0 - gate))


def row_of(column):
    n = column.shape[0]
    eye = lax.broadcasted_iota(jnp.int32, (n, n), 0) == lax.broadcasted_iota(jnp.int32, (n, n), 1)
    return jnp.sum(jnp.where(eye, column, 0.0), axis=0, keepdims=True)


def onehot(mask):
    return jnp.where(mask, 1.0, 0.0).astype(BF16)


def edge_forward(features, weight_in, recv, send, recv_t, slope_ref, chunk):
    width = features.shape[1]
    to_recv = side(mm(features, weight_in[:width]))
    to_send = side(mm(features, weight_in[width:]))
    total = None
    for start in range(0, recv.shape[0], chunk):
        rows = pl.ds(start, chunk)
        pre = fold(dot(recv[rows, :], to_recv) + dot(send[rows, :], to_send))
        act, slope = silu_parts(pre)
        slope_ref[rows, :] = slope
        part = dot(recv_t[:, rows], side(act))
        total = part if total is None else total + part
    return fold(total)


def edge_backward(local_grad, weight_out, recv, recv_t, send_t, slope_ref, chunk):
    spread = side(mmt(local_grad, weight_out))
    total_r = total_s = None
    for start in range(0, recv.shape[0], chunk):
        rows = pl.ds(start, chunk)
        grad = side(fold(dot(recv[rows, :], spread)) * slope_ref[rows, :])
        part_r = dot(recv_t[:, rows], grad)
        part_s = dot(send_t[:, rows], grad)
        total_r = part_r if total_r is None else total_r + part_r
        total_s = part_s if total_s is None else total_s + part_s
    return fold(total_r), fold(total_s)


def node_forward(features, summed, weight_in, weight_out):
    width = features.shape[1]
    pre = mm(features, weight_in[:width]) + mm(summed, weight_in[width:])
    act, slope = silu_parts(pre)
    return features + mm(act, weight_out), act, slope


def put_blocks(value, refs):
    size = refs[0].shape[0]
    for at, ref in enumerate(refs):
        ref[...] = value[at * size : (at + 1) * size]


AXES = ("dom", "dom", "sub", "sub")
OFFSETS = (1, 0, 0, 1)


def kept(at, value):
    if pairs(lax.axis_size(AXES[at]), OFFSETS[at])[1]:
        partner = jnp.bitwise_xor(lax.axis_index(AXES[at]) + OFFSETS[at], 1) - OFFSETS[at]
        there = jnp.logical_and(partner >= 0, partner < lax.axis_size(AXES[at]))
        return jnp.where(there, value, 0.0)
    return value


def take_sum(own, came):
    parts = [
        ref[...] + kept(at, came[at][...]) if came[at] is not None else ref[...]
        for at, ref in enumerate(own)
    ]
    return jnp.concatenate(parts, axis=0)


def even(axis):
    return lax.rem(lax.axis_index(axis), 2) == 0


def first_kernel(
    chunk, feats_hbm, index_hbm, halo_hbm, target_hbm, decoder_hbm, *refs
):
    weights_hbm, refs = refs[:4], refs[4:]
    (target, decoder, edge_in, edge_out, node_in, node_out,
     flat_out, recv, send, recv_t, send_t, h_out, slope, q_out, raw) = refs[:15]
    blocks, (feats, index, halo, sems) = refs[15:19], refs[19:]
    copies = [
        pltpu.make_async_copy(source, place, sems.at[at])
        for at, (source, place) in enumerate(
            zip(
                (index_hbm, halo_hbm, feats_hbm, *weights_hbm, target_hbm, decoder_hbm),
                (index, halo, feats, edge_in, edge_out, node_in, node_out, target, decoder),
            )
        )
    ]
    for copy in copies:
        copy.start()
    copies[0].wait()
    copies[1].wait()
    nodes = feats.shape[0]
    edges = index.shape[1]
    lanes = 128
    count = edges // lanes
    size = halo.shape[2]
    pieces = [index[0:1, pl.ds(b * lanes, lanes)] for b in range(count)]
    pieces += [index[1:2, pl.ds(b * lanes, lanes)] for b in range(count)]
    table = jnp.concatenate(pieces, axis=0).astype(F32)
    lists = jnp.concatenate([halo[0].astype(F32), jnp.zeros((4, lanes - size), F32)], axis=1)
    rest = jnp.zeros((lanes - 2 * count - 4, lanes), F32)
    columns = jnp.concatenate([table, lists, rest], axis=0).T
    by_dir = [columns[:size, 2 * count + k : 2 * count + k + 1] for k in range(4)]
    dom_even, sub_even = even("dom"), even("sub")
    flat = jnp.concatenate(
        [
            jnp.where(dom_even, by_dir[0], by_dir[1]),
            jnp.where(dom_even, by_dir[1], by_dir[0]),
            jnp.where(sub_even, by_dir[3], by_dir[2]),
            jnp.where(sub_even, by_dir[2], by_dir[3]),
        ],
        axis=0,
    )
    raw[nodes:, :] = jnp.concatenate(
        [
            table,
            jnp.where(dom_even, lists[0:1], lists[1:2]),
            jnp.where(dom_even, lists[1:2], lists[0:1]),
            jnp.where(sub_even, lists[3:4], lists[2:3]),
            jnp.where(sub_even, lists[2:3], lists[3:4]),
        ],
        axis=0,
    )
    flat_row = row_of(flat)
    flat_out[...] = jnp.broadcast_to(flat, flat_out.shape)
    for b in range(count):
        rows = pl.ds(b * lanes, lanes)
        recv[rows, :] = onehot(columns[:, b : b + 1] == flat_row)
        send[rows, :] = onehot(columns[:, count + b : count + b + 1] == flat_row)
        recv_t[:, rows] = onehot(flat == table[b : b + 1])
        send_t[:, rows] = onehot(flat == table[count + b : count + b + 1])
    place = onehot(flat == lax.broadcasted_iota(jnp.int32, (nodes, nodes), 1).astype(F32))
    copies[2].wait()
    plain = feats[...]
    raw[:nodes, :] = plain
    features = fold(dot(place, side(plain)))
    h_out[...] = features
    copies[3].wait()
    q = edge_forward(features, edge_in[0], recv, send, recv_t, slope, chunk)
    q_out[...] = q
    copies[4].wait()
    put_blocks(mm(q, edge_out[0]), blocks)
    for copy in copies[5:]:
        copy.wait()


def unpack(names, refs):
    came = []
    at = 0
    for there in names:
        came.append(refs[at] if there else None)
        at += there
    return came, refs[at:]


def middle_kernel(chunk, names, *refs):
    own, refs = refs[:4], refs[4:]
    came, refs = unpack(names, refs)
    (h, flat_ref, target, decoder, recv, send, recv_t, node_in, node_out, edge_in, edge_out,
     agg_out, h_out, node_act, node_slope, slope, q_out, pre_out, known_out, *messages) = refs
    nodes, width = h.shape
    summed = take_sum(own, came)
    agg_out[...] = summed
    features, act, gate = node_forward(h[...], summed, node_in[0], node_out[0])
    h_out[...] = features
    node_act[...] = act
    node_slope[...] = gate
    pre = mm(features, node_in[1, :width])
    pre_out[...] = pre
    base = jnp.sum(features * decoder[...], axis=1, keepdims=True)
    here = flat_ref[:, 0:1] == lax.broadcasted_iota(jnp.int32, (nodes, nodes), 1).astype(F32)
    wanted = jnp.sum(jnp.where(here, target[...], 0.0), axis=1, keepdims=True)
    first = lax.broadcasted_iota(jnp.int32, (nodes, width), 1) == 0
    known_out[...] = jnp.where(first, base, wanted)
    size = own[0].shape[0]
    short = base - wanted
    for at, message in enumerate(messages):
        rows = slice(at * size, (at + 1) * size)
        message[size : 2 * size, :] = pre[rows]
        line = row_of(short[rows])
        line = jnp.concatenate([line, jnp.zeros((1, width - size), F32)], axis=1)
        message[2 * size :, :] = jnp.concatenate(
            [line, jnp.zeros((EXTRA - 1, width), F32)], axis=0
        )
    q = edge_forward(features, edge_in[1], recv, send, recv_t, slope, chunk)
    q_out[...] = q
    local = mm(q, edge_out[1])
    for at, message in enumerate(messages):
        message[:size, :] = local[at * size : (at + 1) * size]


def column_of(row):
    n = row.shape[1]
    eye = lax.broadcasted_iota(jnp.int32, (n, n), 0) == lax.broadcasted_iota(jnp.int32, (n, n), 1)
    return jnp.sum(jnp.where(eye, row, 0.0), axis=1, keepdims=True)


def row_product(row, weight):
    return mm(jnp.broadcast_to(row, (8, row.shape[1])), weight)[0:1]


def back_kernel(chunk, count, names, *refs):
    own, refs = refs[:4], refs[4:]
    came, refs = unpack(names, refs)
    (flat_ref, decoder, pre_ref, known, node_slope, recv, recv_t, send_t, slope,
     edge_in, edge_out, node_in, node_out, _,
     agg_out, act_out, pre1_out, seed_out, local_out, recv_out, send_out, top_out, pre0_out,
     pred_out, loss_out, *blocks) = refs
    nodes, width = pre_ref.shape
    size = blocks[0].shape[0]
    summed = jnp.concatenate(
        [
            ref[:size, :] + kept(at, came[at][:size, :]) if came[at] is not None else ref[:size, :]
            for at, ref in enumerate(own)
        ],
        axis=0,
    )
    agg_out[...] = summed
    pre_agg = mm(summed, node_in[1, width:])
    act, gate = silu_parts(pre_ref[...] + pre_agg)
    act_out[...] = act
    weights = decoder[...]
    lead = row_of(jnp.sum(node_out[1] * weights, axis=1, keepdims=True))
    base, wanted = known[:, 0:1], known[:, 1:2]
    predicted = base + jnp.sum(act * lead, axis=1, keepdims=True)
    misfit = predicted - wanted
    seed = 2.0 * misfit / count
    seed_out[...] = jnp.broadcast_to(seed, seed_out.shape)
    here = flat_ref[:, 0:1] == lax.broadcasted_iota(jnp.int32, (nodes, nodes), 1).astype(F32)
    pred_out[...] = jnp.sum(jnp.where(here, predicted, 0.0), axis=0, keepdims=True)
    loss_out[...] = jnp.broadcast_to(
        jnp.sum(misfit * misfit, axis=0, keepdims=True), loss_out.shape
    )
    pre_grad = seed * lead * gate
    pre1_out[...] = pre_grad
    shared = []
    for at in range(4):
        rows = slice(at * size, (at + 1) * size)
        if came[at] is None:
            shared.append(pre_grad[rows])
            continue
        far_act, far_gate = silu_parts(came[at][size : 2 * size, :] + pre_agg[rows])
        far_misfit = column_of(came[at][2 * size : 2 * size + 1, :size])
        far_misfit = far_misfit + jnp.sum(far_act * lead, axis=1, keepdims=True)
        far_seed = kept(at, 2.0 * far_misfit / count)
        shared.append(pre_grad[rows] + far_seed * lead * far_gate)
    local_grad = mmt(jnp.concatenate(shared, axis=0), node_in[1, width:])
    local_out[...] = local_grad
    to_recv, to_send = edge_backward(local_grad, edge_out[1], recv, recv_t, send_t, slope, chunk)
    recv_out[...] = to_recv
    send_out[...] = to_send
    top = (
        seed * weights
        + mmt(pre_grad, node_in[1, :width])
        + mmt(to_recv, edge_in[1, :width])
        + mmt(to_send, edge_in[1, width:])
    )
    top_out[...] = top
    pre0 = mmt(top, node_out[0]) * node_slope[...]
    pre0_out[...] = pre0
    put_blocks(mmt(pre0, node_in[0, width:]), blocks)


def grads_kernel(
    h0, agg0, act0, pre0, top0, h1, agg1, act1, pre1, seed, q1, local1, to_recv1, to_send1,
    decoder, node_out, loss, block, raw, shared, far_slope, far_q, far_recv, far_recv_t, far_send_t,
    edge_out, high, low, far, tail, *, chunk
):
    width = h0.shape[1]
    rows = seed[...]
    top1 = rows * decoder[...]
    act = act1[...]
    parts = [
        tmm(h1[...], pre1[...]),
        tmm(agg1[...], pre1[...]),
        tmm(act, top1),
        tmm(h1[...], to_recv1[...]),
        tmm(h1[...], to_send1[...]),
        tmm(q1[...], local1[...]),
    ]
    for at, part in enumerate(parts):
        high[at * width : (at + 1) * width, :] = part
    low[0:width, :] = tmm(h0[...], pre0[...])
    low[width : 2 * width, :] = tmm(agg0[...], pre0[...])
    low[2 * width :, :] = tmm(act0[...], top0[...])
    far_grad = kept(0, block[...])
    to_recv, to_send = edge_backward(
        far_grad, edge_out[0], far_recv, far_recv_t, far_send_t, far_slope, chunk
    )
    far[0:width, :] = tmm(shared[...], to_recv)
    far[width : 2 * width, :] = tmm(raw[: h0.shape[0], :], to_send)
    far[2 * width :, :] = tmm(far_q[...], far_grad)
    line = jnp.sum(rows * h1[...], axis=0, keepdims=True)
    line = line + row_product(jnp.sum(rows * act, axis=0, keepdims=True), node_out[1])
    tail[...] = jnp.concatenate([line, loss[...], jnp.zeros((EXTRA - 2, width), F32)], axis=0)


def far_kernel(chunk, names, size, *refs):
    raws, refs = unpack(names, refs)
    edge_in, refs = refs[0], refs[1:]
    at = 0
    for place, raw in enumerate(raws):
        if raw is None:
            continue
        shared_out, slope, q_out, recv, recv_t, send, send_t = refs[at : at + 7]
        at += 7
        edges, width = slope.shape
        nodes = send_t.shape[0]
        count = edges // width
        block = jnp.concatenate(
            [raw[nodes:, :], jnp.zeros((width + nodes - raw.shape[0], width), F32)], axis=0
        )
        columns = block.T
        own = block[2 * count + place : 2 * count + place + 1, :size]
        down = columns[:size, 2 * count + place : 2 * count + place + 1]
        along = lax.broadcasted_iota(jnp.int32, (1, nodes), 1).astype(F32)
        across = lax.broadcasted_iota(jnp.int32, (nodes, 1), 0).astype(F32)
        for b in range(count):
            rows = pl.ds(b * width, width)
            recv[rows, :] = onehot(columns[:, b : b + 1] == own)
            send[rows, :] = onehot(columns[:, count + b : count + b + 1] == along)
            recv_t[:, rows] = onehot(down == block[b : b + 1])
            send_t[:, rows] = onehot(across == block[count + b : count + b + 1])
        features = raw[:nodes, :]
        shared = fold(dot(onehot(down == along), side(features)))
        shared_out[...] = shared
        to_recv = side(mm(shared, edge_in[0, :width]))
        to_send = side(mm(features, edge_in[0, width:]))
        total = None
        for start in range(0, edges, chunk):
            rows = pl.ds(start, chunk)
            pre = fold(dot(recv[rows, :], to_recv) + dot(send[rows, :], to_send))
            act, rise = silu_parts(pre)
            slope[rows, :] = rise
            part = dot(recv_t[:, rows], side(act))
            total = part if total is None else total + part
        q_out[...] = fold(total)


def put_rows(ref, at, value):
    ref[at : at + value.shape[0], :] = value
    return at + value.shape[0]


def end_kernel(chunk, names, *refs):
    own, refs = refs[:4], refs[4:]
    came, refs = unpack(names, refs)
    h, q, recv, recv_t, send_t, slope, edge_out, node_low, high, far, tail, mine, other = refs
    local_grad = take_sum(own, came)
    to_recv, to_send = edge_backward(local_grad, edge_out[0], recv, recv_t, send_t, slope, chunk)
    width = h.shape[1]
    low = [
        node_low[...],
        tmm(h[...], to_recv) + far[0:width, :],
        tmm(h[...], to_send) + far[width : 2 * width, :],
        tmm(q[...], local_grad) + far[2 * width :, :],
        tail[...],
    ]

    def write(ref_high, ref_low):
        at = 0
        for value in low:
            at = put_rows(ref_low, at, value)
        put_rows(ref_high, put_rows(ref_high, 0, high[...]), tail[...])

    first = lax.axis_index("sub") == 0
    pl.when(first)(lambda: write(mine, other))
    pl.when(jnp.logical_not(first))(lambda: write(other, mine))


def quarters_kernel(mine, other, *outs):
    per = outs[0].shape[0] - EXTRA
    own = lax.rem(lax.axis_index("dom"), 4)
    tail = mine[4 * per :, :] + other[4 * per :, :]
    for away, out in enumerate(outs):
        rows = pl.ds(pl.multiple_of(jnp.bitwise_xor(own, away) * per, 8), per)
        out[:per, :] = mine[rows, :] + other[rows, :]
        out[per:, :] = tail


def four_kernel(a, b, c, d, out):
    out[...] = (a[...] + b[...]) + (c[...] + d[...])


def two_kernel(a, b, out):
    out[...] = a[...] + b[...]


def last_sum_kernel(a, b, out, tail):
    per = out.shape[0]
    out[...] = a[:per, :] + b[:per, :]
    tail[...] = a[per:, :] + b[per:, :]


def scale_kernel(params, count, *refs):
    near, far = refs[:4], refs[4:8]
    tail, loss, edge_in, edge_out, node_in, node_out, decoder = refs[8:]
    width = tail.shape[1]
    line = tail[0:1]
    squares = []
    for group in (near, far):
        sums = [jnp.sum(ref[...] * ref[...], axis=0, keepdims=True) for ref in group]
        squares.append((sums[0] + sums[1]) + (sums[2] + sums[3]))
    every = jnp.sum(squares[0] + squares[1] + line * line, axis=1, keepdims=True)
    scale = 1.0 / jnp.sqrt(every / params + 1e-06)
    decoder[...] = line * scale
    loss[...] = tail[1:2] / count
    where = [(node_in, at) for at in range(2)] + [(node_out, 0)]
    where = where + [(edge_in, at) for at in range(2)] + [(edge_out, 0)]

    def write(own, layer, group):
        per = group[0].shape[0]
        for quarter in range(4):
            ref = group[quarter ^ own]
            at = 0
            while at < per:
                block, inside = divmod(quarter * per + at, width)
                take = min(width - inside, per - at)
                out, half = where[block]
                first = half * width + inside
                out[layer, first : first + take, :] = ref[at : at + take, :] * scale
                at += take

    here = lax.rem(lax.axis_index("dom"), 4)
    side_here = lax.axis_index("sub")
    for own in range(4):
        for core in range(2):
            def both(own=own, core=core):
                write(own, 1 - core, near)
                write(own, core, far)

            pl.when(jnp.logical_and(here == own, side_here == core))(both)


def call(kernel, outs, *args):
    shapes = [jax.ShapeDtypeStruct(shape, dtype) for shape, dtype in outs]
    return pl.pallas_call(
        kernel,
        out_shape=shapes,
        in_specs=[VMEM] * len(args),
        out_specs=[VMEM] * len(shapes),
        compiler_params=pltpu.CompilerParams(vmem_limit_bytes=16 * 2**20),
    )(*args)


def pairs(count, offset):
    found = []
    for low in range(offset, count - 1, 2):
        found += [(low, low + 1), (low + 1, low)]
    paired = [source for source, _ in found]
    return found, [at for at in range(count) if found and at not in paired]


def moves(n_dom, n_sub, at):
    along, other = (n_dom, n_sub) if AXES[at] == "dom" else (n_sub, n_dom)
    found, alone = pairs(along, OFFSETS[at])

    def spot(here, there):
        return here * n_sub + there if AXES[at] == "dom" else there * n_sub + here

    listed = []
    for there in range(other):
        listed += [(spot(source, there), spot(target, there)) for source, target in found]
        beside = there if other % 2 else there ^ 1
        listed += [(spot(end, there), spot(end, beside)) for end in alone]
    return listed


def per_device(
    node_feats, edge_in, edge_out, node_in, node_out, decoder, edge_index, halo_index, target
):
    nodes, width = node_feats.shape
    edges = edge_index.shape[1]
    size = halo_index.shape[2]
    n_dom, n_sub = lax.axis_size("dom"), lax.axis_size("sub")
    count = nodes * n_dom * n_sub
    if n_dom < 3 or edge_in.shape[0] != 2 or 4 * size != nodes:
        raise ValueError("unsupported sizes")
    chunk = 256
    links = [moves(n_dom, n_sub, at) for at in range(4)]
    names = tuple(1 if link else 0 for link in links)

    def exchange(blocks, last=4, first=0):
        came = [None] * 4
        for at in range(first, last):
            if links[at]:
                came[at] = lax.ppermute(blocks[at], ("dom", "sub"), links[at])
        return [block for block in came if block is not None]

    node_shape = ((nodes, width), F32)
    edge_shape = ((edges, width), F32)
    block_shapes = [((size, width), F32)] * 4

    weights = (edge_in, edge_out, node_in, node_out)
    sources = (
        node_feats, edge_index, halo_index, target.reshape(1, nodes), decoder.reshape(1, width),
        *weights,
    )
    raw_shape = ((nodes + 2 * edges // width + 4, width), F32)
    shapes = [
        ((1, nodes), F32), ((1, width), F32), *[(weight.shape, F32) for weight in weights],
        ((nodes, 128), F32),
        ((edges, nodes), BF16), ((edges, nodes), BF16),
        ((nodes, edges), BF16), ((nodes, edges), BF16),
        node_shape, edge_shape, node_shape, raw_shape, *block_shapes,
    ]
    (wanted, readout, edge_in, edge_out, node_in, node_out,
     flat, recv, send, recv_t, send_t, h0, slope0, q0, raw, *blocks) = pl.pallas_call(
        functools.partial(first_kernel, chunk),
        out_shape=[jax.ShapeDtypeStruct(shape, dtype) for shape, dtype in shapes],
        in_specs=[pl.BlockSpec(memory_space=pltpu.HBM)] * len(sources),
        out_specs=[VMEM] * len(shapes),
        scratch_shapes=[
            pltpu.VMEM(node_feats.shape, F32),
            pltpu.VMEM(edge_index.shape, jnp.int32),
            pltpu.VMEM(halo_index.shape, jnp.int32),
            pltpu.SemaphoreType.DMA((len(sources),)),
        ],
        compiler_params=pltpu.CompilerParams(vmem_limit_bytes=16 * 2**20),
    )(*[pltpu.with_memory_space_constraint(source, pltpu.HBM) for source in sources])
    message = ((2 * size + EXTRA, width), F32)
    came = exchange(blocks)
    far_names = (names[0], 0, 0, 0)
    raws = exchange([raw], 1, 0)
    agg0, h1, act0, gate0, slope1, q1, pre, known, *messages = call(
        functools.partial(middle_kernel, chunk, names),
        [node_shape, node_shape, node_shape, node_shape, edge_shape, node_shape,
         node_shape, node_shape, *[message] * 4],
        *blocks, *came,
        h0, flat, wanted, readout, recv, send, recv_t, node_in, node_out, edge_in, edge_out,
    )
    came = exchange(messages)
    far_shapes = [
        ((size, width), F32), edge_shape, ((size, width), F32),
        ((edges, size), BF16), ((size, edges), BF16), ((edges, nodes), BF16), ((nodes, edges), BF16),
    ]
    fars = call(
        functools.partial(far_kernel, chunk, far_names, size), far_shapes * len(raws), *raws, edge_in
    )
    shared, far_slope, far_q, far_recv, far_recv_t, _, far_send_t = fars
    (agg1, act1, pre1, seed, local1, to_recv1, to_send1, top0, pre0, pred, loss,
     *blocks) = call(
        functools.partial(back_kernel, chunk, count, names),
        [*[node_shape] * 9, ((1, nodes), F32), ((1, width), F32), *block_shapes],
        *messages, *came,
        flat, readout, pre, known, gate0, recv, recv_t, send_t, slope1,
        edge_in, edge_out, node_in, node_out, far_q,
    )
    came = exchange(blocks, 4, 1)
    high, node_low, far, tail = call(
        functools.partial(grads_kernel, chunk=chunk),
        [((6 * width, width), F32), ((3 * width, width), F32), ((3 * width, width), F32),
         ((EXTRA, width), F32)],
        h0, agg0, act0, pre0, top0, h1, agg1, act1, pre1, seed, q1, local1, to_recv1, to_send1,
        readout, node_out, loss, blocks[0], *raws, shared, far_slope, far_q, far_recv, far_recv_t,
        far_send_t, edge_out,
    )
    rows = 6 * width
    groups = n_dom // 4
    half = ((rows + EXTRA, width), F32)
    end_grads = call(
        functools.partial(end_kernel, chunk, (0,) + names[1:]),
        [half, half],
        *blocks, *came, h0, q0, recv, recv_t, send_t, slope0, edge_out, node_low, high, far, tail,
    )
    if n_sub != 2 or n_dom % 4 or groups & (groups - 1) or rows % 32:
        return slow_tail(count, *end_grads, pred)
    per = rows // 4
    quarter = ((per + EXTRA, width), F32)
    mine, other = end_grads

    def swap(value):
        return lax.ppermute(value, "sub", pairs(n_sub, 0)[0])

    def across(value, away):
        return lax.ppermute(value, "dom", [(at, at ^ away) for at in range(n_dom)])

    def beside(value, first, second):
        moves = [
            (at * n_sub + core, (at ^ away) * n_sub + core)
            for at in range(n_dom)
            for core, away in enumerate((first, second))
        ]
        return lax.ppermute(value, ("dom", "sub"), moves)

    parts = call(quarters_kernel, [quarter] * 4, mine, swap(other))
    came = [across(parts[away], away) for away in (3, 2, 1)]
    (total,) = call(four_kernel, [quarter], parts[0], came[2], came[1], came[0])
    aways = [4 << at for at in range(groups.bit_length() - 1)]
    for step in range(len(aways) - 1):
        (total,) = call(two_kernel, [quarter], total, beside(total, aways[step], aways[-1 - step]))
    far = beside(total, aways[-1], aways[0]) if aways else jnp.zeros_like(total)
    total, tail = call(
        last_sum_kernel, [((per, width), F32), ((EXTRA, width), F32)], total, far
    )
    near = [total] + [across(total, away) for away in range(1, 4)]
    far = [swap(value) for value in near]
    params = 2 * 6 * width * width + width
    loss, g_edge_in, g_edge_out, g_node_in, g_node_out, g_decoder = call(
        functools.partial(scale_kernel, params, count),
        [
            ((1, width), F32),
            ((2, 2 * width, width), F32), ((2, width, width), F32),
            ((2, 2 * width, width), F32), ((2, width, width), F32),
            ((1, width), F32),
        ],
        *near, *far, tail,
    )
    return (
        loss[0, 0], pred.reshape(nodes), g_edge_in, g_edge_out, g_node_in, g_node_out,
        g_decoder.reshape(width),
    )


def slow_tail(count, mine, other, pred):
    first = lax.axis_index("sub") == 0
    width = mine.shape[1]
    rows = mine.shape[0] - EXTRA
    high = jnp.where(first, mine, other)
    low = jnp.where(first, other, mine)
    total = lax.psum(jnp.concatenate([low[:rows], high], axis=0), ("dom", "sub"))
    body = total[: 2 * rows + 1]
    params = (2 * rows + 1) * width
    scale = 1.0 / jnp.sqrt(jnp.sum(body * body) / params + 1e-06)
    grads = (total[: 2 * rows] * scale).reshape(2, 2, 3 * width, width)
    return (
        total[2 * rows + 1, 0] / count, pred.reshape(-1),
        grads[:, 1, : 2 * width], grads[:, 1, 2 * width :],
        grads[:, 0, : 2 * width], grads[:, 0, 2 * width :],
        total[2 * rows] * scale,
    )


def solution(mesh):
    placed = (
        P(("dom", "sub"), None),
        P(),
        P(),
        P(),
        P(),
        P(),
        P(None, ("dom", "sub")),
        P(("dom", "sub"), None, None),
        P(("dom", "sub")),
    )
    return jax.shard_map(
        per_device,
        mesh=mesh,
        in_specs=placed,
        out_specs=(P(), P(("dom", "sub")), P(), P(), P(), P(), P()),
        check_vma=False,
    )
```

```python
import functools

import jax
import jax.numpy as jnp
from jax import lax
from jax.experimental import pallas as pl
from jax.experimental.pallas import tpu as pltpu
from jax.sharding import PartitionSpec as P


F32 = jnp.float32
BF16 = jnp.bfloat16
VMEM = pl.BlockSpec(memory_space=pltpu.VMEM)
EXTRA = 8


def halves(x):
    high = x.astype(BF16)
    low = (x - high.astype(F32)).astype(BF16)
    return high, low


def side(x):
    return jnp.concatenate(halves(x), axis=1)


def fold(x):
    width = x.shape[1] // 2
    return x[:, :width] + x[:, width:]


def dot(a, b, dims=((1,), (0,))):
    return lax.dot_general(a, b, (dims, ((), ())), preferred_element_type=F32)


def mm(x, w):
    wide = side(w)
    return fold(dot(side(x), jnp.concatenate([wide, wide], axis=0)))


def mmt(x, w):
    high, low = halves(w)
    both = jnp.concatenate(
        [jnp.concatenate([high, high], axis=1), jnp.concatenate([low, low], axis=1)], axis=0
    )
    return fold(dot(side(x), both, ((1,), (1,))))


def tmm(x, y):
    wide = fold(dot(side(x), side(y), ((0,), (0,))))
    width = x.shape[1]
    return wide[:width] + wide[width:]


def silu_parts(v):
    gate = 1.0 / (1.0 + jnp.exp(-v))
    return v * gate, gate * (1.0 + v * (1.0 - gate))


def row_of(column):
    n = column.shape[0]
    eye = lax.broadcasted_iota(jnp.int32, (n, n), 0) == lax.broadcasted_iota(jnp.int32, (n, n), 1)
    return jnp.sum(jnp.where(eye, column, 0.0), axis=0, keepdims=True)


def onehot(left, right):
    return jnp.where(left.astype(BF16) == right.astype(BF16), BF16(1), BF16(0))


def edge_forward(features, weight_in, recv, send, recv_t, slope_ref, chunk):
    width = features.shape[1]
    to_recv = side(mm(features, weight_in[:width]))
    to_send = side(mm(features, weight_in[width:]))
    total = None
    for start in range(0, recv.shape[0], chunk):
        rows = pl.ds(start, chunk)
        pre = fold(dot(recv[rows, :], to_recv) + dot(send[rows, :], to_send))
        act, slope = silu_parts(pre)
        slope_ref[rows, :] = slope
        part = dot(recv_t[:, rows], side(act))
        total = part if total is None else total + part
    return fold(total)


def edge_backward(local_grad, weight_out, recv, recv_t, send_t, slope_ref, chunk):
    spread = side(mmt(local_grad, weight_out))
    total_r = total_s = None
    for start in range(0, recv.shape[0], chunk):
        rows = pl.ds(start, chunk)
        grad = side(fold(dot(recv[rows, :], spread)) * slope_ref[rows, :])
        part_r = dot(recv_t[:, rows], grad)
        part_s = dot(send_t[:, rows], grad)
        total_r = part_r if total_r is None else total_r + part_r
        total_s = part_s if total_s is None else total_s + part_s
    return fold(total_r), fold(total_s)


def node_forward(features, summed, weight_in, weight_out):
    width = features.shape[1]
    pre = mm(features, weight_in[:width]) + mm(summed, weight_in[width:])
    act, slope = silu_parts(pre)
    return features + mm(act, weight_out), act, slope


def put_blocks(value, refs):
    size = refs[0].shape[0]
    for at, ref in enumerate(refs):
        ref[...] = value[at * size : (at + 1) * size]


AXES = ("dom", "dom", "sub", "sub")
OFFSETS = (1, 0, 0, 1)


def kept(at, value):
    if pairs(lax.axis_size(AXES[at]), OFFSETS[at])[1]:
        partner = jnp.bitwise_xor(lax.axis_index(AXES[at]) + OFFSETS[at], 1) - OFFSETS[at]
        there = jnp.logical_and(partner >= 0, partner < lax.axis_size(AXES[at]))
        return jnp.where(there, value, 0.0)
    return value


def take_sum(own, came):
    parts = [
        ref[...] + kept(at, came[at][...]) if came[at] is not None else ref[...]
        for at, ref in enumerate(own)
    ]
    return jnp.concatenate(parts, axis=0)


def even(axis):
    return lax.rem(lax.axis_index(axis), 2) == 0


def first_kernel(
    chunk, feats_hbm, index_hbm, halo_hbm, target_hbm, decoder_hbm, *refs
):
    weights_hbm, refs = refs[:4], refs[4:]
    (target, decoder, edge_in, edge_out, node_in, node_out,
     flat_out, recv, send, recv_t, h_out, slope, q_out, raw) = refs[:14]
    blocks, (feats, index, halo, sems) = refs[14:18], refs[18:]
    copies = [
        pltpu.make_async_copy(source, place, sems.at[at])
        for at, (source, place) in enumerate(
            zip(
                (index_hbm, halo_hbm, feats_hbm, *weights_hbm, target_hbm, decoder_hbm),
                (index, halo, feats, edge_in, edge_out, node_in, node_out, target, decoder),
            )
        )
    ]
    for copy in copies:
        copy.start()
    copies[0].wait()
    copies[1].wait()
    nodes = feats.shape[0]
    edges = index.shape[1]
    lanes = 128
    count = edges // lanes
    size = halo.shape[2]
    pieces = [index[0:1, pl.ds(b * lanes, lanes)] for b in range(count)]
    pieces += [index[1:2, pl.ds(b * lanes, lanes)] for b in range(count)]
    table = jnp.concatenate(pieces, axis=0).astype(F32)
    lists = jnp.concatenate([halo[0].astype(F32), jnp.zeros((4, lanes - size), F32)], axis=1)
    rest = jnp.zeros((lanes - 2 * count - 4, lanes), F32)
    columns = jnp.concatenate([table, lists, rest], axis=0).T
    by_dir = [columns[:size, 2 * count + k : 2 * count + k + 1] for k in range(4)]
    dom_even, sub_even = even("dom"), even("sub")
    flat = jnp.concatenate(
        [
            jnp.where(dom_even, by_dir[0], by_dir[1]),
            jnp.where(dom_even, by_dir[1], by_dir[0]),
            jnp.where(sub_even, by_dir[3], by_dir[2]),
            jnp.where(sub_even, by_dir[2], by_dir[3]),
        ],
        axis=0,
    )
    raw[nodes:, :] = jnp.concatenate(
        [
            table,
            jnp.where(dom_even, lists[0:1], lists[1:2]),
            jnp.where(dom_even, lists[1:2], lists[0:1]),
            jnp.where(sub_even, lists[3:4], lists[2:3]),
            jnp.where(sub_even, lists[2:3], lists[3:4]),
        ],
        axis=0,
    )
    flat_row = row_of(flat)
    flat_out[...] = jnp.broadcast_to(flat, flat_out.shape)
    for b in range(count):
        rows = pl.ds(b * lanes, lanes)
        recv[rows, :] = onehot(columns[:, b : b + 1], flat_row)
        send[rows, :] = onehot(columns[:, count + b : count + b + 1], flat_row)
        recv_t[:, rows] = onehot(flat, table[b : b + 1])
    place = onehot(flat, lax.broadcasted_iota(jnp.int32, (1, nodes), 1).astype(F32))
    copies[2].wait()
    plain = feats[...]
    raw[:nodes, :] = plain
    features = fold(dot(place, side(plain)))
    h_out[...] = features
    copies[3].wait()
    q = edge_forward(features, edge_in[0], recv, send, recv_t, slope, chunk)
    q_out[...] = q
    copies[4].wait()
    put_blocks(mm(q, edge_out[0]), blocks)
    for copy in copies[5:]:
        copy.wait()


def unpack(names, refs):
    came = []
    at = 0
    for there in names:
        came.append(refs[at] if there else None)
        at += there
    return came, refs[at:]


def middle_kernel(chunk, names, *refs):
    own, refs = refs[:4], refs[4:]
    came, refs = unpack(names, refs)
    (h, flat_ref, target, decoder, recv, send, recv_t, node_in, node_out, edge_in, edge_out,
     agg_out, h_out, node_act, node_slope, slope, q_out, pre_out, known_out, *messages) = refs
    nodes, width = h.shape
    summed = take_sum(own, came)
    agg_out[...] = summed
    features, act, gate = node_forward(h[...], summed, node_in[0], node_out[0])
    h_out[...] = features
    node_act[...] = act
    node_slope[...] = gate
    pre = mm(features, node_in[1, :width])
    pre_out[...] = pre
    base = jnp.sum(features * decoder[...], axis=1, keepdims=True)
    here = flat_ref[:, 0:1] == lax.broadcasted_iota(jnp.int32, (nodes, nodes), 1).astype(F32)
    wanted = jnp.sum(jnp.where(here, target[...], 0.0), axis=1, keepdims=True)
    first = lax.broadcasted_iota(jnp.int32, (nodes, width), 1) == 0
    known_out[...] = jnp.where(first, base, wanted)
    size = own[0].shape[0]
    short = base - wanted
    for at, message in enumerate(messages):
        rows = slice(at * size, (at + 1) * size)
        message[size : 2 * size, :] = pre[rows]
        line = row_of(short[rows])
        line = jnp.concatenate([line, jnp.zeros((1, width - size), F32)], axis=1)
        message[2 * size :, :] = jnp.concatenate(
            [line, jnp.zeros((EXTRA - 1, width), F32)], axis=0
        )
    q = edge_forward(features, edge_in[1], recv, send, recv_t, slope, chunk)
    q_out[...] = q
    local = mm(q, edge_out[1])
    for at, message in enumerate(messages):
        message[:size, :] = local[at * size : (at + 1) * size]


def column_of(row):
    n = row.shape[1]
    eye = lax.broadcasted_iota(jnp.int32, (n, n), 0) == lax.broadcasted_iota(jnp.int32, (n, n), 1)
    return jnp.sum(jnp.where(eye, row, 0.0), axis=1, keepdims=True)


def row_product(row, weight):
    return mm(jnp.broadcast_to(row, (8, row.shape[1])), weight)[0:1]


def back_kernel(chunk, count, names, *refs):
    own, refs = refs[:4], refs[4:]
    came, refs = unpack(names, refs)
    (flat_ref, decoder, pre_ref, known, node_slope, recv, recv_t, send_t, slope,
     edge_in, edge_out, node_in, node_out, _,
     agg_out, act_out, pre1_out, seed_out, local_out, recv_out, send_out, top_out, pre0_out,
     pred_out, loss_out, *blocks) = refs
    nodes, width = pre_ref.shape
    size = blocks[0].shape[0]
    summed = jnp.concatenate(
        [
            ref[:size, :] + kept(at, came[at][:size, :]) if came[at] is not None else ref[:size, :]
            for at, ref in enumerate(own)
        ],
        axis=0,
    )
    agg_out[...] = summed
    pre_agg = mm(summed, node_in[1, width:])
    act, gate = silu_parts(pre_ref[...] + pre_agg)
    act_out[...] = act
    weights = decoder[...]
    lead = row_of(jnp.sum(node_out[1] * weights, axis=1, keepdims=True))
    base, wanted = known[:, 0:1], known[:, 1:2]
    predicted = base + jnp.sum(act * lead, axis=1, keepdims=True)
    misfit = predicted - wanted
    seed = 2.0 * misfit / count
    seed_out[...] = jnp.broadcast_to(seed, seed_out.shape)
    here = flat_ref[:, 0:1] == lax.broadcasted_iota(jnp.int32, (nodes, nodes), 1).astype(F32)
    pred_out[...] = jnp.sum(jnp.where(here, predicted, 0.0), axis=0, keepdims=True)
    loss_out[...] = jnp.broadcast_to(
        jnp.sum(misfit * misfit, axis=0, keepdims=True), loss_out.shape
    )
    pre_grad = seed * lead * gate
    pre1_out[...] = pre_grad
    shared = []
    for at in range(4):
        rows = slice(at * size, (at + 1) * size)
        if came[at] is None:
            shared.append(pre_grad[rows])
            continue
        far_act, far_gate = silu_parts(came[at][size : 2 * size, :] + pre_agg[rows])
        far_misfit = column_of(came[at][2 * size : 2 * size + 1, :size])
        far_misfit = far_misfit + jnp.sum(far_act * lead, axis=1, keepdims=True)
        far_seed = kept(at, 2.0 * far_misfit / count)
        shared.append(pre_grad[rows] + far_seed * lead * far_gate)
    local_grad = mmt(jnp.concatenate(shared, axis=0), node_in[1, width:])
    local_out[...] = local_grad
    to_recv, to_send = edge_backward(local_grad, edge_out[1], recv, recv_t, send_t, slope, chunk)
    recv_out[...] = to_recv
    send_out[...] = to_send
    top = (
        seed * weights
        + mmt(pre_grad, node_in[1, :width])
        + mmt(to_recv, edge_in[1, :width])
        + mmt(to_send, edge_in[1, width:])
    )
    top_out[...] = top
    pre0 = mmt(top, node_out[0]) * node_slope[...]
    pre0_out[...] = pre0
    put_blocks(mmt(pre0, node_in[0, width:]), blocks)


def grads_kernel(
    h0, agg0, act0, pre0, top0, h1, agg1, act1, pre1, seed, q1, local1, to_recv1, to_send1,
    decoder, node_out, loss, block, raw, shared, far_slope, far_q, far_recv, far_recv_t, far_send_t,
    edge_out, high, low, far, tail, *, chunk
):
    width = h0.shape[1]
    rows = seed[...]
    top1 = rows * decoder[...]
    act = act1[...]
    parts = [
        tmm(h1[...], pre1[...]),
        tmm(agg1[...], pre1[...]),
        tmm(act, top1),
        tmm(h1[...], to_recv1[...]),
        tmm(h1[...], to_send1[...]),
        tmm(q1[...], local1[...]),
    ]
    for at, part in enumerate(parts):
        high[at * width : (at + 1) * width, :] = part
    low[0:width, :] = tmm(h0[...], pre0[...])
    low[width : 2 * width, :] = tmm(agg0[...], pre0[...])
    low[2 * width :, :] = tmm(act0[...], top0[...])
    far_grad = kept(0, block[...])
    to_recv, to_send = edge_backward(
        far_grad, edge_out[0], far_recv, far_recv_t, far_send_t, far_slope, chunk
    )
    far[0:width, :] = tmm(shared[...], to_recv)
    far[width : 2 * width, :] = tmm(raw[: h0.shape[0], :], to_send)
    far[2 * width :, :] = tmm(far_q[...], far_grad)
    line = jnp.sum(rows * h1[...], axis=0, keepdims=True)
    line = line + row_product(jnp.sum(rows * act, axis=0, keepdims=True), node_out[1])
    tail[...] = jnp.concatenate([line, loss[...], jnp.zeros((EXTRA - 2, width), F32)], axis=0)


def far_kernel(chunk, names, size, *refs):
    raws, refs = unpack(names, refs)
    (edge_in, flat, mine, *refs), own_send_t = refs[:-1], refs[-1]
    edges = own_send_t.shape[1]
    lanes = edge_in.shape[2]
    first = own_send_t.shape[0] + edges // lanes
    flat_column = flat[:, 0:1]
    for b in range(edges // lanes):
        own_send_t[:, pl.ds(b * lanes, lanes)] = onehot(
            flat_column, mine[first + b : first + b + 1, :]
        )
    at = 0
    for place, raw in enumerate(raws):
        if raw is None:
            continue
        shared_out, slope, q_out, recv, recv_t, send, send_t = refs[at : at + 7]
        at += 7
        edges, width = slope.shape
        nodes = send_t.shape[0]
        count = edges // width
        block = jnp.concatenate(
            [raw[nodes:, :], jnp.zeros((width + nodes - raw.shape[0], width), F32)], axis=0
        )
        columns = block.T
        own = block[2 * count + place : 2 * count + place + 1, :size]
        down = columns[:size, 2 * count + place : 2 * count + place + 1]
        along = lax.broadcasted_iota(jnp.int32, (1, nodes), 1).astype(F32)
        across = lax.broadcasted_iota(jnp.int32, (nodes, 1), 0).astype(F32)
        for b in range(count):
            rows = pl.ds(b * width, width)
            recv[rows, :] = onehot(columns[:, b : b + 1], own)
            send[rows, :] = onehot(columns[:, count + b : count + b + 1], along)
            recv_t[:, rows] = onehot(down, block[b : b + 1])
            send_t[:, rows] = onehot(across, block[count + b : count + b + 1])
        features = raw[:nodes, :]
        shared = fold(dot(onehot(down, along), side(features)))
        shared_out[...] = shared
        to_recv = side(mm(shared, edge_in[0, :width]))
        to_send = side(mm(features, edge_in[0, width:]))
        total = None
        for start in range(0, edges, chunk):
            rows = pl.ds(start, chunk)
            pre = fold(dot(recv[rows, :], to_recv) + dot(send[rows, :], to_send))
            act, rise = silu_parts(pre)
            slope[rows, :] = rise
            part = dot(recv_t[:, rows], side(act))
            total = part if total is None else total + part
        q_out[...] = fold(total)


def put_rows(ref, at, value):
    ref[at : at + value.shape[0], :] = value
    return at + value.shape[0]


def end_kernel(chunk, names, *refs):
    own, refs = refs[:4], refs[4:]
    came, refs = unpack(names, refs)
    h, q, recv, recv_t, send_t, slope, edge_out, node_low, high, far, tail, mine, other = refs
    local_grad = take_sum(own, came)
    to_recv, to_send = edge_backward(local_grad, edge_out[0], recv, recv_t, send_t, slope, chunk)
    width = h.shape[1]
    low = [
        node_low[...],
        tmm(h[...], to_recv) + far[0:width, :],
        tmm(h[...], to_send) + far[width : 2 * width, :],
        tmm(q[...], local_grad) + far[2 * width :, :],
        tail[...],
    ]

    def write(ref_high, ref_low):
        at = 0
        for value in low:
            at = put_rows(ref_low, at, value)
        put_rows(ref_high, put_rows(ref_high, 0, high[...]), tail[...])

    first = lax.axis_index("sub") == 0
    pl.when(first)(lambda: write(mine, other))
    pl.when(jnp.logical_not(first))(lambda: write(other, mine))


def quarters_kernel(mine, other, *outs):
    per = outs[0].shape[0] - EXTRA
    own = lax.rem(lax.axis_index("dom"), 4)
    tail = mine[4 * per :, :] + other[4 * per :, :]
    for away, out in enumerate(outs):
        rows = pl.ds(pl.multiple_of(jnp.bitwise_xor(own, away) * per, 8), per)
        out[:per, :] = mine[rows, :] + other[rows, :]
        out[per:, :] = tail


def four_kernel(a, b, c, d, out):
    out[...] = (a[...] + b[...]) + (c[...] + d[...])


def two_kernel(a, b, out):
    out[...] = a[...] + b[...]


def last_sum_kernel(a, b, out, tail):
    per = out.shape[0]
    out[...] = a[:per, :] + b[:per, :]
    tail[...] = a[per:, :] + b[per:, :]


def scale_kernel(params, count, *refs):
    near, far = refs[:4], refs[4:8]
    tail, loss, edge_in, edge_out, node_in, node_out, decoder = refs[8:]
    width = tail.shape[1]
    line = tail[0:1]
    squares = []
    for group in (near, far):
        sums = [jnp.sum(ref[...] * ref[...], axis=0, keepdims=True) for ref in group]
        squares.append((sums[0] + sums[1]) + (sums[2] + sums[3]))
    every = jnp.sum(squares[0] + squares[1] + line * line, axis=1, keepdims=True)
    scale = 1.0 / jnp.sqrt(every / params + 1e-06)
    decoder[...] = line * scale
    loss[...] = tail[1:2] / count
    where = [(node_in, at) for at in range(2)] + [(node_out, 0)]
    where = where + [(edge_in, at) for at in range(2)] + [(edge_out, 0)]

    def write(own, layer, group):
        per = group[0].shape[0]
        for quarter in range(4):
            ref = group[quarter ^ own]
            at = 0
            while at < per:
                block, inside = divmod(quarter * per + at, width)
                take = min(width - inside, per - at)
                out, half = where[block]
                first = half * width + inside
                out[layer, first : first + take, :] = ref[at : at + take, :] * scale
                at += take

    here = lax.rem(lax.axis_index("dom"), 4)
    side_here = lax.axis_index("sub")
    for own in range(4):
        for core in range(2):
            def both(own=own, core=core):
                write(own, 1 - core, near)
                write(own, core, far)

            pl.when(jnp.logical_and(here == own, side_here == core))(both)


def call(kernel, outs, *args):
    shapes = [jax.ShapeDtypeStruct(shape, dtype) for shape, dtype in outs]
    return pl.pallas_call(
        kernel,
        out_shape=shapes,
        in_specs=[VMEM] * len(args),
        out_specs=[VMEM] * len(shapes),
        compiler_params=pltpu.CompilerParams(vmem_limit_bytes=16 * 2**20),
    )(*args)


def pairs(count, offset):
    found = []
    for low in range(offset, count - 1, 2):
        found += [(low, low + 1), (low + 1, low)]
    paired = [source for source, _ in found]
    return found, [at for at in range(count) if found and at not in paired]


def moves(n_dom, n_sub, at):
    along, other = (n_dom, n_sub) if AXES[at] == "dom" else (n_sub, n_dom)
    found, alone = pairs(along, OFFSETS[at])

    def spot(here, there):
        return here * n_sub + there if AXES[at] == "dom" else there * n_sub + here

    listed = []
    for there in range(other):
        listed += [(spot(source, there), spot(target, there)) for source, target in found]
        beside = there if other % 2 else there ^ 1
        listed += [(spot(end, there), spot(end, beside)) for end in alone]
    return listed


def per_device(
    node_feats, edge_in, edge_out, node_in, node_out, decoder, edge_index, halo_index, target
):
    nodes, width = node_feats.shape
    edges = edge_index.shape[1]
    size = halo_index.shape[2]
    n_dom, n_sub = lax.axis_size("dom"), lax.axis_size("sub")
    count = nodes * n_dom * n_sub
    if n_dom < 3 or nodes > 256 or edge_in.shape[0] != 2 or 4 * size != nodes:
        raise ValueError("unsupported sizes")
    chunk = 256
    links = [moves(n_dom, n_sub, at) for at in range(4)]
    names = tuple(1 if link else 0 for link in links)

    def exchange(blocks, last=4, first=0):
        came = [None] * 4
        for at in range(first, last):
            if links[at]:
                came[at] = lax.ppermute(blocks[at], ("dom", "sub"), links[at])
        return [block for block in came if block is not None]

    node_shape = ((nodes, width), F32)
    edge_shape = ((edges, width), F32)
    block_shapes = [((size, width), F32)] * 4

    weights = (edge_in, edge_out, node_in, node_out)
    sources = (
        node_feats, edge_index, halo_index, target.reshape(1, nodes), decoder.reshape(1, width),
        *weights,
    )
    raw_shape = ((nodes + 2 * edges // width + 4, width), F32)
    shapes = [
        ((1, nodes), F32), ((1, width), F32), *[(weight.shape, F32) for weight in weights],
        ((nodes, 128), F32),
        ((edges, nodes), BF16), ((edges, nodes), BF16), ((nodes, edges), BF16),
        node_shape, edge_shape, node_shape, raw_shape, *block_shapes,
    ]
    (wanted, readout, edge_in, edge_out, node_in, node_out,
     flat, recv, send, recv_t, h0, slope0, q0, raw, *blocks) = pl.pallas_call(
        functools.partial(first_kernel, chunk),
        out_shape=[jax.ShapeDtypeStruct(shape, dtype) for shape, dtype in shapes],
        in_specs=[pl.BlockSpec(memory_space=pltpu.HBM)] * len(sources),
        out_specs=[VMEM] * len(shapes),
        scratch_shapes=[
            pltpu.VMEM(node_feats.shape, F32),
            pltpu.VMEM(edge_index.shape, jnp.int32),
            pltpu.VMEM(halo_index.shape, jnp.int32),
            pltpu.SemaphoreType.DMA((len(sources),)),
        ],
        compiler_params=pltpu.CompilerParams(vmem_limit_bytes=16 * 2**20),
    )(*[pltpu.with_memory_space_constraint(source, pltpu.HBM) for source in sources])
    message = ((2 * size + EXTRA, width), F32)
    came = exchange(blocks)
    far_names = (names[0], 0, 0, 0)
    raws = exchange([raw], 1, 0)
    agg0, h1, act0, gate0, slope1, q1, pre, known, *messages = call(
        functools.partial(middle_kernel, chunk, names),
        [node_shape, node_shape, node_shape, node_shape, edge_shape, node_shape,
         node_shape, node_shape, *[message] * 4],
        *blocks, *came,
        h0, flat, wanted, readout, recv, send, recv_t, node_in, node_out, edge_in, edge_out,
    )
    came = exchange(messages)
    far_shapes = [
        ((size, width), F32), edge_shape, ((size, width), F32),
        ((edges, size), BF16), ((size, edges), BF16), ((edges, nodes), BF16), ((nodes, edges), BF16),
    ]
    fars = call(
        functools.partial(far_kernel, chunk, far_names, size),
        far_shapes * len(raws) + [((nodes, edges), BF16)],
        *raws, edge_in, flat, raw,
    )
    shared, far_slope, far_q, far_recv, far_recv_t, _, far_send_t, send_t = fars
    (agg1, act1, pre1, seed, local1, to_recv1, to_send1, top0, pre0, pred, loss,
     *blocks) = call(
        functools.partial(back_kernel, chunk, count, names),
        [*[node_shape] * 9, ((1, nodes), F32), ((1, width), F32), *block_shapes],
        *messages, *came,
        flat, readout, pre, known, gate0, recv, recv_t, send_t, slope1,
        edge_in, edge_out, node_in, node_out, far_q,
    )
    came = exchange(blocks, 4, 1)
    high, node_low, far, tail = call(
        functools.partial(grads_kernel, chunk=chunk),
        [((6 * width, width), F32), ((3 * width, width), F32), ((3 * width, width), F32),
         ((EXTRA, width), F32)],
        h0, agg0, act0, pre0, top0, h1, agg1, act1, pre1, seed, q1, local1, to_recv1, to_send1,
        readout, node_out, loss, blocks[0], *raws, shared, far_slope, far_q, far_recv, far_recv_t,
        far_send_t, edge_out,
    )
    rows = 6 * width
    groups = n_dom // 4
    half = ((rows + EXTRA, width), F32)
    end_grads = call(
        functools.partial(end_kernel, chunk, (0,) + names[1:]),
        [half, half],
        *blocks, *came, h0, q0, recv, recv_t, send_t, slope0, edge_out, node_low, high, far, tail,
    )
    if n_sub != 2 or n_dom % 4 or groups & (groups - 1) or rows % 32:
        return slow_tail(count, *end_grads, pred)
    per = rows // 4
    quarter = ((per + EXTRA, width), F32)
    mine, other = end_grads

    def swap(value):
        return lax.ppermute(value, "sub", pairs(n_sub, 0)[0])

    def across(value, away):
        return lax.ppermute(value, "dom", [(at, at ^ away) for at in range(n_dom)])

    def beside(value, first, second):
        moves = [
            (at * n_sub + core, (at ^ away) * n_sub + core)
            for at in range(n_dom)
            for core, away in enumerate((first, second))
        ]
        return lax.ppermute(value, ("dom", "sub"), moves)

    parts = call(quarters_kernel, [quarter] * 4, mine, swap(other))
    came = [across(parts[away], away) for away in (3, 2, 1)]
    (total,) = call(four_kernel, [quarter], parts[0], came[2], came[1], came[0])
    aways = [4 << at for at in range(groups.bit_length() - 1)]
    for step in range(len(aways) - 1):
        (total,) = call(two_kernel, [quarter], total, beside(total, aways[step], aways[-1 - step]))
    far = beside(total, aways[-1], aways[0]) if aways else jnp.zeros_like(total)
    total, tail = call(
        last_sum_kernel, [((per, width), F32), ((EXTRA, width), F32)], total, far
    )
    near = [total] + [across(total, away) for away in range(1, 4)]
    far = [swap(value) for value in near]
    params = 2 * 6 * width * width + width
    loss, g_edge_in, g_edge_out, g_node_in, g_node_out, g_decoder = call(
        functools.partial(scale_kernel, params, count),
        [
            ((1, width), F32),
            ((2, 2 * width, width), F32), ((2, width, width), F32),
            ((2, 2 * width, width), F32), ((2, width, width), F32),
            ((1, width), F32),
        ],
        *near, *far, tail,
    )
    return (
        loss[0, 0], pred.reshape(nodes), g_edge_in, g_edge_out, g_node_in, g_node_out,
        g_decoder.reshape(width),
    )


def slow_tail(count, mine, other, pred):
    first = lax.axis_index("sub") == 0
    width = mine.shape[1]
    rows = mine.shape[0] - EXTRA
    high = jnp.where(first, mine, other)
    low = jnp.where(first, other, mine)
    total = lax.psum(jnp.concatenate([low[:rows], high], axis=0), ("dom", "sub"))
    body = total[: 2 * rows + 1]
    params = (2 * rows + 1) * width
    scale = 1.0 / jnp.sqrt(jnp.sum(body * body) / params + 1e-06)
    grads = (total[: 2 * rows] * scale).reshape(2, 2, 3 * width, width)
    return (
        total[2 * rows + 1, 0] / count, pred.reshape(-1),
        grads[:, 1, : 2 * width], grads[:, 1, 2 * width :],
        grads[:, 0, : 2 * width], grads[:, 0, 2 * width :],
        total[2 * rows] * scale,
    )


def solution(mesh):
    placed = (
        P(("dom", "sub"), None),
        P(),
        P(),
        P(),
        P(),
        P(),
        P(None, ("dom", "sub")),
        P(("dom", "sub"), None, None),
        P(("dom", "sub")),
    )
    return jax.shard_map(
        per_device,
        mesh=mesh,
        in_specs=placed,
        out_specs=(P(), P(("dom", "sub")), P(), P(), P(), P(), P()),
        check_vma=False,
    )
```

```python
import functools

import jax
import jax.numpy as jnp
from jax import lax
from jax.experimental import pallas as pl
from jax.experimental.pallas import tpu as pltpu
from jax.sharding import PartitionSpec as P


F32 = jnp.float32
BF16 = jnp.bfloat16
VMEM = pl.BlockSpec(memory_space=pltpu.VMEM)
EXTRA = 8


def halves(x):
    high = x.astype(BF16)
    low = (x - high.astype(F32)).astype(BF16)
    return high, low


def side(x):
    return jnp.concatenate(halves(x), axis=1)


def fold(x):
    width = x.shape[1] // 2
    return x[:, :width] + x[:, width:]


def dot(a, b, dims=((1,), (0,))):
    return lax.dot_general(a, b, (dims, ((), ())), preferred_element_type=F32)


def mm(x, w):
    wide = side(w)
    return fold(dot(side(x), jnp.concatenate([wide, wide], axis=0)))


def mmt(x, w):
    high, low = halves(w)
    both = jnp.concatenate(
        [jnp.concatenate([high, high], axis=1), jnp.concatenate([low, low], axis=1)], axis=0
    )
    return fold(dot(side(x), both, ((1,), (1,))))


def tmm(x, y):
    wide = fold(dot(side(x), side(y), ((0,), (0,))))
    width = x.shape[1]
    return wide[:width] + wide[width:]


def silu_parts(v):
    gate = 1.0 / (1.0 + jnp.exp(-v))
    return v * gate, gate * (1.0 + v * (1.0 - gate))


def row_of(column):
    n = column.shape[0]
    eye = lax.broadcasted_iota(jnp.int32, (n, n), 0) == lax.broadcasted_iota(jnp.int32, (n, n), 1)
    return jnp.sum(jnp.where(eye, column, 0.0), axis=0, keepdims=True)


def onehot(left, right):
    return jnp.where(left.astype(BF16) == right.astype(BF16), BF16(1), BF16(0))


def edge_forward(features, weight_in, recv, send, recv_t, slope_ref, chunk):
    width = features.shape[1]
    to_recv = side(mm(features, weight_in[:width]))
    to_send = side(mm(features, weight_in[width:]))
    total = None
    for start in range(0, recv.shape[0], chunk):
        rows = pl.ds(start, chunk)
        pre = fold(dot(recv[rows, :], to_recv) + dot(send[rows, :], to_send))
        act, slope = silu_parts(pre)
        slope_ref[rows, :] = slope
        part = dot(recv_t[:, rows], side(act))
        total = part if total is None else total + part
    return fold(total)


def edge_backward(local_grad, weight_out, recv, recv_t, send_t, slope_ref, chunk):
    spread = side(mmt(local_grad, weight_out))
    total_r = total_s = None
    for start in range(0, recv.shape[0], chunk):
        rows = pl.ds(start, chunk)
        grad = side(fold(dot(recv[rows, :], spread)) * slope_ref[rows, :])
        part_r = dot(recv_t[:, rows], grad)
        part_s = dot(send_t[:, rows], grad)
        total_r = part_r if total_r is None else total_r + part_r
        total_s = part_s if total_s is None else total_s + part_s
    return fold(total_r), fold(total_s)


def node_forward(features, summed, weight_in, weight_out):
    width = features.shape[1]
    pre = mm(features, weight_in[:width]) + mm(summed, weight_in[width:])
    act, slope = silu_parts(pre)
    return features + mm(act, weight_out), act, slope


def put_blocks(value, refs):
    size = refs[0].shape[0]
    for at, ref in enumerate(refs):
        ref[...] = value[at * size : (at + 1) * size]


AXES = ("dom", "dom", "sub", "sub")
OFFSETS = (1, 0, 0, 1)


def kept(at, value):
    if pairs(lax.axis_size(AXES[at]), OFFSETS[at])[1]:
        partner = jnp.bitwise_xor(lax.axis_index(AXES[at]) + OFFSETS[at], 1) - OFFSETS[at]
        there = jnp.logical_and(partner >= 0, partner < lax.axis_size(AXES[at]))
        return jnp.where(there, value, 0.0)
    return value


def take_sum(own, came):
    parts = [
        ref[...] + kept(at, came[at][...]) if came[at] is not None else ref[...]
        for at, ref in enumerate(own)
    ]
    return jnp.concatenate(parts, axis=0)


def even(axis):
    return lax.rem(lax.axis_index(axis), 2) == 0


def first_kernel(
    chunk, feats_hbm, index_hbm, halo_hbm, target_hbm, decoder_hbm, *refs
):
    weights_hbm, refs = refs[:4], refs[4:]
    (target, decoder, edge_in, edge_out, node_in, node_out,
     flat_out, recv, send, recv_t, h_out, slope, q_out, raw) = refs[:14]
    blocks, (feats, index, halo, sems) = refs[14:18], refs[18:]
    copies = [
        pltpu.make_async_copy(source, place, sems.at[at])
        for at, (source, place) in enumerate(
            zip(
                (index_hbm, halo_hbm, feats_hbm, *weights_hbm, target_hbm, decoder_hbm),
                (index, halo, feats, edge_in, edge_out, node_in, node_out, target, decoder),
            )
        )
    ]
    for copy in copies:
        copy.start()
    copies[0].wait()
    copies[1].wait()
    nodes = feats.shape[0]
    edges = index.shape[1]
    lanes = 128
    count = edges // lanes
    size = halo.shape[2]
    pieces = [index[0:1, pl.ds(b * lanes, lanes)] for b in range(count)]
    pieces += [index[1:2, pl.ds(b * lanes, lanes)] for b in range(count)]
    table = jnp.concatenate(pieces, axis=0).astype(F32)
    lists = jnp.concatenate([halo[0].astype(F32), jnp.zeros((4, lanes - size), F32)], axis=1)
    rest = jnp.zeros((lanes - 2 * count - 4, lanes), F32)
    columns = jnp.concatenate([table, lists, rest], axis=0).T
    by_dir = [columns[:size, 2 * count + k : 2 * count + k + 1] for k in range(4)]
    dom_even, sub_even = even("dom"), even("sub")
    flat = jnp.concatenate(
        [
            jnp.where(dom_even, by_dir[0], by_dir[1]),
            jnp.where(dom_even, by_dir[1], by_dir[0]),
            jnp.where(sub_even, by_dir[3], by_dir[2]),
            jnp.where(sub_even, by_dir[2], by_dir[3]),
        ],
        axis=0,
    )
    raw[nodes:, :] = jnp.concatenate(
        [
            table,
            jnp.where(dom_even, lists[0:1], lists[1:2]),
            jnp.where(dom_even, lists[1:2], lists[0:1]),
            jnp.where(sub_even, lists[3:4], lists[2:3]),
            jnp.where(sub_even, lists[2:3], lists[3:4]),
        ],
        axis=0,
    )
    flat_row = row_of(flat)
    flat_out[...] = jnp.broadcast_to(flat, flat_out.shape)
    for b in range(count):
        rows = pl.ds(b * lanes, lanes)
        recv[rows, :] = onehot(columns[:, b : b + 1], flat_row)
        send[rows, :] = onehot(columns[:, count + b : count + b + 1], flat_row)
        recv_t[:, rows] = onehot(flat, table[b : b + 1])
    place = onehot(flat, lax.broadcasted_iota(jnp.int32, (1, nodes), 1).astype(F32))
    copies[2].wait()
    plain = feats[...]
    raw[:nodes, :] = plain
    features = fold(dot(place, side(plain)))
    h_out[...] = features
    copies[3].wait()
    q = edge_forward(features, edge_in[0], recv, send, recv_t, slope, chunk)
    q_out[...] = q
    copies[4].wait()
    put_blocks(mm(q, edge_out[0]), blocks)
    for copy in copies[5:]:
        copy.wait()


def unpack(names, refs):
    came = []
    at = 0
    for there in names:
        came.append(refs[at] if there else None)
        at += there
    return came, refs[at:]


def middle_kernel(chunk, names, *refs):
    own, refs = refs[:4], refs[4:]
    came, refs = unpack(names, refs)
    (h, flat_ref, target, decoder, recv, send, recv_t, node_in, node_out, edge_in, edge_out,
     agg_out, h_out, node_act, node_slope, slope, q_out, pre_out, known_out, *messages) = refs
    nodes, width = h.shape
    summed = take_sum(own, came)
    agg_out[...] = summed
    features, act, gate = node_forward(h[...], summed, node_in[0], node_out[0])
    h_out[...] = features
    node_act[...] = act
    node_slope[...] = gate
    pre = mm(features, node_in[1, :width])
    pre_out[...] = pre
    base = jnp.sum(features * decoder[...], axis=1, keepdims=True)
    here = flat_ref[:, 0:1] == lax.broadcasted_iota(jnp.int32, (nodes, nodes), 1).astype(F32)
    wanted = jnp.sum(jnp.where(here, target[...], 0.0), axis=1, keepdims=True)
    first = lax.broadcasted_iota(jnp.int32, (nodes, width), 1) == 0
    known_out[...] = jnp.where(first, base, wanted)
    size = own[0].shape[0]
    short = base - wanted
    for at, message in enumerate(messages):
        rows = slice(at * size, (at + 1) * size)
        message[size : 2 * size, :] = pre[rows]
        line = row_of(short[rows])
        line = jnp.concatenate([line, jnp.zeros((1, width - size), F32)], axis=1)
        message[2 * size :, :] = jnp.concatenate(
            [line, jnp.zeros((EXTRA - 1, width), F32)], axis=0
        )
    q = edge_forward(features, edge_in[1], recv, send, recv_t, slope, chunk)
    q_out[...] = q
    local = mm(q, edge_out[1])
    for at, message in enumerate(messages):
        message[:size, :] = local[at * size : (at + 1) * size]


def column_of(row):
    n = row.shape[1]
    eye = lax.broadcasted_iota(jnp.int32, (n, n), 0) == lax.broadcasted_iota(jnp.int32, (n, n), 1)
    return jnp.sum(jnp.where(eye, row, 0.0), axis=1, keepdims=True)


def row_product(row, weight):
    return mm(jnp.broadcast_to(row, (8, row.shape[1])), weight)[0:1]


def back_kernel(chunk, count, names, *refs):
    own, refs = refs[:4], refs[4:]
    came, refs = unpack(names, refs)
    (flat_ref, decoder, pre_ref, known, node_slope, recv, recv_t, send_t, slope,
     edge_in, edge_out, node_in, node_out, _,
     agg_out, act_out, pre1_out, seed_out, local_out, recv_out, send_out, top_out, pre0_out,
     pred_out, loss_out, *blocks) = refs
    nodes, width = pre_ref.shape
    size = blocks[0].shape[0]
    summed = jnp.concatenate(
        [
            ref[:size, :] + kept(at, came[at][:size, :]) if came[at] is not None else ref[:size, :]
            for at, ref in enumerate(own)
        ],
        axis=0,
    )
    agg_out[...] = summed
    pre_agg = mm(summed, node_in[1, width:])
    act, gate = silu_parts(pre_ref[...] + pre_agg)
    act_out[...] = act
    weights = decoder[...]
    lead = row_of(jnp.sum(node_out[1] * weights, axis=1, keepdims=True))
    base, wanted = known[:, 0:1], known[:, 1:2]
    predicted = base + jnp.sum(act * lead, axis=1, keepdims=True)
    misfit = predicted - wanted
    seed = 2.0 * misfit / count
    seed_out[...] = jnp.broadcast_to(seed, seed_out.shape)
    here = flat_ref[:, 0:1] == lax.broadcasted_iota(jnp.int32, (nodes, nodes), 1).astype(F32)
    pred_out[...] = jnp.sum(jnp.where(here, predicted, 0.0), axis=0, keepdims=True)
    loss_out[...] = jnp.broadcast_to(
        jnp.sum(misfit * misfit, axis=0, keepdims=True), loss_out.shape
    )
    pre_grad = seed * lead * gate
    pre1_out[...] = pre_grad
    shared = []
    for at in range(4):
        rows = slice(at * size, (at + 1) * size)
        if came[at] is None:
            shared.append(pre_grad[rows])
            continue
        far_act, far_gate = silu_parts(came[at][size : 2 * size, :] + pre_agg[rows])
        far_misfit = column_of(came[at][2 * size : 2 * size + 1, :size])
        far_misfit = far_misfit + jnp.sum(far_act * lead, axis=1, keepdims=True)
        far_seed = kept(at, 2.0 * far_misfit / count)
        shared.append(pre_grad[rows] + far_seed * lead * far_gate)
    local_grad = mmt(jnp.concatenate(shared, axis=0), node_in[1, width:])
    local_out[...] = local_grad
    to_recv, to_send = edge_backward(local_grad, edge_out[1], recv, recv_t, send_t, slope, chunk)
    recv_out[...] = to_recv
    send_out[...] = to_send
    top = (
        seed * weights
        + mmt(pre_grad, node_in[1, :width])
        + mmt(to_recv, edge_in[1, :width])
        + mmt(to_send, edge_in[1, width:])
    )
    top_out[...] = top
    pre0 = mmt(top, node_out[0]) * node_slope[...]
    pre0_out[...] = pre0
    put_blocks(mmt(pre0, node_in[0, width:]), blocks)


def grads_kernel(
    h0, agg0, act0, pre0, top0, h1, agg1, act1, pre1, seed, q1, local1, to_recv1, to_send1,
    decoder, node_out, loss, block, raw, shared, far_slope, far_q, far_recv, far_recv_t, far_send_t,
    edge_out, high, low, far, tail, early, *, chunk
):
    width = h0.shape[1]
    rows = seed[...]
    top1 = rows * decoder[...]
    act = act1[...]
    parts = [
        tmm(h1[...], pre1[...]),
        tmm(agg1[...], pre1[...]),
        tmm(act, top1),
        tmm(h1[...], to_recv1[...]),
        tmm(h1[...], to_send1[...]),
        tmm(q1[...], local1[...]),
    ]
    for at, part in enumerate(parts):
        high[at * width : (at + 1) * width, :] = part
    low[0:width, :] = tmm(h0[...], pre0[...])
    low[width : 2 * width, :] = tmm(agg0[...], pre0[...])
    low[2 * width :, :] = tmm(act0[...], top0[...])
    far_grad = kept(0, block[...])
    to_recv, to_send = edge_backward(
        far_grad, edge_out[0], far_recv, far_recv_t, far_send_t, far_slope, chunk
    )
    far[0:width, :] = tmm(shared[...], to_recv)
    far[width : 2 * width, :] = tmm(raw[: h0.shape[0], :], to_send)
    far[2 * width :, :] = tmm(far_q[...], far_grad)
    line = jnp.sum(rows * h1[...], axis=0, keepdims=True)
    line = line + row_product(jnp.sum(rows * act, axis=0, keepdims=True), node_out[1])
    end = jnp.concatenate([line, loss[...], jnp.zeros((EXTRA - 2, width), F32)], axis=0)
    tail[...] = end
    rows_high = high.shape[0]
    early[rows_high:, :] = end
    first = lax.axis_index("sub") == 0

    @pl.when(first)
    def _():
        early[: low.shape[0], :] = low[...]
        early[low.shape[0] : rows_high, :] = jnp.zeros(low.shape, F32)

    @pl.when(jnp.logical_not(first))
    def _():
        early[:rows_high, :] = high[...]


def far_kernel(chunk, names, size, *refs):
    raws, refs = unpack(names, refs)
    (edge_in, flat, mine, *refs), own_send_t = refs[:-1], refs[-1]
    edges = own_send_t.shape[1]
    lanes = edge_in.shape[2]
    first = own_send_t.shape[0] + edges // lanes
    flat_column = flat[:, 0:1]
    for b in range(edges // lanes):
        own_send_t[:, pl.ds(b * lanes, lanes)] = onehot(
            flat_column, mine[first + b : first + b + 1, :]
        )
    at = 0
    for place, raw in enumerate(raws):
        if raw is None:
            continue
        shared_out, slope, q_out, recv, recv_t, send, send_t = refs[at : at + 7]
        at += 7
        edges, width = slope.shape
        nodes = send_t.shape[0]
        count = edges // width
        block = jnp.concatenate(
            [raw[nodes:, :], jnp.zeros((width + nodes - raw.shape[0], width), F32)], axis=0
        )
        columns = block.T
        own = block[2 * count + place : 2 * count + place + 1, :size]
        down = columns[:size, 2 * count + place : 2 * count + place + 1]
        along = lax.broadcasted_iota(jnp.int32, (1, nodes), 1).astype(F32)
        across = lax.broadcasted_iota(jnp.int32, (nodes, 1), 0).astype(F32)
        for b in range(count):
            rows = pl.ds(b * width, width)
            recv[rows, :] = onehot(columns[:, b : b + 1], own)
            send[rows, :] = onehot(columns[:, count + b : count + b + 1], along)
            recv_t[:, rows] = onehot(down, block[b : b + 1])
            send_t[:, rows] = onehot(across, block[count + b : count + b + 1])
        features = raw[:nodes, :]
        shared = fold(dot(onehot(down, along), side(features)))
        shared_out[...] = shared
        to_recv = side(mm(shared, edge_in[0, :width]))
        to_send = side(mm(features, edge_in[0, width:]))
        total = None
        for start in range(0, edges, chunk):
            rows = pl.ds(start, chunk)
            pre = fold(dot(recv[rows, :], to_recv) + dot(send[rows, :], to_send))
            act, rise = silu_parts(pre)
            slope[rows, :] = rise
            part = dot(recv_t[:, rows], side(act))
            total = part if total is None else total + part
        q_out[...] = fold(total)


def end_kernel(chunk, names, *refs):
    own, refs = refs[:4], refs[4:]
    came, refs = unpack(names, refs)
    h, q, recv, recv_t, send_t, slope, edge_out, far, out = refs
    local_grad = take_sum(own, came)
    to_recv, to_send = edge_backward(local_grad, edge_out[0], recv, recv_t, send_t, slope, chunk)
    width = h.shape[1]
    out[0:width, :] = tmm(h[...], to_recv) + far[0:width, :]
    out[width : 2 * width, :] = tmm(h[...], to_send) + far[width : 2 * width, :]
    out[2 * width :, :] = tmm(q[...], local_grad) + far[2 * width :, :]


def quarters_kernel(high, node_low, edge_low, tail, early, late, *refs):
    outs, half = refs[:-1], refs[-1]
    per = outs[0].shape[0] - EXTRA
    own = lax.rem(lax.axis_index("dom"), 4)
    first = lax.axis_index("sub") == 0

    @pl.when(first)
    def _():
        half[...] = high[...] + early[: 4 * per, :]

    @pl.when(jnp.logical_not(first))
    def _():
        half[: 2 * per, :] = node_low[...] + early[: 2 * per, :]
        half[2 * per :, :] = edge_low[...] + late[...]

    end = tail[...] + early[4 * per :, :]
    for away, out in enumerate(outs):
        rows = pl.ds(pl.multiple_of(jnp.bitwise_xor(own, away) * per, 8), per)
        out[:per, :] = half[rows, :]
        out[per:, :] = end


def four_kernel(a, b, c, d, out):
    out[...] = (a[...] + b[...]) + (c[...] + d[...])


def two_kernel(a, b, out):
    out[...] = a[...] + b[...]


def last_sum_kernel(a, b, out, tail):
    per = out.shape[0]
    out[...] = a[:per, :] + b[:per, :]
    tail[...] = a[per:, :] + b[per:, :]


def scale_kernel(params, count, *refs):
    near, far = refs[:4], refs[4:8]
    tail, loss, edge_in, edge_out, node_in, node_out, decoder = refs[8:]
    width = tail.shape[1]
    line = tail[0:1]
    squares = []
    for group in (near, far):
        sums = [jnp.sum(ref[...] * ref[...], axis=0, keepdims=True) for ref in group]
        squares.append((sums[0] + sums[1]) + (sums[2] + sums[3]))
    every = jnp.sum(squares[0] + squares[1] + line * line, axis=1, keepdims=True)
    scale = 1.0 / jnp.sqrt(every / params + 1e-06)
    decoder[...] = line * scale
    loss[...] = tail[1:2] / count
    where = [(node_in, at) for at in range(2)] + [(node_out, 0)]
    where = where + [(edge_in, at) for at in range(2)] + [(edge_out, 0)]

    def write(own, layer, group):
        per = group[0].shape[0]
        for quarter in range(4):
            ref = group[quarter ^ own]
            at = 0
            while at < per:
                block, inside = divmod(quarter * per + at, width)
                take = min(width - inside, per - at)
                out, half = where[block]
                first = half * width + inside
                out[layer, first : first + take, :] = ref[at : at + take, :] * scale
                at += take

    here = lax.rem(lax.axis_index("dom"), 4)
    side_here = lax.axis_index("sub")
    for own in range(4):
        for core in range(2):
            def both(own=own, core=core):
                write(own, 1 - core, near)
                write(own, core, far)

            pl.when(jnp.logical_and(here == own, side_here == core))(both)


def call(kernel, outs, *args):
    shapes = [jax.ShapeDtypeStruct(shape, dtype) for shape, dtype in outs]
    return pl.pallas_call(
        kernel,
        out_shape=shapes,
        in_specs=[VMEM] * len(args),
        out_specs=[VMEM] * len(shapes),
        compiler_params=pltpu.CompilerParams(vmem_limit_bytes=16 * 2**20),
    )(*args)


def pairs(count, offset):
    found = []
    for low in range(offset, count - 1, 2):
        found += [(low, low + 1), (low + 1, low)]
    paired = [source for source, _ in found]
    return found, [at for at in range(count) if found and at not in paired]


def moves(n_dom, n_sub, at):
    along, other = (n_dom, n_sub) if AXES[at] == "dom" else (n_sub, n_dom)
    found, alone = pairs(along, OFFSETS[at])

    def spot(here, there):
        return here * n_sub + there if AXES[at] == "dom" else there * n_sub + here

    listed = []
    for there in range(other):
        listed += [(spot(source, there), spot(target, there)) for source, target in found]
        beside = there if other % 2 else there ^ 1
        listed += [(spot(end, there), spot(end, beside)) for end in alone]
    return listed


def per_device(
    node_feats, edge_in, edge_out, node_in, node_out, decoder, edge_index, halo_index, target
):
    nodes, width = node_feats.shape
    edges = edge_index.shape[1]
    size = halo_index.shape[2]
    n_dom, n_sub = lax.axis_size("dom"), lax.axis_size("sub")
    count = nodes * n_dom * n_sub
    if n_dom < 3 or nodes > 256 or edge_in.shape[0] != 2 or 4 * size != nodes:
        raise ValueError("unsupported sizes")
    chunk = 256
    links = [moves(n_dom, n_sub, at) for at in range(4)]
    names = tuple(1 if link else 0 for link in links)

    def exchange(blocks, last=4, first=0):
        came = [None] * 4
        for at in range(first, last):
            if links[at]:
                came[at] = lax.ppermute(blocks[at], ("dom", "sub"), links[at])
        return [block for block in came if block is not None]

    node_shape = ((nodes, width), F32)
    edge_shape = ((edges, width), F32)
    block_shapes = [((size, width), F32)] * 4

    weights = (edge_in, edge_out, node_in, node_out)
    sources = (
        node_feats, edge_index, halo_index, target.reshape(1, nodes), decoder.reshape(1, width),
        *weights,
    )
    raw_shape = ((nodes + 2 * edges // width + 4, width), F32)
    shapes = [
        ((1, nodes), F32), ((1, width), F32), *[(weight.shape, F32) for weight in weights],
        ((nodes, 128), F32),
        ((edges, nodes), BF16), ((edges, nodes), BF16), ((nodes, edges), BF16),
        node_shape, edge_shape, node_shape, raw_shape, *block_shapes,
    ]
    (wanted, readout, edge_in, edge_out, node_in, node_out,
     flat, recv, send, recv_t, h0, slope0, q0, raw, *blocks) = pl.pallas_call(
        functools.partial(first_kernel, chunk),
        out_shape=[jax.ShapeDtypeStruct(shape, dtype) for shape, dtype in shapes],
        in_specs=[pl.BlockSpec(memory_space=pltpu.HBM)] * len(sources),
        out_specs=[VMEM] * len(shapes),
        scratch_shapes=[
            pltpu.VMEM(node_feats.shape, F32),
            pltpu.VMEM(edge_index.shape, jnp.int32),
            pltpu.VMEM(halo_index.shape, jnp.int32),
            pltpu.SemaphoreType.DMA((len(sources),)),
        ],
        compiler_params=pltpu.CompilerParams(vmem_limit_bytes=16 * 2**20),
    )(*[pltpu.with_memory_space_constraint(source, pltpu.HBM) for source in sources])
    message = ((2 * size + EXTRA, width), F32)
    came = exchange(blocks)
    far_names = (names[0], 0, 0, 0)
    raws = exchange([raw], 1, 0)
    agg0, h1, act0, gate0, slope1, q1, pre, known, *messages = call(
        functools.partial(middle_kernel, chunk, names),
        [node_shape, node_shape, node_shape, node_shape, edge_shape, node_shape,
         node_shape, node_shape, *[message] * 4],
        *blocks, *came,
        h0, flat, wanted, readout, recv, send, recv_t, node_in, node_out, edge_in, edge_out,
    )
    came = exchange(messages)
    far_shapes = [
        ((size, width), F32), edge_shape, ((size, width), F32),
        ((edges, size), BF16), ((size, edges), BF16), ((edges, nodes), BF16), ((nodes, edges), BF16),
    ]
    fars = call(
        functools.partial(far_kernel, chunk, far_names, size),
        far_shapes * len(raws) + [((nodes, edges), BF16)],
        *raws, edge_in, flat, raw,
    )
    shared, far_slope, far_q, far_recv, far_recv_t, _, far_send_t, send_t = fars
    (agg1, act1, pre1, seed, local1, to_recv1, to_send1, top0, pre0, pred, loss,
     *blocks) = call(
        functools.partial(back_kernel, chunk, count, names),
        [*[node_shape] * 9, ((1, nodes), F32), ((1, width), F32), *block_shapes],
        *messages, *came,
        flat, readout, pre, known, gate0, recv, recv_t, send_t, slope1,
        edge_in, edge_out, node_in, node_out, far_q,
    )
    came = exchange(blocks, 4, 1)
    high, node_low, far, tail, early = call(
        functools.partial(grads_kernel, chunk=chunk),
        [((6 * width, width), F32), ((3 * width, width), F32), ((3 * width, width), F32),
         ((EXTRA, width), F32), ((6 * width + EXTRA, width), F32)],
        h0, agg0, act0, pre0, top0, h1, agg1, act1, pre1, seed, q1, local1, to_recv1, to_send1,
        readout, node_out, loss, blocks[0], *raws, shared, far_slope, far_q, far_recv, far_recv_t,
        far_send_t, edge_out,
    )
    rows = 6 * width
    groups = n_dom // 4
    (edge_low,) = call(
        functools.partial(end_kernel, chunk, (0,) + names[1:]),
        [((3 * width, width), F32)],
        *blocks, *came, h0, q0, recv, recv_t, send_t, slope0, edge_out, far,
    )
    if n_sub != 2 or n_dom % 4 or groups & (groups - 1) or rows % 32:
        return slow_tail(count, [node_low, edge_low, high, tail], pred)
    per = rows // 4
    quarter = ((per + EXTRA, width), F32)

    def swap(value):
        return lax.ppermute(value, "sub", pairs(n_sub, 0)[0])

    def across(value, away):
        return lax.ppermute(value, "dom", [(at, at ^ away) for at in range(n_dom)])

    def beside(value, first, second):
        moves = [
            (at * n_sub + core, (at ^ away) * n_sub + core)
            for at in range(n_dom)
            for core, away in enumerate((first, second))
        ]
        return lax.ppermute(value, ("dom", "sub"), moves)

    parts = pl.pallas_call(
        quarters_kernel,
        out_shape=[jax.ShapeDtypeStruct(*quarter)] * 4,
        in_specs=[VMEM] * 6,
        out_specs=[VMEM] * 4,
        scratch_shapes=[pltpu.VMEM((rows, width), F32)],
        compiler_params=pltpu.CompilerParams(vmem_limit_bytes=16 * 2**20),
    )(high, node_low, edge_low, tail, swap(early), swap(edge_low))
    came = [across(parts[away], away) for away in (3, 2, 1)]
    (total,) = call(four_kernel, [quarter], parts[0], came[2], came[1], came[0])
    aways = [4 << at for at in range(groups.bit_length() - 1)]
    for step in range(len(aways) - 1):
        (total,) = call(two_kernel, [quarter], total, beside(total, aways[step], aways[-1 - step]))
    far = beside(total, aways[-1], aways[0]) if aways else jnp.zeros_like(total)
    total, tail = call(
        last_sum_kernel, [((per, width), F32), ((EXTRA, width), F32)], total, far
    )
    near = [total] + [across(total, away) for away in range(1, 4)]
    far = [swap(value) for value in near]
    params = 2 * 6 * width * width + width
    loss, g_edge_in, g_edge_out, g_node_in, g_node_out, g_decoder = call(
        functools.partial(scale_kernel, params, count),
        [
            ((1, width), F32),
            ((2, 2 * width, width), F32), ((2, width, width), F32),
            ((2, 2 * width, width), F32), ((2, width, width), F32),
            ((1, width), F32),
        ],
        *near, *far, tail,
    )
    return (
        loss[0, 0], pred.reshape(nodes), g_edge_in, g_edge_out, g_node_in, g_node_out,
        g_decoder.reshape(width),
    )


def slow_tail(count, parts, pred):
    total = lax.psum(jnp.concatenate(parts, axis=0), ("dom", "sub"))
    width = total.shape[1]
    rows = (total.shape[0] - EXTRA) // 2
    body = total[: 2 * rows + 1]
    params = (2 * rows + 1) * width
    scale = 1.0 / jnp.sqrt(jnp.sum(body * body) / params + 1e-06)
    grads = (total[: 2 * rows] * scale).reshape(2, 2, 3 * width, width)
    return (
        total[2 * rows + 1, 0] / count, pred.reshape(-1),
        grads[:, 1, : 2 * width], grads[:, 1, 2 * width :],
        grads[:, 0, : 2 * width], grads[:, 0, 2 * width :],
        total[2 * rows] * scale,
    )


def solution(mesh):
    placed = (
        P(("dom", "sub"), None),
        P(),
        P(),
        P(),
        P(),
        P(),
        P(None, ("dom", "sub")),
        P(("dom", "sub"), None, None),
        P(("dom", "sub")),
    )
    return jax.shard_map(
        per_device,
        mesh=mesh,
        in_specs=placed,
        out_specs=(P(), P(("dom", "sub")), P(), P(), P(), P(), P()),
        check_vma=False,
    )
```
